16 devices in a mesh: rep: 1, dp: 16 (over x, y, z, core).
Axes of the slice: x: 2, y: 2, z: 2, core: 2. Of those that a mesh axis runs over, the one named last changes fastest.
Arguments:
- x: bfloat16 [16, 2048, 896], P(('rep', 'dp'))
- dy: bfloat16 [16, 2048, 896], P(('rep', 'dp'))
- w_gate: bfloat16 [2, 896, 2560], replicated
- w_up: bfloat16 [2, 896, 2560], replicated
- w_down: bfloat16 [2, 2560, 896], replicated
- m_w_gate: float32 [2, 896, 2560], P(None, 'dp')
- m_w_up: float32 [2, 896, 2560], P(None, 'dp')
- m_w_down: float32 [2, 2560, 896], P(None, 'dp')
- v_w_gate: float32 [2, 896, 2560], P(None, 'dp')
- v_w_up: float32 [2, 896, 2560], P(None, 'dp')
- v_w_down: float32 [2, 2560, 896], P(None, 'dp')
Outputs:
- output 1: bfloat16 [2, 896, 2560], P('rep')
- output 2: bfloat16 [2, 896, 2560], P('rep')
- output 3: bfloat16 [2, 2560, 896], P('rep')
- output 4: float32 [2, 896, 2560], P('rep', 'dp')
- output 5: float32 [2, 896, 2560], P('rep', 'dp')
- output 6: float32 [2, 2560, 896], P('rep', 'dp')
- output 7: float32 [2, 896, 2560], P('rep', 'dp')
- output 8: float32 [2, 896, 2560], P('rep', 'dp')
- output 9: float32 [2, 2560, 896], P('rep', 'dp')
All inputs are finite; a program needn't handle non-finite values.
Results may differ from the reference program's by a relative error of at most 0.022.
Values are sent between devices in bfloat16 or wider.
A program may use at most 2 GiB of HBM per device.

```python
import jax
import jax.numpy as jnp
from jax import lax

SEQUENCES = 16
TOKENS = 2048
D = 896
FF = 2560
LAYERS = 2
NAMES = ("w_gate", "w_up", "w_down")
SHAPES = {"w_gate": (LAYERS, D, FF), "w_up": (LAYERS, D, FF), "w_down": (LAYERS, FF, D)}


def bump(key, n, height):
    away = (jnp.arange(n, dtype=jnp.int32) - jax.random.randint(key, (), 0, n, jnp.int32)) % n
    return jnp.where(away < n // 8, height, 1.0)


def together(key, own, strength):
    shared = jax.random.normal(key, own.shape[1:], jnp.float32)
    return (own + strength * shared) * lax.rsqrt(1 + strength * strength)


def setup_inputs(seed: int = 0, part: int = 0) -> dict:
    kx, kdy, ka, kb, kz, kf, kh, kl, *keys = jax.random.split(jax.random.key(seed), 8 + 3 * len(NAMES))
    kx, kdy, ka, kb = (jax.random.fold_in(k, part) for k in (kx, kdy, ka, kb))
    kw, km, kv = (keys[i::3] for i in range(3))
    shape = (SEQUENCES, TOKENS, D)
    much_x, much_dy = jax.random.uniform(kz, (2,), jnp.float32, 0.0, 1.0)
    loud = 2.0 ** jax.random.uniform(jax.random.fold_in(kz, 1), (), jnp.float32, -1.0, 2.0)
    layers = 2.0 ** jax.random.uniform(kl, (LAYERS, 1, 1), jnp.float32, -1.0, 1.0)
    x = together(ka, jax.random.normal(kx, shape, jnp.float32), much_x) * bump(kf, D, 4.0)
    dy = together(kb, jax.random.normal(kdy, shape, jnp.float32), much_dy)
    drawn = {"x": x.astype(jnp.bfloat16), "dy": (loud * dy * (SEQUENCES * TOKENS) ** -0.5).astype(jnp.bfloat16)}
    for key, name in zip(kw, NAMES, strict=True):
        w = jax.random.normal(key, SHAPES[name], jnp.float32) * SHAPES[name][1] ** -0.5
        drawn[name] = (w * {"w_gate": 1.0, "w_up": bump(kh, FF, 4.0), "w_down": layers}[name]).astype(jnp.bfloat16)
    for key, name in zip(km, NAMES, strict=True):
        drawn[f"m_{name}"] = 0.1 * jax.random.normal(key, SHAPES[name], jnp.float32)
    for key, name in zip(kv, NAMES, strict=True):
        drawn[f"v_{name}"] = jax.random.uniform(key, SHAPES[name], jnp.float32, 0.005, 0.015)
    return drawn


def matmul(a, w):
    return jnp.dot(a, w, preferred_element_type=jnp.float32).astype(jnp.bfloat16)


def normed(h):
    wide = h.astype(jnp.float32)
    scale = lax.rsqrt(jnp.mean(wide**2, -1, keepdims=True) + 1e-6)
    return (wide * scale).astype(jnp.bfloat16)


def layer(h, w):
    a = normed(h)
    gate = jnp.dot(a, w["w_gate"], preferred_element_type=jnp.float32)
    up = jnp.dot(a, w["w_up"], preferred_element_type=jnp.float32)
    return h + matmul((jax.nn.silu(gate) * up).astype(jnp.bfloat16), w["w_down"])


def adamw(w, m, v, g):
    m = 0.9 * m + 0.1 * g
    v = 0.95 * v + 0.05 * g * g
    step = m * lax.rsqrt(v + 1e-8) + 0.1 * w
    return (w - 0.02 * step).astype(jnp.bfloat16), m, v


def clipped(gradients, sum_of_squares, count):
    factor = jnp.minimum(1.0, 0.5 * lax.rsqrt(sum_of_squares / count + 1e-30))
    return [g * factor for g in gradients]


def stack(weights, h):
    return lax.scan(lambda h, w: (layer(h, w), None), h, weights)[0]


def reference(x, dy, w_gate, w_up, w_down, m_w_gate, m_w_up, m_w_down, v_w_gate, v_w_up, v_w_down):
    weights = dict(zip(NAMES, (w_gate, w_up, w_down), strict=True))

    def take(so_far, sequence):
        h, by_y = sequence
        _, back = jax.vjp(lambda w: stack(w, h), weights)
        return jax.tree.map(lambda total, term: total + term.astype(jnp.float32), so_far, back(by_y)[0]), None

    none_yet = {name: jnp.zeros(w.shape, jnp.float32) for name, w in weights.items()}
    by_weights, _ = lax.scan(take, none_yet, (x, dy))
    gradients = [by_weights[name].astype(jnp.bfloat16).astype(jnp.float32) for name in NAMES]
    gradients = clipped(gradients, sum(jnp.sum(g * g) for g in gradients), sum(g.size for g in gradients))
    new = [
        adamw(w.astype(jnp.float32), m, v, g)
        for w, m, v, g in zip((w_gate, w_up, w_down), (m_w_gate, m_w_up, m_w_down), (v_w_gate, v_w_up, v_w_down), gradients, strict=True)
    ]
    return tuple(one[which] for which in range(3) for one in new)
```

```python
import jax
import jax.numpy as jnp
from jax import lax
from jax.sharding import PartitionSpec as P

NAMES = ("w_gate", "w_up", "w_down")
DEVICES = 16


def matmul(a, w):
    return jnp.dot(a, w, preferred_element_type=jnp.float32).astype(jnp.bfloat16)


def normed(h):
    wide = h.astype(jnp.float32)
    scale = lax.rsqrt(jnp.mean(wide**2, -1, keepdims=True) + 1e-6)
    return (wide * scale).astype(jnp.bfloat16)


def layer(h, w):
    a = normed(h)
    gate = jnp.dot(a, w["w_gate"], preferred_element_type=jnp.float32)
    up = jnp.dot(a, w["w_up"], preferred_element_type=jnp.float32)
    return h + matmul((jax.nn.silu(gate) * up).astype(jnp.bfloat16), w["w_down"])


def adamw(w, m, v, g):
    m = 0.9 * m + 0.1 * g
    v = 0.95 * v + 0.05 * g * g
    step = m * lax.rsqrt(v + 1e-8) + 0.1 * w
    return (w - 0.02 * step).astype(jnp.bfloat16), m, v


def solution(mesh):
    def step(x, dy, wg, wu, wd, *moments):
        m, v = moments[:3], moments[3:]
        layers = [dict(zip(NAMES, (wg[i], wu[i], wd[i]), strict=True)) for i in range(2)]
        h = x[0]
        backs = []
        for w in layers:
            h, back = jax.vjp(layer, h, w)
            backs.append(back)
        shards = [None, None]
        d = dy[0]
        for i in (1, 0):
            d, dw = backs[i](d)
            shards[i] = [lax.psum_scatter(dw[n], "dp", scatter_dimension=0, tiled=True) for n in NAMES]
        g = [jnp.stack([shards[0][k], shards[1][k]]).astype(jnp.float32) for k in range(3)]
        total = lax.psum(sum(jnp.sum(t * t) for t in g), "dp")
        count = sum(t.size for t in g) * DEVICES
        factor = jnp.minimum(1.0, 0.5 * lax.rsqrt(total / count + 1e-30))
        me = lax.axis_index("dp")
        news, ms, vs = [], [], []
        for k, w in enumerate((wg, wu, wd)):
            rows = w.shape[1] // DEVICES
            own = lax.dynamic_slice_in_dim(w, me * rows, rows, 1).astype(jnp.float32)
            nw, nm, nv = adamw(own, m[k], v[k], g[k] * factor)
            news.append(lax.all_gather(nw, "dp", axis=1, tiled=True))
            ms.append(nm)
            vs.append(nv)
        return (*news, *ms, *vs)

    seq = P(("rep", "dp"), None, None)
    whole = P(None, None, None)
    part = P(None, "dp", None)
    return jax.shard_map(
        step,
        mesh=mesh,
        in_specs=(seq, seq, whole, whole, whole) + (part,) * 6,
        out_specs=(P("rep", None, None),) * 3 + (P("rep", "dp", None),) * 6,
        check_vma=False,
    )
```

```python
import functools

import jax
import jax.numpy as jnp
from jax import lax
from jax.experimental import pallas as pl
from jax.experimental.pallas import tpu as pltpu
from jax.sharding import PartitionSpec as P

MESH = pl.DeviceIdType.MESH
F32, BF16 = jnp.float32, jnp.bfloat16
DEVICES, TOKENS, D, FF = 16, 2048, 896, 2560
COUNT = 2 * 3 * D * FF
TM = 256
NB = 256
ANY = pl.BlockSpec(memory_space=pl.ANY)
WHOLE = pl.BlockSpec(memory_space=pltpu.VMEM)

STRIDE = (8, 4, 2)
ORDER = ((0, 1, 2), (1, 2, 0), (2, 0, 1))
WIDE = (56, 2560, tuple((slice(0, 56), s) for s in (slice(0, 896), slice(896, 1792), slice(1792, 2560))))
TALL = (160, 896, tuple((s, slice(0, 896)) for s in (slice(0, 56), slice(56, 112), slice(112, 160))))


def size(s):
    return s.stop - s.start


def place():
    me = lax.axis_index("dp")
    return me, (me // 8 % 2, me // 4 % 2, me // 2 % 2), me % 2


def beside(me, xyz, axis):
    return me + STRIDE[axis] * (1 - 2 * xyz[axis])


def partner(me, core):
    return me + 1 - 2 * core


def rs_scratch(kind):
    r, c, parts = kind
    flat = [pltpu.VMEM((8, r, c), BF16), pltpu.VMEM((8, r, c), BF16)]
    for rows, cols in parts:
        flat += [pltpu.VMEM((7, size(rows), size(cols)), BF16)] * 2
    return flat + [pltpu.SemaphoreType.DMA((10,)), pltpu.SemaphoreType.DMA((10,)), pltpu.SemaphoreType.DMA(())]


RS_SCRATCH = 11


class Reduce:
    def __init__(self, kind, g, out, scratch):
        self.kind, self.g, self.out = kind, g, out
        self.own, self.other = scratch[:2]
        self.send, self.got = scratch[2:8:2], scratch[3:8:2]
        self.ssem, self.rsem, self.lsem = scratch[8:]
        self.me, self.xyz, self.core = place()

    def swap(self):
        return pltpu.make_async_remote_copy(
            self.g.at[:, 1 - self.core],
            self.other,
            self.ssem.at[9],
            self.rsem.at[9],
            device_id={"dp": partner(self.me, self.core)},
            device_id_type=MESH,
        )

    def load(self):
        return pltpu.make_async_copy(self.g.at[:, self.core], self.own, self.lsem)

    def hop(self, t, phase):
        at = pl.ds((0, 4, 6)[phase], (4, 2, 1)[phase])
        return pltpu.make_async_remote_copy(
            self.send[t].at[at],
            self.got[t].at[at],
            self.ssem.at[3 * t + phase],
            self.rsem.at[3 * t + phase],
            device_id={"dp": beside(self.me, self.xyz, ORDER[t][phase])},
            device_id_type=MESH,
        )

    def total(self, t, at, got):
        rows, cols = self.kind[2][t]
        block = sum(p * (4, 2, 1)[axis] for p, axis in zip(at, ORDER[t], strict=True))
        sum_ = self.own[block, rows, cols].astype(F32) + self.other[block, rows, cols].astype(F32)
        for i in got:
            sum_ = sum_ + self.got[t][i].astype(F32)
        return sum_

    def start(self):
        self.swap().start()
        self.load().start()

    def stage(self, n):
        if n == 0:
            self.load().wait()
            self.swap().wait_recv()
        for t in range(3):
            p1, p2, p3 = (self.xyz[axis] for axis in ORDER[t])
            if n:
                self.hop(t, n - 1).wait_recv()
            if n == 0:
                for j in range(2):
                    for k in range(2):
                        self.send[t][2 * j + k] = self.total(t, (1 - p1, j, k), ()).astype(BF16)
            elif n == 1:
                for k in range(2):
                    self.send[t][4 + k] = self.total(t, (p1, 1 - p2, k), (2 * (1 - p2) + k,)).astype(BF16)
            elif n == 2:
                self.send[t][6] = self.total(t, (p1, p2, 1 - p3), (2 * p2 + 1 - p3, 5 - p3)).astype(BF16)
            else:
                rows, cols = self.kind[2][t]
                self.out[rows, cols] = self.total(t, (p1, p2, p3), (2 * p2 + p3, 4 + p3, 6)).astype(BF16)
            if n < 3:
                self.hop(t, n).start()

    def finish(self):
        self.swap().wait_send()
        for t in range(3):
            for phase in range(3):
                self.hop(t, phase).wait_send()


def squares(g):
    wide = g.astype(F32)
    rows, cols = wide.shape
    s = jnp.sum((wide * wide).reshape(rows // 8, 8, cols), 0)
    return sum(s[:, i : i + 128] for i in range(0, cols, 128))


def clip_factor(shards, factor, squared, sums, ssem, rsem):
    me = lax.axis_index("dp")
    squared[...] = sum(squares(g[...]) for g in shards)

    def give(k, slot):
        to = (me + k) % DEVICES
        return pltpu.make_async_remote_copy(
            squared, sums.at[slot], ssem.at[k], rsem.at[slot], device_id={"dp": to}, device_id_type=MESH
        )

    for k in range(1, DEVICES):
        give(k, me).start()
    sums[me] = squared[...]
    for k in range(1, DEVICES):
        give(k, (me + k) % DEVICES).wait_recv()
    for k in range(1, DEVICES):
        give(k, me).wait_send()
    total = jnp.sum(jnp.sum(jnp.sum(sums[...], 0), 0, keepdims=True), 1, keepdims=True)
    f = jnp.minimum(1.0, 0.5 * lax.rsqrt(total / COUNT + 1e-30))
    factor[...] = jnp.broadcast_to(f, factor.shape)


def reduce_kernel(kinds, earlier, *refs):
    n = len(kinds)
    grads, before, outs, factor = refs[:n], refs[n : n + earlier], refs[n + earlier : 2 * n + earlier], refs[2 * n + earlier]
    scratch = refs[2 * n + earlier + 1 :]
    units = [
        Reduce(kinds[i], grads[i], outs[i], scratch[RS_SCRATCH * i : RS_SCRATCH * (i + 1)]) for i in range(n)
    ]
    for u in units:
        u.start()
    for s in range(4):
        for u in units:
            u.stage(s)
    for u in units:
        u.finish()
    clip_factor([*before, *outs], factor, *scratch[RS_SCRATCH * n :])


def reduce_scatter(kinds, grads, before):
    scratch = sum((rs_scratch(k) for k in kinds), [])
    scratch += [
        pltpu.VMEM((8, 128), F32),
        pltpu.VMEM((DEVICES, 8, 128), F32),
        pltpu.SemaphoreType.DMA((DEVICES,)),
        pltpu.SemaphoreType.DMA((DEVICES,)),
    ]
    return pl.pallas_call(
        functools.partial(reduce_kernel, kinds, len(before)),
        out_shape=[jax.ShapeDtypeStruct(k[:2], BF16) for k in kinds] + [jax.ShapeDtypeStruct((8, 128), F32)],
        in_specs=[ANY] * len(kinds) + [WHOLE] * len(before),
        out_specs=[WHOLE] * (len(kinds) + 1),
        scratch_shapes=scratch,
        compiler_params=pltpu.CompilerParams(has_side_effects=True, vmem_limit_bytes=60 * 1024 * 1024),
        name="reduce_scatter",
    )(*[g.reshape(8, 2, *k[:2]) for g, k in zip(grads, kinds, strict=True)], *before)


class Gather:
    def __init__(self, kind, own, out, layer, ssem, rsem, csem):
        self.kind, self.own, self.out, self.layer = kind, own, out, layer
        self.ssem, self.rsem, self.csem = ssem, rsem, csem
        self.me, self.xyz, self.core = place()

    def local(self):
        x, y, z = self.xyz
        return pltpu.make_async_copy(self.own, self.out.at[self.layer, x, y, z, self.core], self.csem)

    def blocks(self, t, core, known, other=None):
        rows, cols = self.kind[2][t]
        index = []
        for axis in range(3):
            p = self.xyz[axis]
            index.append(slice(None) if axis in known else (1 - p if axis == other else p))
        return self.out.at[(self.layer, *index, core, rows, cols)]

    def hop(self, t, phase, arriving=False):
        axis = ORDER[t][phase]
        known = ORDER[t][:phase]
        src = self.blocks(t, self.core, known)
        dst = self.blocks(t, self.core, known, axis) if arriving else src
        if phase == 0 and not arriving:
            src = self.own.at[self.kind[2][t]]
        return pltpu.make_async_remote_copy(
            src,
            dst,
            self.ssem.at[3 * t + phase],
            self.rsem.at[3 * t + phase],
            device_id={"dp": beside(self.me, self.xyz, axis)},
            device_id_type=MESH,
        )

    def share(self, t, phase, core):
        ref = self.blocks(t, core, ORDER[t][:phase], ORDER[t][phase])
        return pltpu.make_async_remote_copy(
            ref,
            ref,
            self.ssem.at[10 + 3 * t + phase],
            self.rsem.at[10 + 3 * t + phase],
            device_id={"dp": partner(self.me, self.core)},
            device_id_type=MESH,
        )

    def share_own(self, core):
        x, y, z = self.xyz
        return pltpu.make_async_remote_copy(
            self.own,
            self.out.at[self.layer, x, y, z, core],
            self.ssem.at[9],
            self.rsem.at[9],
            device_id={"dp": partner(self.me, self.core)},
            device_id_type=MESH,
        )

    def start(self):
        self.local().start()
        for t in range(3):
            self.hop(t, 0).start()
        self.share_own(self.core).start()

    def stage(self, phase):
        if phase == 0:
            self.local().wait()
        for t in range(3):
            self.hop(t, phase, True).wait_recv()
            if phase < 2:
                self.hop(t, phase + 1).start()
            self.share(t, phase, self.core).start()

    def finish(self):
        self.share_own(1 - self.core).wait_recv()
        self.share_own(self.core).wait_send()
        for t in range(3):
            for phase in range(3):
                self.share(t, phase, 1 - self.core).wait_recv()
                self.share(t, phase, self.core).wait_send()
                self.hop(t, phase).wait_send()


def gather_kernel(*refs):
    owns, outs, (ssem, rsem, csem) = refs[:3], refs[3:6], refs[6:]
    units = []
    for layer in range(2):
        for i, kind in enumerate((WIDE, WIDE, TALL)):
            u = 3 * layer + i
            units.append(Gather(kind, owns[i].at[layer], outs[i], layer, ssem.at[u], rsem.at[u], csem.at[u]))
    for u in units:
        u.start()
    for phase in range(3):
        for u in units:
            u.stage(phase)
    for u in units:
        u.finish()


def all_gather(owns):
    outs = pl.pallas_call(
        gather_kernel,
        out_shape=[jax.ShapeDtypeStruct((2, 2, 2, 2, 2, *o.shape[1:]), BF16) for o in owns],
        in_specs=[WHOLE] * 3,
        out_specs=[ANY] * 3,
        scratch_shapes=[
            pltpu.SemaphoreType.DMA((6, 19)),
            pltpu.SemaphoreType.DMA((6, 19)),
            pltpu.SemaphoreType.DMA((6,)),
        ],
        compiler_params=pltpu.CompilerParams(has_side_effects=True),
        name="all_gather",
    )(*owns)
    return [o.reshape(2, DEVICES * o.shape[-2], o.shape[-1]) for o in outs]


def dot(a, b):
    return jnp.dot(a, b, preferred_element_type=F32)


def dot_t(a, b):
    return lax.dot_general(a, b, (((1,), (1,)), ((), ())), preferred_element_type=F32)


def norm(h):
    wide = h.astype(F32)
    scale = lax.rsqrt(jnp.mean(wide * wide, -1, keepdims=True) + 1e-6)
    return wide, scale, (wide * scale).astype(BF16)


def gated_back(gate, up, dact):
    sig = jax.nn.sigmoid(gate)
    d = dact.astype(F32)
    dup = d * (gate * sig)
    dgate = d * up * (sig * (1 + gate * (1 - sig)))
    return dgate.astype(BF16), dup.astype(BF16)


def forward_kernel(x, wg, wu, wd, h1, at, act, gate, up):
    h = x[...]
    _, _, a = norm(h)
    at[...] = a.T
    g = dot(a, wg[...])
    u = dot(a, wu[...])
    gate[...] = g
    up[...] = u
    s = (g * jax.nn.sigmoid(g) * u).astype(BF16)
    act[...] = s
    h1[...] = h + dot(s, wd[...]).astype(BF16)


def last_kernel(h1, dy, wg, wu, wd, at, dyt, act, dgate, dup):
    _, _, a = norm(h1[...])
    at[...] = a.T
    dyt[...] = dy[...].T
    g = dot(a, wg[...])
    u = dot(a, wu[...])
    act[...] = (g * jax.nn.sigmoid(g) * u).astype(BF16)
    dact = dot_t(dy[...], wd[...]).astype(BF16)
    dgate[...], dup[...] = gated_back(g, u, dact)


def between_kernel(dg1, du1, h1, dy, gate, up, wg, wu, wd, dht, dgate, dup):
    da = dot_t(dg1[...], wg[...]).astype(BF16) + dot_t(du1[...], wu[...]).astype(BF16)
    wide, scale, _ = norm(h1[...])
    d = da.astype(F32)
    through = d * scale - wide * (scale * scale * scale * (jnp.sum(d * wide, -1, keepdims=True) / D))
    dh = dy[...] + through.astype(BF16)
    dht[...] = dh.T
    dact = dot_t(dh, wd[...]).astype(BF16)
    dgate[...], dup[...] = gated_back(gate[...], up[...], dact)


def rows(cols):
    return pl.BlockSpec((TM, cols), lambda i: (i, 0))


SEQ = pl.BlockSpec((None, TM, D), lambda i: (0, i, 0))
COLUMNS = pl.BlockSpec((D, TM), lambda i: (0, i))


def weight(layer, shape):
    return pl.BlockSpec((None, *shape), lambda i: (layer, 0, 0), pipeline_mode=pl.Buffered(1))


def matrix(r, c, t=BF16):
    return jax.ShapeDtypeStruct((r, c), t)


def cost(matmuls):
    return pl.CostEstimate(flops=matmuls * 2 * TOKENS * D * FF, bytes_accessed=60 << 20, transcendentals=0)


def params():
    return pltpu.CompilerParams(vmem_limit_bytes=60 * 1024 * 1024)


def forward(x, wg, wu, wd):
    return pl.pallas_call(
        forward_kernel,
        grid=(TOKENS // TM,),
        in_specs=[SEQ, weight(0, (D, FF)), weight(0, (D, FF)), weight(0, (FF, D))],
        out_specs=[rows(D), COLUMNS, rows(FF), rows(FF), rows(FF)],
        out_shape=[matrix(TOKENS, D), matrix(D, TOKENS), matrix(TOKENS, FF), matrix(TOKENS, FF, F32), matrix(TOKENS, FF, F32)],
        compiler_params=params(),
        cost_estimate=cost(3),
        name="forward",
    )(x, wg, wu, wd)


def last(h1, dy, wg, wu, wd):
    return pl.pallas_call(
        last_kernel,
        grid=(TOKENS // TM,),
        in_specs=[rows(D), SEQ, weight(1, (D, FF)), weight(1, (D, FF)), weight(1, (FF, D))],
        out_specs=[COLUMNS, COLUMNS, rows(FF), rows(FF), rows(FF)],
        out_shape=[matrix(D, TOKENS)] * 2 + [matrix(TOKENS, FF)] * 3,
        compiler_params=params(),
        cost_estimate=cost(3),
        name="last",
    )(h1, dy, wg, wu, wd)


def between(dg1, du1, h1, dy, gate, up, wg, wu, wd):
    return pl.pallas_call(
        between_kernel,
        grid=(TOKENS // TM,),
        in_specs=[rows(FF), rows(FF), rows(D), SEQ, rows(FF), rows(FF)]
        + [weight(1, (D, FF)), weight(1, (D, FF)), weight(0, (FF, D))],
        out_specs=[COLUMNS, rows(FF), rows(FF)],
        out_shape=[matrix(D, TOKENS)] + [matrix(TOKENS, FF)] * 2,
        compiler_params=params(),
        cost_estimate=cost(3),
        name="between",
    )(dg1, du1, h1, dy, gate, up, wg, wu, wd)


def wide_kernel(at, dg, du, og, ou):
    og[...] = dot(at[...], dg[...]).astype(BF16)
    ou[...] = dot(at[...], du[...]).astype(BF16)


def tall_kernel(dt, act, o):
    o[...] = dot(dt[...], act[...]).astype(BF16).T


WHOLE_T = pl.BlockSpec((D, TOKENS), lambda i: (0, 0), pipeline_mode=pl.Buffered(1))
BY_COLUMN = pl.BlockSpec((TOKENS, NB), lambda i: (0, i))


def wide_gradients(at, dg, du):
    out = pl.BlockSpec((D, NB), lambda i: (0, i))
    return pl.pallas_call(
        wide_kernel,
        grid=(FF // NB,),
        in_specs=[WHOLE_T, BY_COLUMN, BY_COLUMN],
        out_specs=[out, out],
        out_shape=[matrix(D, FF)] * 2,
        compiler_params=params(),
        cost_estimate=cost(2),
        name="wide_gradients",
    )(at, dg, du)


def tall_gradient(dt, act):
    return pl.pallas_call(
        tall_kernel,
        grid=(FF // NB,),
        in_specs=[WHOLE_T, BY_COLUMN],
        out_specs=pl.BlockSpec((NB, D), lambda i: (i, 0)),
        out_shape=matrix(FF, D),
        compiler_params=params(),
        cost_estimate=cost(1),
        name="tall_gradient",
    )(dt, act)


def adamw(w, m, v, g):
    m = 0.9 * m + 0.1 * g
    v = 0.95 * v + 0.05 * g * g
    step = m * lax.rsqrt(v + 1e-8) + 0.1 * w
    return (w - 0.02 * step).astype(BF16), m, v


def solution(mesh):
    def step(x, dy, wg, wu, wd, *moments):
        h1, a0, act0, gate0, up0 = forward(x, wg, wu, wd)
        a1, dyt, act1, dg1, du1 = last(h1, dy, wg, wu, wd)
        gd1 = tall_gradient(dyt, act1)
        gg1, gu1 = wide_gradients(a1, dg1, du1)
        dht, dg0, du0 = between(dg1, du1, h1, dy, gate0, up0, wg, wu, wd)
        gd0 = tall_gradient(dht, act0)
        gg0, gu0 = wide_gradients(a0, dg0, du0)
        r1 = reduce_scatter((TALL, WIDE, WIDE), (gd1, gg1, gu1), ())
        d1, g1, u1 = r1[:3]
        d0, g0, u0, factor = reduce_scatter((TALL, WIDE, WIDE), (gd0, gg0, gu0), (d1, g1, u1))
        shards = [jnp.stack(pair).astype(F32) for pair in ((g0, g1), (u0, u1), (d0, d1))]
        me = lax.axis_index("dp")
        f = factor[0, 0]
        new = []
        for k, w in enumerate((wg, wu, wd)):
            r = w.shape[1] // DEVICES
            own = lax.dynamic_slice_in_dim(w, me * r, r, 1).astype(F32)
            new.append(adamw(own, moments[k], moments[3 + k], shards[k] * f))
        gathered = all_gather([n[0] for n in new])
        return (*gathered, *(n[1] for n in new), *(n[2] for n in new))

    seq = P(("rep", "dp"), None, None)
    whole = P(None, None, None)
    part = P(None, "dp", None)
    return jax.shard_map(
        step,
        mesh=mesh,
        in_specs=(seq, seq, whole, whole, whole) + (part,) * 6,
        out_specs=(P("rep", None, None),) * 3 + (P("rep", "dp", None),) * 6,
        check_vma=False,
    )
```

```python
import functools

import jax
import jax.numpy as jnp
from jax import lax
from jax.experimental import pallas as pl
from jax.experimental.pallas import tpu as pltpu
from jax.sharding import PartitionSpec as P

MESH = pl.DeviceIdType.MESH
F32, BF16 = jnp.float32, jnp.bfloat16
DEVICES, TOKENS, D, FF = 16, 2048, 896, 2560
COUNT = 2 * 3 * D * FF
TM = 256
NB = 512
STEPS = FF // NB
ANY = pl.BlockSpec(memory_space=pl.ANY)
WHOLE = pl.BlockSpec(memory_space=pltpu.VMEM)

STRIDE = (8, 4, 2)
ORDER = ((0, 1, 2), (1, 2, 0), (2, 0, 1))
WIDE = (56, 2560, tuple((slice(0, 56), s) for s in (slice(0, 896), slice(896, 1792), slice(1792, 2560))))
TALL = (160, 896, tuple((s, slice(0, 896)) for s in (slice(0, 56), slice(56, 112), slice(112, 160))))


def size(s):
    return s.stop - s.start


def place():
    me = lax.axis_index("dp")
    return me, (me // 8 % 2, me // 4 % 2, me // 2 % 2), me % 2


def beside(me, xyz, axis):
    return me + STRIDE[axis] * (1 - 2 * xyz[axis])


def partner(me, core):
    return me + 1 - 2 * core


def rs_scratch(kind, here):
    r, c, parts = kind
    flat = [pltpu.VMEM((8, 2, r, c) if here else (8, r, c), BF16), pltpu.VMEM((8, r, c), BF16)]
    for rows, cols in parts:
        flat += [pltpu.VMEM((7, size(rows), size(cols)), BF16)] * 2
    return flat + [pltpu.SemaphoreType.DMA((10,)), pltpu.SemaphoreType.DMA((10,)), pltpu.SemaphoreType.DMA(())]


RS_SCRATCH = 11


class Reduce:
    def __init__(self, kind, g, out, scratch):
        self.kind, self.out, self.here = kind, out, g is None
        self.own, self.other = scratch[:2]
        self.g = self.own if self.here else g
        self.send, self.got = scratch[2:8:2], scratch[3:8:2]
        self.ssem, self.rsem, self.lsem = scratch[8:]
        self.me, self.xyz, self.core = place()

    def swap(self):
        return pltpu.make_async_remote_copy(
            self.g.at[:, 1 - self.core],
            self.other,
            self.ssem.at[9],
            self.rsem.at[9],
            device_id={"dp": partner(self.me, self.core)},
            device_id_type=MESH,
        )

    def load(self):
        return pltpu.make_async_copy(self.g.at[:, self.core], self.own, self.lsem)

    def hop(self, t, phase):
        at = pl.ds((0, 4, 6)[phase], (4, 2, 1)[phase])
        return pltpu.make_async_remote_copy(
            self.send[t].at[at],
            self.got[t].at[at],
            self.ssem.at[3 * t + phase],
            self.rsem.at[3 * t + phase],
            device_id={"dp": beside(self.me, self.xyz, ORDER[t][phase])},
            device_id_type=MESH,
        )

    def total(self, t, at, got):
        rows, cols = self.kind[2][t]
        block = sum(p * (4, 2, 1)[axis] for p, axis in zip(at, ORDER[t], strict=True))
        own = self.own[block, self.core, rows, cols] if self.here else self.own[block, rows, cols]
        sum_ = own.astype(F32) + self.other[block, rows, cols].astype(F32)
        for i in got:
            sum_ = sum_ + self.got[t][i].astype(F32)
        return sum_

    def start(self):
        self.swap().start()
        if not self.here:
            self.load().start()

    def stage(self, n):
        if n == 0:
            if not self.here:
                self.load().wait()
            self.swap().wait_recv()
        for t in range(3):
            p1, p2, p3 = (self.xyz[axis] for axis in ORDER[t])
            if n:
                self.hop(t, n - 1).wait_recv()
            if n == 0:
                for j in range(2):
                    for k in range(2):
                        self.send[t][2 * j + k] = self.total(t, (1 - p1, j, k), ()).astype(BF16)
            elif n == 1:
                for k in range(2):
                    self.send[t][4 + k] = self.total(t, (p1, 1 - p2, k), (2 * (1 - p2) + k,)).astype(BF16)
            elif n == 2:
                self.send[t][6] = self.total(t, (p1, p2, 1 - p3), (2 * p2 + 1 - p3, 5 - p3)).astype(BF16)
            else:
                rows, cols = self.kind[2][t]
                self.out[rows, cols] = self.total(t, (p1, p2, p3), (2 * p2 + p3, 4 + p3, 6)).astype(BF16)
            if n < 3:
                self.hop(t, n).start()

    def finish(self):
        self.swap().wait_send()
        for t in range(3):
            for phase in range(3):
                self.hop(t, phase).wait_send()


def squares(g):
    wide = g.astype(F32)
    rows, cols = wide.shape
    s = jnp.sum((wide * wide).reshape(rows // 8, 8, cols), 0)
    return sum(s[:, i : i + 128] for i in range(0, cols, 128))


def clip_factor(shards, factor, squared, sums, ssem, rsem):
    me = lax.axis_index("dp")
    squared[...] = sum(squares(g[...]) for g in shards)

    def give(k, slot):
        to = (me + k) % DEVICES
        return pltpu.make_async_remote_copy(
            squared, sums.at[slot], ssem.at[k], rsem.at[slot], device_id={"dp": to}, device_id_type=MESH
        )

    for k in range(1, DEVICES):
        give(k, me).start()
    sums[me] = squared[...]
    for k in range(1, DEVICES):
        give(k, (me + k) % DEVICES).wait_recv()
    for k in range(1, DEVICES):
        give(k, me).wait_send()
    total = jnp.sum(jnp.sum(jnp.sum(sums[...], 0), 0, keepdims=True), 1, keepdims=True)
    f = jnp.minimum(1.0, 0.5 * lax.rsqrt(total / COUNT + 1e-30))
    factor[...] = jnp.broadcast_to(f, factor.shape)


CLIP_SCRATCH = [
    pltpu.VMEM((8, 128), F32),
    pltpu.VMEM((DEVICES, 8, 128), F32),
    pltpu.SemaphoreType.DMA((DEVICES,)),
    pltpu.SemaphoreType.DMA((DEVICES,)),
]


def at_end_of(step, plan):
    for when, entries in plan.items():

        @pl.when(step == when)
        def _(entries=entries):
            for unit, stage in entries:
                if stage == "start":
                    unit.start()
                elif stage == "finish":
                    unit.finish()
                else:
                    unit.stage(stage)


class Gather:
    def __init__(self, kind, own, out, layer, ssem, rsem, csem):
        self.kind, self.own, self.out, self.layer = kind, own, out, layer
        self.ssem, self.rsem, self.csem = ssem, rsem, csem
        self.me, self.xyz, self.core = place()

    def local(self):
        x, y, z = self.xyz
        return pltpu.make_async_copy(self.own, self.out.at[self.layer, x, y, z, self.core], self.csem)

    def blocks(self, t, core, known, other=None):
        rows, cols = self.kind[2][t]
        index = []
        for axis in range(3):
            p = self.xyz[axis]
            index.append(slice(None) if axis in known else (1 - p if axis == other else p))
        return self.out.at[(self.layer, *index, core, rows, cols)]

    def hop(self, t, phase, arriving=False):
        axis = ORDER[t][phase]
        known = ORDER[t][:phase]
        src = self.blocks(t, self.core, known)
        dst = self.blocks(t, self.core, known, axis) if arriving else src
        if phase == 0 and not arriving:
            src = self.own.at[self.kind[2][t]]
        return pltpu.make_async_remote_copy(
            src,
            dst,
            self.ssem.at[3 * t + phase],
            self.rsem.at[3 * t + phase],
            device_id={"dp": beside(self.me, self.xyz, axis)},
            device_id_type=MESH,
        )

    def share(self, t, phase, core):
        ref = self.blocks(t, core, ORDER[t][:phase], ORDER[t][phase])
        return pltpu.make_async_remote_copy(
            ref,
            ref,
            self.ssem.at[10 + 3 * t + phase],
            self.rsem.at[10 + 3 * t + phase],
            device_id={"dp": partner(self.me, self.core)},
            device_id_type=MESH,
        )

    def share_own(self, core):
        x, y, z = self.xyz
        return pltpu.make_async_remote_copy(
            self.own,
            self.out.at[self.layer, x, y, z, core],
            self.ssem.at[9],
            self.rsem.at[9],
            device_id={"dp": partner(self.me, self.core)},
            device_id_type=MESH,
        )

    def start(self):
        self.local().start()
        for t in range(3):
            self.hop(t, 0).start()
        self.share_own(self.core).start()

    def stage(self, phase):
        if phase == 0:
            self.local().wait()
        for t in range(3):
            self.hop(t, phase, True).wait_recv()
            if phase < 2:
                self.hop(t, phase + 1).start()
            self.share(t, phase, self.core).start()

    def finish(self):
        self.share_own(1 - self.core).wait_recv()
        self.share_own(self.core).wait_send()
        for t in range(3):
            for phase in range(3):
                self.share(t, phase, 1 - self.core).wait_recv()
                self.share(t, phase, self.core).wait_send()
                self.hop(t, phase).wait_send()


def gather_kernel(*refs):
    owns, outs, (ssem, rsem, csem) = refs[:3], refs[3:6], refs[6:]
    units = []
    for layer in range(2):
        for i, kind in enumerate((WIDE, WIDE, TALL)):
            u = 3 * layer + i
            units.append(Gather(kind, owns[i].at[layer], outs[i], layer, ssem.at[u], rsem.at[u], csem.at[u]))
    for u in units:
        u.start()
    for phase in range(3):
        for u in units:
            u.stage(phase)
    for u in units:
        u.finish()


def all_gather(owns):
    outs = pl.pallas_call(
        gather_kernel,
        out_shape=[jax.ShapeDtypeStruct((2, 2, 2, 2, 2, *o.shape[1:]), BF16) for o in owns],
        in_specs=[WHOLE] * 3,
        out_specs=[ANY] * 3,
        scratch_shapes=[
            pltpu.SemaphoreType.DMA((6, 19)),
            pltpu.SemaphoreType.DMA((6, 19)),
            pltpu.SemaphoreType.DMA((6,)),
        ],
        compiler_params=pltpu.CompilerParams(has_side_effects=True),
        name="all_gather",
    )(*owns)
    return [o.reshape(2, DEVICES * o.shape[-2], o.shape[-1]) for o in outs]


def dot(a, b):
    return jnp.dot(a, b, preferred_element_type=F32)


def dot_t(a, b):
    return lax.dot_general(a, b, (((1,), (1,)), ((), ())), preferred_element_type=F32)


def norm(h):
    wide = h.astype(F32)
    scale = lax.rsqrt(jnp.mean(wide * wide, -1, keepdims=True) + 1e-6)
    return wide, scale, (wide * scale).astype(BF16)


def gated_back(gate, up, dact):
    sig = jax.nn.sigmoid(gate)
    d = dact.astype(F32)
    dup = d * (gate * sig)
    dgate = d * up * (sig * (1 + gate * (1 - sig)))
    return dgate.astype(BF16), dup.astype(BF16)


def forward_kernel(x, wg, wu, wd, h1, at, act, gate, up):
    h = x[...]
    _, _, a = norm(h)
    at[...] = a.T
    g = dot(a, wg[...])
    u = dot(a, wu[...])
    gate[...] = g
    up[...] = u
    s = (g * jax.nn.sigmoid(g) * u).astype(BF16)
    act[...] = s
    h1[...] = h + dot(s, wd[...]).astype(BF16)


def last_kernel(h1, dy, wg, wu, wd, at, dyt, act, dgate, dup):
    _, _, a = norm(h1[...])
    at[...] = a.T
    dyt[...] = dy[...].T
    g = dot(a, wg[...])
    u = dot(a, wu[...])
    act[...] = (g * jax.nn.sigmoid(g) * u).astype(BF16)
    dact = dot_t(dy[...], wd[...]).astype(BF16)
    dgate[...], dup[...] = gated_back(g, u, dact)


def between_kernel(dg1, du1, h1, dy, gate, up, wg, wu, wd, gg, gu, dht, dgate, dup, og, ou, *scratch):
    step = pl.program_id(0)
    units = [Reduce(WIDE, gg, og, scratch[:RS_SCRATCH]), Reduce(WIDE, gu, ou, scratch[RS_SCRATCH:])]

    @pl.when(step == 0)
    def _():
        for u in units:
            u.start()

    da = dot_t(dg1[...], wg[...]).astype(BF16) + dot_t(du1[...], wu[...]).astype(BF16)
    wide, scale, _ = norm(h1[...])
    d = da.astype(F32)
    through = d * scale - wide * (scale * scale * scale * (jnp.sum(d * wide, -1, keepdims=True) / D))
    dh = dy[...] + through.astype(BF16)
    dht[...] = dh.T
    dact = dot_t(dh, wd[...]).astype(BF16)
    dgate[...], dup[...] = gated_back(gate[...], up[...], dact)
    plan = {when: [(u, stage) for u in units] for when, stage in ((1, 0), (4, 1), (6, 2))}
    plan[7] = [(u, stage) for stage in (3, "finish") for u in units]
    at_end_of(step, plan)


def rows(cols):
    return pl.BlockSpec((TM, cols), lambda i: (i, 0))


SEQ = pl.BlockSpec((None, TM, D), lambda i: (0, i, 0))
COLUMNS = pl.BlockSpec((D, TM), lambda i: (0, i))


def weight(layer, shape):
    return pl.BlockSpec((None, *shape), lambda i: (layer, 0, 0), pipeline_mode=pl.Buffered(1))


def matrix(r, c, t=BF16):
    return jax.ShapeDtypeStruct((r, c), t)


def cost(matmuls):
    return pl.CostEstimate(flops=matmuls * 2 * TOKENS * D * FF, bytes_accessed=60 << 20, transcendentals=0)


def params(remote=False):
    return pltpu.CompilerParams(vmem_limit_bytes=60 * 1024 * 1024, has_side_effects=remote)


def forward(x, wg, wu, wd):
    return pl.pallas_call(
        forward_kernel,
        grid=(TOKENS // TM,),
        in_specs=[SEQ, weight(0, (D, FF)), weight(0, (D, FF)), weight(0, (FF, D))],
        out_specs=[rows(D), COLUMNS, rows(FF), rows(FF), rows(FF)],
        out_shape=[matrix(TOKENS, D), matrix(D, TOKENS), matrix(TOKENS, FF), matrix(TOKENS, FF, F32), matrix(TOKENS, FF, F32)],
        compiler_params=params(),
        cost_estimate=cost(3),
        name="forward",
    )(x, wg, wu, wd)


def last(h1, dy, wg, wu, wd):
    return pl.pallas_call(
        last_kernel,
        grid=(TOKENS // TM,),
        in_specs=[rows(D), SEQ, weight(1, (D, FF)), weight(1, (D, FF)), weight(1, (FF, D))],
        out_specs=[COLUMNS, COLUMNS, rows(FF), rows(FF), rows(FF)],
        out_shape=[matrix(D, TOKENS)] * 2 + [matrix(TOKENS, FF)] * 3,
        compiler_params=params(),
        cost_estimate=cost(3),
        name="last",
    )(h1, dy, wg, wu, wd)


def shard(kind):
    return pl.BlockSpec(kind[:2], lambda i: (0, 0))


def between(dg1, du1, h1, dy, gate, up, wg, wu, wd, gg, gu):
    return pl.pallas_call(
        between_kernel,
        grid=(TOKENS // TM,),
        in_specs=[rows(FF), rows(FF), rows(D), SEQ, rows(FF), rows(FF)]
        + [weight(1, (D, FF)), weight(1, (D, FF)), weight(0, (FF, D)), ANY, ANY],
        out_specs=[COLUMNS, rows(FF), rows(FF), shard(WIDE), shard(WIDE)],
        out_shape=[matrix(D, TOKENS)] + [matrix(TOKENS, FF)] * 2 + [matrix(*WIDE[:2])] * 2,
        scratch_shapes=rs_scratch(WIDE, False) * 2,
        compiler_params=params(True),
        cost_estimate=cost(3),
        name="between",
    )(dg1, du1, h1, dy, gate, up, wg, wu, wd, gg, gu)


def tall_into(g, i, dt, act):
    g.reshape(FF, D)[pl.ds(pl.multiple_of(i * NB, NB), NB)] = dot(dt[...], act[...]).astype(BF16).T


def wide_block(at, dg):
    return dot(at[...], dg[...]).reshape(8, 2, 56, NB).astype(BF16)


def upper_kernel(dt, at, act, dg, du, gg, gu, od, *scratch):
    step = pl.program_id(0)
    d = Reduce(TALL, None, od, scratch)

    @pl.when(step < STEPS)
    def _():
        tall_into(d.g, step, dt, act)

    @pl.when((step >= STEPS) & (step < 2 * STEPS))
    def _():
        gg[...] = wide_block(at, dg)

    @pl.when(step >= 2 * STEPS)
    def _():
        gu[...] = wide_block(at, du)

    at_end_of(step, {4: [(d, "start")], 6: [(d, 0)], 11: [(d, 1)], 13: [(d, 2)], 14: [(d, 3), (d, "finish")]})


def lower_kernel(dt, at, act, dg, du, d1, g1, u1, od, og, ou, factor, *scratch):
    step = pl.program_id(0)
    d, g, u = (
        Reduce(kind, None, o, scratch[RS_SCRATCH * i : RS_SCRATCH * (i + 1)])
        for i, (kind, o) in enumerate(((TALL, od), (WIDE, og), (WIDE, ou)))
    )

    @pl.when(step < STEPS)
    def _():
        tall_into(d.g, step, dt, act)

    def columns(first):
        return pl.ds(pl.multiple_of((step - first) * NB, NB), NB)

    @pl.when((step >= STEPS) & (step < 2 * STEPS))
    def _():
        g.g[:, :, :, columns(STEPS)] = wide_block(at, dg)

    @pl.when(step >= 2 * STEPS)
    def _():
        u.g[:, :, :, columns(2 * STEPS)] = wide_block(at, du)

    tail = [(u, "start"), (d, 3), (g, 1), (u, 0), (g, 2), (u, 1), (g, 3), (u, 2), (u, 3)]
    at_end_of(
        step,
        {4: [(d, "start")], 6: [(d, 0)], 9: [(g, "start")], 11: [(d, 1), (g, 0)], 13: [(d, 2)]}
        | {14: tail + [(unit, "finish") for unit in (d, g, u)]},
    )

    @pl.when(step == 3 * STEPS - 1)
    def _():
        clip_factor([d1, g1, u1, od, og, ou], factor, *scratch[3 * RS_SCRATCH :])


WHOLE_T = pl.BlockSpec((D, TOKENS), lambda i: (0, 0), pipeline_mode=pl.Buffered(1))


def in_turn(turn, block, index):
    return pl.BlockSpec(block, lambda i: index(jnp.clip(i - turn * STEPS, 0, STEPS - 1)))


COLUMNS_IN_TURN = [in_turn(turn, (TOKENS, NB), lambda i: (0, i)) for turn in range(3)]


def upper_gradients(dt, at, act, dg, du):
    return pl.pallas_call(
        upper_kernel,
        grid=(3 * STEPS,),
        in_specs=[WHOLE_T, WHOLE_T, *COLUMNS_IN_TURN],
        out_specs=[in_turn(turn, (8, 2, 56, NB), lambda i: (0, 0, 0, i)) for turn in (1, 2)] + [shard(TALL)],
        out_shape=[jax.ShapeDtypeStruct((8, 2, 56, FF), BF16)] * 2 + [matrix(*TALL[:2])],
        scratch_shapes=rs_scratch(TALL, True),
        compiler_params=params(True),
        cost_estimate=cost(3),
        name="upper_gradients",
    )(dt, at, act, dg, du)


def lower_gradients(dt, at, act, dg, du, before):
    kinds = (TALL, WIDE, WIDE)
    return pl.pallas_call(
        lower_kernel,
        grid=(3 * STEPS,),
        in_specs=[WHOLE_T, WHOLE_T, *COLUMNS_IN_TURN] + [shard(k) for k in kinds],
        out_specs=[shard(k) for k in kinds] + [pl.BlockSpec((8, 128), lambda i: (0, 0))],
        out_shape=[matrix(*k[:2]) for k in kinds] + [matrix(8, 128, F32)],
        scratch_shapes=sum((rs_scratch(k, True) for k in kinds), []) + CLIP_SCRATCH,
        compiler_params=params(True),
        cost_estimate=cost(3),
        name="lower_gradients",
    )(dt, at, act, dg, du, *before)


def adamw(w, m, v, g):
    m = 0.9 * m + 0.1 * g
    v = 0.95 * v + 0.05 * g * g
    step = m * lax.rsqrt(v + 1e-8) + 0.1 * w
    return (w - 0.02 * step).astype(BF16), m, v


def solution(mesh):
    def step(x, dy, wg, wu, wd, *moments):
        h1, a0, act0, gate0, up0 = forward(x, wg, wu, wd)
        a1, dyt, act1, dg1, du1 = last(h1, dy, wg, wu, wd)
        gg1, gu1, d1 = upper_gradients(dyt, a1, act1, dg1, du1)
        dht, dg0, du0, g1, u1 = between(dg1, du1, h1, dy, gate0, up0, wg, wu, wd, gg1, gu1)
        d0, g0, u0, factor = lower_gradients(dht, a0, act0, dg0, du0, (d1, g1, u1))
        shards = [jnp.stack(pair).astype(F32) for pair in ((g0, g1), (u0, u1), (d0, d1))]
        me = lax.axis_index("dp")
        f = factor[0, 0]
        new = []
        for k, w in enumerate((wg, wu, wd)):
            r = w.shape[1] // DEVICES
            own = lax.dynamic_slice_in_dim(w, me * r, r, 1).astype(F32)
            new.append(adamw(own, moments[k], moments[3 + k], shards[k] * f))
        gathered = all_gather([n[0] for n in new])
        return (*gathered, *(n[1] for n in new), *(n[2] for n in new))

    seq = P(("rep", "dp"), None, None)
    whole = P(None, None, None)
    part = P(None, "dp", None)
    return jax.shard_map(
        step,
        mesh=mesh,
        in_specs=(seq, seq, whole, whole, whole) + (part,) * 6,
        out_specs=(P("rep", None, None),) * 3 + (P("rep", "dp", None),) * 6,
        check_vma=False,
    )
```

```python
import functools

import jax
import jax.numpy as jnp
from jax import lax
from jax.experimental import pallas as pl
from jax.experimental.pallas import tpu as pltpu
from jax.sharding import PartitionSpec as P

MESH = pl.DeviceIdType.MESH
F32, BF16 = jnp.float32, jnp.bfloat16
DEVICES, TOKENS, D, FF = 16, 2048, 896, 2560
COUNT = 2 * 3 * D * FF
TM = 256
NB = 512
STEPS = FF // NB
ANY = pl.BlockSpec(memory_space=pl.ANY)
WHOLE = pl.BlockSpec(memory_space=pltpu.VMEM)

STRIDE = (8, 4, 2)
ORDER = ((0, 1, 2), (1, 2, 0), (2, 0, 1))
WIDE = (56, 2560, tuple((slice(0, 56), s) for s in (slice(0, 896), slice(896, 1792), slice(1792, 2560))))
TALL = (160, 896, tuple((s, slice(0, 896)) for s in (slice(0, 56), slice(56, 112), slice(112, 160))))


def size(s):
    return s.stop - s.start


def place():
    me = lax.axis_index("dp")
    return me, (me // 8 % 2, me // 4 % 2, me // 2 % 2), me % 2


def beside(me, xyz, axis):
    return me + STRIDE[axis] * (1 - 2 * xyz[axis])


def partner(me, core):
    return me + 1 - 2 * core


def rs_scratch(kind, here):
    r, c, parts = kind
    flat = [pltpu.VMEM((8, 2, r, c) if here else (8, r, c), BF16), pltpu.VMEM((8, r, c), BF16)]
    for rows, cols in parts:
        flat += [pltpu.VMEM((7, size(rows), size(cols)), BF16)] * 2
    return flat + [pltpu.SemaphoreType.DMA((10,)), pltpu.SemaphoreType.DMA((10,)), pltpu.SemaphoreType.DMA(())]


RS_SCRATCH = 11


class Reduce:
    def __init__(self, kind, g, out, scratch):
        self.kind, self.out, self.here = kind, out, g is None
        self.own, self.other = scratch[:2]
        self.g = self.own if self.here else g
        self.send, self.got = scratch[2:8:2], scratch[3:8:2]
        self.ssem, self.rsem, self.lsem = scratch[8:]
        self.me, self.xyz, self.core = place()

    def swap(self):
        return pltpu.make_async_remote_copy(
            self.g.at[:, 1 - self.core],
            self.other,
            self.ssem.at[9],
            self.rsem.at[9],
            device_id={"dp": partner(self.me, self.core)},
            device_id_type=MESH,
        )

    def load(self):
        return pltpu.make_async_copy(self.g.at[:, self.core], self.own, self.lsem)

    def hop(self, t, phase):
        at = pl.ds((0, 4, 6)[phase], (4, 2, 1)[phase])
        return pltpu.make_async_remote_copy(
            self.send[t].at[at],
            self.got[t].at[at],
            self.ssem.at[3 * t + phase],
            self.rsem.at[3 * t + phase],
            device_id={"dp": beside(self.me, self.xyz, ORDER[t][phase])},
            device_id_type=MESH,
        )

    def total(self, t, at, got):
        rows, cols = self.kind[2][t]
        block = sum(p * (4, 2, 1)[axis] for p, axis in zip(at, ORDER[t], strict=True))
        own = self.own[block, self.core, rows, cols] if self.here else self.own[block, rows, cols]
        sum_ = own.astype(F32) + self.other[block, rows, cols].astype(F32)
        for i in got:
            sum_ = sum_ + self.got[t][i].astype(F32)
        return sum_

    def start(self):
        self.swap().start()
        if not self.here:
            self.load().start()

    def stage(self, n):
        if n == 0:
            if not self.here:
                self.load().wait()
            self.swap().wait_recv()
        for t in range(3):
            p1, p2, p3 = (self.xyz[axis] for axis in ORDER[t])
            if n:
                self.hop(t, n - 1).wait_recv()
            if n == 0:
                for j in range(2):
                    for k in range(2):
                        self.send[t][2 * j + k] = self.total(t, (1 - p1, j, k), ()).astype(BF16)
            elif n == 1:
                for k in range(2):
                    self.send[t][4 + k] = self.total(t, (p1, 1 - p2, k), (2 * (1 - p2) + k,)).astype(BF16)
            elif n == 2:
                self.send[t][6] = self.total(t, (p1, p2, 1 - p3), (2 * p2 + 1 - p3, 5 - p3)).astype(BF16)
            else:
                rows, cols = self.kind[2][t]
                self.out[rows, cols] = self.total(t, (p1, p2, p3), (2 * p2 + p3, 4 + p3, 6)).astype(BF16)
            if n < 3:
                self.hop(t, n).start()

    def finish(self):
        self.swap().wait_send()
        for t in range(3):
            for phase in range(3):
                self.hop(t, phase).wait_send()


def squares(g):
    wide = g.astype(F32)
    rows, cols = wide.shape
    s = jnp.sum((wide * wide).reshape(rows // 8, 8, cols), 0)
    return sum(s[:, i : i + 128] for i in range(0, cols, 128))


def clip_factor(shards, factor, squared, sums, ssem, rsem):
    me = lax.axis_index("dp")
    squared[...] = sum(squares(g[...]) for g in shards)

    def give(k, slot):
        to = (me + k) % DEVICES
        return pltpu.make_async_remote_copy(
            squared, sums.at[slot], ssem.at[k], rsem.at[slot], device_id={"dp": to}, device_id_type=MESH
        )

    for k in range(1, DEVICES):
        give(k, me).start()
    sums[me] = squared[...]
    for k in range(1, DEVICES):
        give(k, (me + k) % DEVICES).wait_recv()
    for k in range(1, DEVICES):
        give(k, me).wait_send()
    total = jnp.sum(jnp.sum(jnp.sum(sums[...], 0), 0, keepdims=True), 1, keepdims=True)
    f = jnp.minimum(1.0, 0.5 * lax.rsqrt(total / COUNT + 1e-30))
    factor[...] = jnp.broadcast_to(f, factor.shape)


CLIP_SCRATCH = [
    pltpu.VMEM((8, 128), F32),
    pltpu.VMEM((DEVICES, 8, 128), F32),
    pltpu.SemaphoreType.DMA((DEVICES,)),
    pltpu.SemaphoreType.DMA((DEVICES,)),
]


def at_end_of(step, plan):
    for when, entries in plan.items():

        @pl.when(step == when)
        def _(entries=entries):
            for unit, stage in entries:
                if stage == "start":
                    unit.start()
                elif stage == "finish":
                    unit.finish()
                else:
                    unit.stage(stage)


class Gather:
    def __init__(self, kind, own, out, layer, ssem, rsem, csem):
        self.kind, self.own, self.out, self.layer = kind, own, out, layer
        self.ssem, self.rsem, self.csem = ssem, rsem, csem
        self.me, self.xyz, self.core = place()

    def local(self):
        x, y, z = self.xyz
        return pltpu.make_async_copy(self.own, self.out.at[self.layer, x, y, z, self.core], self.csem)

    def blocks(self, t, core, known, other=None):
        rows, cols = self.kind[2][t]
        index = []
        for axis in range(3):
            p = self.xyz[axis]
            index.append(slice(None) if axis in known else (1 - p if axis == other else p))
        return self.out.at[(self.layer, *index, core, rows, cols)]

    def hop(self, t, phase, arriving=False):
        axis = ORDER[t][phase]
        known = ORDER[t][:phase]
        src = self.blocks(t, self.core, known)
        dst = self.blocks(t, self.core, known, axis) if arriving else src
        if phase == 0 and not arriving:
            src = self.own.at[self.kind[2][t]]
        return pltpu.make_async_remote_copy(
            src,
            dst,
            self.ssem.at[3 * t + phase],
            self.rsem.at[3 * t + phase],
            device_id={"dp": beside(self.me, self.xyz, axis)},
            device_id_type=MESH,
        )

    def share(self, t, phase, core):
        ref = self.blocks(t, core, ORDER[t][:phase], ORDER[t][phase])
        return pltpu.make_async_remote_copy(
            ref,
            ref,
            self.ssem.at[10 + 3 * t + phase],
            self.rsem.at[10 + 3 * t + phase],
            device_id={"dp": partner(self.me, self.core)},
            device_id_type=MESH,
        )

    def share_own(self, core):
        x, y, z = self.xyz
        return pltpu.make_async_remote_copy(
            self.own,
            self.out.at[self.layer, x, y, z, core],
            self.ssem.at[9],
            self.rsem.at[9],
            device_id={"dp": partner(self.me, self.core)},
            device_id_type=MESH,
        )

    def start(self):
        self.local().start()
        for t in range(3):
            self.hop(t, 0).start()
        self.share_own(self.core).start()

    def stage(self, phase):
        if phase == 0:
            self.local().wait()
        for t in range(3):
            self.hop(t, phase, True).wait_recv()
            if phase < 2:
                self.hop(t, phase + 1).start()
            self.share(t, phase, self.core).start()

    def finish(self):
        self.share_own(1 - self.core).wait_recv()
        self.share_own(self.core).wait_send()
        for t in range(3):
            for phase in range(3):
                self.share(t, phase, 1 - self.core).wait_recv()
                self.share(t, phase, self.core).wait_send()
                self.hop(t, phase).wait_send()


def gather_kernel(*refs):
    owns, outs, (ssem, rsem, csem) = refs[:3], refs[3:6], refs[6:]
    units = []
    for layer in range(2):
        for i, kind in enumerate((WIDE, WIDE, TALL)):
            u = 3 * layer + i
            units.append(Gather(kind, owns[i].at[layer], outs[i], layer, ssem.at[u], rsem.at[u], csem.at[u]))
    for u in units:
        u.start()
    for phase in range(3):
        for u in units:
            u.stage(phase)
    for u in units:
        u.finish()


def all_gather(owns):
    outs = pl.pallas_call(
        gather_kernel,
        out_shape=[pltpu.VMEM((2, 2, 2, 2, 2, *o.shape[1:]), BF16) for o in owns],
        in_specs=[WHOLE] * 3,
        out_specs=[WHOLE] * 3,
        scratch_shapes=[
            pltpu.SemaphoreType.DMA((6, 19)),
            pltpu.SemaphoreType.DMA((6, 19)),
            pltpu.SemaphoreType.DMA((6,)),
        ],
        compiler_params=pltpu.CompilerParams(has_side_effects=True, vmem_limit_bytes=8 << 20),
        name="all_gather",
    )(*owns)
    outs = pl.pallas_call(
        flush_kernel,
        out_shape=[jax.ShapeDtypeStruct(o.shape, BF16) for o in outs],
        in_specs=[WHOLE] * 3,
        out_specs=[ANY] * 3,
        scratch_shapes=[pltpu.SemaphoreType.DMA((6,))],
        compiler_params=pltpu.CompilerParams(vmem_limit_bytes=1 << 20),
        name="flush",
    )(*outs)
    return [o.reshape(2, DEVICES * o.shape[-2], o.shape[-1]) for o in outs]


def flush_kernel(*refs):
    copies = []
    for i in range(3):
        for layer in range(2):
            copies.append(pltpu.make_async_copy(refs[i].at[layer], refs[3 + i].at[layer], refs[6].at[2 * i + layer]))
    for c in copies:
        c.start()
    for c in copies:
        c.wait()


def dot(a, b):
    return jnp.dot(a, b, preferred_element_type=F32)


def dot_t(a, b):
    return lax.dot_general(a, b, (((1,), (1,)), ((), ())), preferred_element_type=F32)


def norm(h):
    wide = h.astype(F32)
    scale = lax.rsqrt(jnp.mean(wide * wide, -1, keepdims=True) + 1e-6)
    return wide, scale, (wide * scale).astype(BF16)


def gated_back(gate, up, dact):
    sig = jax.nn.sigmoid(gate)
    d = dact.astype(F32)
    dup = d * (gate * sig)
    dgate = d * up * (sig * (1 + gate * (1 - sig)))
    return dgate.astype(BF16), dup.astype(BF16)


def forward_kernel(x, wg, wu, wd, h1, at, act, gate, up):
    h = x[...]
    _, _, a = norm(h)
    at[...] = a.T
    g = dot(a, wg[...])
    u = dot(a, wu[...])
    gate[...] = g
    up[...] = u
    s = (g * jax.nn.sigmoid(g) * u).astype(BF16)
    act[...] = s
    h1[...] = h + dot(s, wd[...]).astype(BF16)


def last_kernel(h1, dy, wg, wu, wd, at, dyt, act, dgate, dup):
    _, _, a = norm(h1[...])
    at[...] = a.T
    dyt[...] = dy[...].T
    g = dot(a, wg[...])
    u = dot(a, wu[...])
    act[...] = (g * jax.nn.sigmoid(g) * u).astype(BF16)
    dact = dot_t(dy[...], wd[...]).astype(BF16)
    dgate[...], dup[...] = gated_back(g, u, dact)


def between_kernel(dg1, du1, h1, dy, gate, up, wg, wu, wd, gg, gu, dht, dgate, dup, og, ou, *scratch):
    step = pl.program_id(0)
    units = [Reduce(WIDE, gg, og, scratch[:RS_SCRATCH]), Reduce(WIDE, gu, ou, scratch[RS_SCRATCH:])]

    @pl.when(step == 0)
    def _():
        for u in units:
            u.start()

    da = dot_t(dg1[...], wg[...]).astype(BF16) + dot_t(du1[...], wu[...]).astype(BF16)
    wide, scale, _ = norm(h1[...])
    d = da.astype(F32)
    through = d * scale - wide * (scale * scale * scale * (jnp.sum(d * wide, -1, keepdims=True) / D))
    dh = dy[...] + through.astype(BF16)
    dht[...] = dh.T
    dact = dot_t(dh, wd[...]).astype(BF16)
    dgate[...], dup[...] = gated_back(gate[...], up[...], dact)
    plan = {when: [(u, stage) for u in units] for when, stage in ((1, 0), (4, 1), (6, 2))}
    plan[7] = [(u, stage) for stage in (3, "finish") for u in units]
    at_end_of(step, plan)


def rows(cols):
    return pl.BlockSpec((TM, cols), lambda i: (i, 0))


SEQ = pl.BlockSpec((None, TM, D), lambda i: (0, i, 0))
COLUMNS = pl.BlockSpec((D, TM), lambda i: (0, i))


def weight(layer, shape):
    return pl.BlockSpec((None, *shape), lambda i: (layer, 0, 0), pipeline_mode=pl.Buffered(1))


def matrix(r, c, t=BF16):
    return jax.ShapeDtypeStruct((r, c), t)


def cost(matmuls):
    return pl.CostEstimate(flops=matmuls * 2 * TOKENS * D * FF, bytes_accessed=60 << 20, transcendentals=0)


def params(remote=False):
    return pltpu.CompilerParams(vmem_limit_bytes=60 * 1024 * 1024, has_side_effects=remote)


def forward(x, wg, wu, wd):
    return pl.pallas_call(
        forward_kernel,
        grid=(TOKENS // TM,),
        in_specs=[SEQ, weight(0, (D, FF)), weight(0, (D, FF)), weight(0, (FF, D))],
        out_specs=[rows(D), COLUMNS, rows(FF), rows(FF), rows(FF)],
        out_shape=[matrix(TOKENS, D), matrix(D, TOKENS), matrix(TOKENS, FF), matrix(TOKENS, FF, F32), matrix(TOKENS, FF, F32)],
        compiler_params=params(),
        cost_estimate=cost(3),
        name="forward",
    )(x, wg, wu, wd)


def last(h1, dy, wg, wu, wd):
    return pl.pallas_call(
        last_kernel,
        grid=(TOKENS // TM,),
        in_specs=[rows(D), SEQ, weight(1, (D, FF)), weight(1, (D, FF)), weight(1, (FF, D))],
        out_specs=[COLUMNS, COLUMNS, rows(FF), rows(FF), rows(FF)],
        out_shape=[matrix(D, TOKENS)] * 2 + [matrix(TOKENS, FF)] * 3,
        compiler_params=params(),
        cost_estimate=cost(3),
        name="last",
    )(h1, dy, wg, wu, wd)


def shard(kind):
    return pl.BlockSpec(kind[:2], lambda i: (0, 0))


def between(dg1, du1, h1, dy, gate, up, wg, wu, wd, gg, gu):
    return pl.pallas_call(
        between_kernel,
        grid=(TOKENS // TM,),
        in_specs=[rows(FF), rows(FF), rows(D), SEQ, rows(FF), rows(FF)]
        + [weight(1, (D, FF)), weight(1, (D, FF)), weight(0, (FF, D)), ANY, ANY],
        out_specs=[COLUMNS, rows(FF), rows(FF), shard(WIDE), shard(WIDE)],
        out_shape=[matrix(D, TOKENS)] + [matrix(TOKENS, FF)] * 2 + [matrix(*WIDE[:2])] * 2,
        scratch_shapes=rs_scratch(WIDE, False) * 2,
        compiler_params=params(True),
        cost_estimate=cost(3),
        name="between",
    )(dg1, du1, h1, dy, gate, up, wg, wu, wd, gg, gu)


def tall_into(g, i, dt, act):
    g.reshape(FF, D)[pl.ds(pl.multiple_of(i * NB, NB), NB)] = dot(dt[...], act[...]).astype(BF16).T


def wide_block(at, dg):
    return dot(at[...], dg[...]).reshape(8, 2, 56, NB).astype(BF16)


def upper_kernel(dt, at, act, dg, du, gg, gu, od, *scratch):
    step = pl.program_id(0)
    d = Reduce(TALL, None, od, scratch)

    @pl.when(step < STEPS)
    def _():
        tall_into(d.g, step, dt, act)

    @pl.when((step >= STEPS) & (step < 2 * STEPS))
    def _():
        gg[...] = wide_block(at, dg)

    @pl.when(step >= 2 * STEPS)
    def _():
        gu[...] = wide_block(at, du)

    at_end_of(step, {4: [(d, "start")], 6: [(d, 0)], 11: [(d, 1)], 13: [(d, 2)], 14: [(d, 3), (d, "finish")]})


def lower_kernel(dt, at, act, dg, du, d1, g1, u1, od, og, ou, factor, *scratch):
    step = pl.program_id(0)
    d, g, u = (
        Reduce(kind, None, o, scratch[RS_SCRATCH * i : RS_SCRATCH * (i + 1)])
        for i, (kind, o) in enumerate(((TALL, od), (WIDE, og), (WIDE, ou)))
    )

    @pl.when(step < STEPS)
    def _():
        tall_into(d.g, step, dt, act)

    def columns(first):
        return pl.ds(pl.multiple_of((step - first) * NB, NB), NB)

    @pl.when((step >= STEPS) & (step < 2 * STEPS))
    def _():
        g.g[:, :, :, columns(STEPS)] = wide_block(at, dg)

    @pl.when(step >= 2 * STEPS)
    def _():
        u.g[:, :, :, columns(2 * STEPS)] = wide_block(at, du)

    tail = [(u, "start"), (d, 3), (g, 1), (u, 0), (g, 2), (u, 1), (g, 3), (u, 2), (u, 3)]
    at_end_of(
        step,
        {4: [(d, "start")], 6: [(d, 0)], 9: [(g, "start")], 11: [(d, 1), (g, 0)], 13: [(d, 2)]}
        | {14: tail + [(unit, "finish") for unit in (d, g, u)]},
    )

    @pl.when(step == 3 * STEPS - 1)
    def _():
        clip_factor([d1, g1, u1, od, og, ou], factor, *scratch[3 * RS_SCRATCH :])


WHOLE_T = pl.BlockSpec((D, TOKENS), lambda i: (0, 0), pipeline_mode=pl.Buffered(1))


def in_turn(turn, block, index):
    return pl.BlockSpec(block, lambda i: index(jnp.clip(i - turn * STEPS, 0, STEPS - 1)))


COLUMNS_IN_TURN = [in_turn(turn, (TOKENS, NB), lambda i: (0, i)) for turn in range(3)]


def upper_gradients(dt, at, act, dg, du):
    return pl.pallas_call(
        upper_kernel,
        grid=(3 * STEPS,),
        in_specs=[WHOLE_T, WHOLE_T, *COLUMNS_IN_TURN],
        out_specs=[in_turn(turn, (8, 2, 56, NB), lambda i: (0, 0, 0, i)) for turn in (1, 2)] + [shard(TALL)],
        out_shape=[jax.ShapeDtypeStruct((8, 2, 56, FF), BF16)] * 2 + [matrix(*TALL[:2])],
        scratch_shapes=rs_scratch(TALL, True),
        compiler_params=params(True),
        cost_estimate=cost(3),
        name="upper_gradients",
    )(dt, at, act, dg, du)


def lower_gradients(dt, at, act, dg, du, before):
    kinds = (TALL, WIDE, WIDE)
    return pl.pallas_call(
        lower_kernel,
        grid=(3 * STEPS,),
        in_specs=[WHOLE_T, WHOLE_T, *COLUMNS_IN_TURN] + [shard(k) for k in kinds],
        out_specs=[shard(k) for k in kinds] + [pl.BlockSpec((8, 128), lambda i: (0, 0))],
        out_shape=[matrix(*k[:2]) for k in kinds] + [matrix(8, 128, F32)],
        scratch_shapes=sum((rs_scratch(k, True) for k in kinds), []) + CLIP_SCRATCH,
        compiler_params=params(True),
        cost_estimate=cost(3),
        name="lower_gradients",
    )(dt, at, act, dg, du, *before)


def adamw(w, m, v, g):
    m = 0.9 * m + 0.1 * g
    v = 0.95 * v + 0.05 * g * g
    step = m * lax.rsqrt(v + 1e-8) + 0.1 * w
    return (w - 0.02 * step).astype(BF16), m, v


def solution(mesh):
    def step(x, dy, wg, wu, wd, *moments):
        h1, a0, act0, gate0, up0 = forward(x, wg, wu, wd)
        a1, dyt, act1, dg1, du1 = last(h1, dy, wg, wu, wd)
        gg1, gu1, d1 = upper_gradients(dyt, a1, act1, dg1, du1)
        dht, dg0, du0, g1, u1 = between(dg1, du1, h1, dy, gate0, up0, wg, wu, wd, gg1, gu1)
        d0, g0, u0, factor = lower_gradients(dht, a0, act0, dg0, du0, (d1, g1, u1))
        shards = [jnp.stack(pair).astype(F32) for pair in ((g0, g1), (u0, u1), (d0, d1))]
        me = lax.axis_index("dp")
        f = factor[0, 0]
        new = []
        for k, w in enumerate((wg, wu, wd)):
            r = w.shape[1] // DEVICES
            own = lax.dynamic_slice_in_dim(w, me * r, r, 1).astype(F32)
            new.append(adamw(own, moments[k], moments[3 + k], shards[k] * f))
        gathered = all_gather([n[0] for n in new])
        return (*gathered, *(n[1] for n in new), *(n[2] for n in new))

    seq = P(("rep", "dp"), None, None)
    whole = P(None, None, None)
    part = P(None, "dp", None)
    return jax.shard_map(
        step,
        mesh=mesh,
        in_specs=(seq, seq, whole, whole, whole) + (part,) * 6,
        out_specs=(P("rep", None, None),) * 3 + (P("rep", "dp", None),) * 6,
        check_vma=False,
    )
```

```python
import functools

import jax
import jax.numpy as jnp
from jax import lax
from jax.experimental import pallas as pl
from jax.experimental.pallas import tpu as pltpu
from jax.sharding import PartitionSpec as P

MESH = pl.DeviceIdType.MESH
F32, BF16 = jnp.float32, jnp.bfloat16
DEVICES, TOKENS, D, FF = 16, 2048, 896, 2560
COUNT = 2 * 3 * D * FF
TM = 256
NB = 512
STEPS = FF // NB
ANY = pl.BlockSpec(memory_space=pl.ANY)
WHOLE = pl.BlockSpec(memory_space=pltpu.VMEM)

STRIDE = (8, 4, 2)
ORDER = ((0, 1, 2), (1, 2, 0), (2, 0, 1))
WIDE = (56, 2560, tuple((slice(0, 56), s) for s in (slice(0, 896), slice(896, 1792), slice(1792, 2560))))
TALL = (160, 896, tuple((s, slice(0, 896)) for s in (slice(0, 56), slice(56, 112), slice(112, 160))))


def size(s):
    return s.stop - s.start


def place():
    me = lax.axis_index("dp")
    return me, (me // 8 % 2, me // 4 % 2, me // 2 % 2), me % 2


def beside(me, xyz, axis):
    return me + STRIDE[axis] * (1 - 2 * xyz[axis])


def partner(me, core):
    return me + 1 - 2 * core


def rs_scratch(kind, here):
    r, c, parts = kind
    flat = [pltpu.VMEM((8, 2, r, c) if here else (8, r, c), BF16), pltpu.VMEM((8, r, c), BF16)]
    for rows, cols in parts:
        flat += [pltpu.VMEM((7, size(rows), size(cols)), BF16)] * 2
    return flat + [pltpu.SemaphoreType.DMA((10,)), pltpu.SemaphoreType.DMA((10,)), pltpu.SemaphoreType.DMA(())]


RS_SCRATCH = 11


class Reduce:
    def __init__(self, kind, g, out, scratch):
        self.kind, self.out, self.here = kind, out, g is None
        self.own, self.other = scratch[:2]
        self.g = self.own if self.here else g
        self.send, self.got = scratch[2:8:2], scratch[3:8:2]
        self.ssem, self.rsem, self.lsem = scratch[8:]
        self.me, self.xyz, self.core = place()

    def swap(self):
        return pltpu.make_async_remote_copy(
            self.g.at[:, 1 - self.core],
            self.other,
            self.ssem.at[9],
            self.rsem.at[9],
            device_id={"dp": partner(self.me, self.core)},
            device_id_type=MESH,
        )

    def load(self):
        return pltpu.make_async_copy(self.g.at[:, self.core], self.own, self.lsem)

    def hop(self, t, phase):
        at = pl.ds((0, 4, 6)[phase], (4, 2, 1)[phase])
        return pltpu.make_async_remote_copy(
            self.send[t].at[at],
            self.got[t].at[at],
            self.ssem.at[3 * t + phase],
            self.rsem.at[3 * t + phase],
            device_id={"dp": beside(self.me, self.xyz, ORDER[t][phase])},
            device_id_type=MESH,
        )

    def total(self, t, at, got):
        rows, cols = self.kind[2][t]
        block = sum(p * (4, 2, 1)[axis] for p, axis in zip(at, ORDER[t], strict=True))
        own = self.own[block, self.core, rows, cols] if self.here else self.own[block, rows, cols]
        sum_ = own.astype(F32) + self.other[block, rows, cols].astype(F32)
        for i in got:
            sum_ = sum_ + self.got[t][i].astype(F32)
        return sum_

    def start(self):
        self.swap().start()
        if not self.here:
            self.load().start()

    def stage(self, n):
        if n == 0:
            if not self.here:
                self.load().wait()
            self.swap().wait_recv()
        for t in range(3):
            p1, p2, p3 = (self.xyz[axis] for axis in ORDER[t])
            if n:
                self.hop(t, n - 1).wait_recv()
            if n == 0:
                for j in range(2):
                    for k in range(2):
                        self.send[t][2 * j + k] = self.total(t, (1 - p1, j, k), ()).astype(BF16)
            elif n == 1:
                for k in range(2):
                    self.send[t][4 + k] = self.total(t, (p1, 1 - p2, k), (2 * (1 - p2) + k,)).astype(BF16)
            elif n == 2:
                self.send[t][6] = self.total(t, (p1, p2, 1 - p3), (2 * p2 + 1 - p3, 5 - p3)).astype(BF16)
            else:
                rows, cols = self.kind[2][t]
                self.out[rows, cols] = self.total(t, (p1, p2, p3), (2 * p2 + p3, 4 + p3, 6)).astype(BF16)
            if n < 3:
                self.hop(t, n).start()

    def finish(self):
        self.swap().wait_send()
        for t in range(3):
            for phase in range(3):
                self.hop(t, phase).wait_send()


def squares(g):
    wide = g.astype(F32)
    rows, cols = wide.shape
    s = jnp.sum((wide * wide).reshape(rows // 8, 8, cols), 0)
    return sum(s[:, i : i + 128] for i in range(0, cols, 128))


def clip_factor(shards, factor, squared, sums, ssem, rsem):
    me = lax.axis_index("dp")
    squared[...] = sum(squares(g[...]) for g in shards)

    def give(k, slot):
        to = (me + k) % DEVICES
        return pltpu.make_async_remote_copy(
            squared, sums.at[slot], ssem.at[k], rsem.at[slot], device_id={"dp": to}, device_id_type=MESH
        )

    for k in range(1, DEVICES):
        give(k, me).start()
    sums[me] = squared[...]
    for k in range(1, DEVICES):
        give(k, (me + k) % DEVICES).wait_recv()
    for k in range(1, DEVICES):
        give(k, me).wait_send()
    total = jnp.sum(jnp.sum(jnp.sum(sums[...], 0), 0, keepdims=True), 1, keepdims=True)
    f = jnp.minimum(1.0, 0.5 * lax.rsqrt(total / COUNT + 1e-30))
    factor[...] = jnp.broadcast_to(f, factor.shape)


CLIP_SCRATCH = [
    pltpu.VMEM((8, 128), F32),
    pltpu.VMEM((DEVICES, 8, 128), F32),
    pltpu.SemaphoreType.DMA((DEVICES,)),
    pltpu.SemaphoreType.DMA((DEVICES,)),
]


def at_end_of(step, plan):
    for when, entries in plan.items():

        @pl.when(step == when)
        def _(entries=entries):
            for unit, stage in entries:
                if stage == "start":
                    unit.start()
                elif stage == "finish":
                    unit.finish()
                else:
                    unit.stage(stage)


class Gather:
    def __init__(self, kind, own, out, layer, ssem, rsem, csem):
        self.kind, self.own, self.out, self.layer = kind, own, out, layer
        self.ssem, self.rsem, self.csem = ssem, rsem, csem
        self.me, self.xyz, self.core = place()

    def local(self):
        x, y, z = self.xyz
        return pltpu.make_async_copy(self.own, self.out.at[self.layer, x, y, z, self.core], self.csem)

    def blocks(self, t, core, known, other=None):
        rows, cols = self.kind[2][t]
        index = []
        for axis in range(3):
            p = self.xyz[axis]
            index.append(slice(None) if axis in known else (1 - p if axis == other else p))
        return self.out.at[(self.layer, *index, core, rows, cols)]

    def hop(self, t, phase, arriving=False):
        axis = ORDER[t][phase]
        known = ORDER[t][:phase]
        src = self.blocks(t, self.core, known)
        dst = self.blocks(t, self.core, known, axis) if arriving else src
        if phase == 0 and not arriving:
            src = self.own.at[self.kind[2][t]]
        return pltpu.make_async_remote_copy(
            src,
            dst,
            self.ssem.at[3 * t + phase],
            self.rsem.at[3 * t + phase],
            device_id={"dp": beside(self.me, self.xyz, axis)},
            device_id_type=MESH,
        )

    def share(self, t, phase, core):
        ref = self.blocks(t, core, ORDER[t][:phase], ORDER[t][phase])
        return pltpu.make_async_remote_copy(
            ref,
            ref,
            self.ssem.at[10 + 3 * t + phase],
            self.rsem.at[10 + 3 * t + phase],
            device_id={"dp": partner(self.me, self.core)},
            device_id_type=MESH,
        )

    def share_own(self, core):
        x, y, z = self.xyz
        return pltpu.make_async_remote_copy(
            self.own,
            self.out.at[self.layer, x, y, z, core],
            self.ssem.at[9],
            self.rsem.at[9],
            device_id={"dp": partner(self.me, self.core)},
            device_id_type=MESH,
        )

    def start(self):
        self.local().start()
        for t in range(3):
            self.hop(t, 0).start()
        self.share_own(self.core).start()

    def stage(self, phase):
        if phase == 0:
            self.local().wait()
        for t in range(3):
            self.hop(t, phase, True).wait_recv()
            if phase < 2:
                self.hop(t, phase + 1).start()
            self.share(t, phase, self.core).start()

    def finish(self):
        self.share_own(1 - self.core).wait_recv()
        self.share_own(self.core).wait_send()
        for t in range(3):
            for phase in range(3):
                self.share(t, phase, 1 - self.core).wait_recv()
                self.share(t, phase, self.core).wait_send()
                self.hop(t, phase).wait_send()


def gather_kernel(*refs):
    owns, outs, (ssem, rsem, csem) = refs[:3], refs[3:6], refs[6:]
    units = []
    for layer in range(2):
        for i, kind in enumerate((WIDE, WIDE, TALL)):
            u = 3 * layer + i
            units.append(Gather(kind, owns[i].at[layer], outs[i], layer, ssem.at[u], rsem.at[u], csem.at[u]))
    for u in units:
        u.start()
    for phase in range(3):
        for u in units:
            u.stage(phase)
    for u in units:
        u.finish()


def all_gather(owns):
    outs = pl.pallas_call(
        gather_kernel,
        out_shape=[pltpu.VMEM((2, 2, 2, 2, 2, *o.shape[1:]), BF16) for o in owns],
        in_specs=[WHOLE] * 3,
        out_specs=[WHOLE] * 3,
        scratch_shapes=[
            pltpu.SemaphoreType.DMA((6, 19)),
            pltpu.SemaphoreType.DMA((6, 19)),
            pltpu.SemaphoreType.DMA((6,)),
        ],
        compiler_params=pltpu.CompilerParams(has_side_effects=True, vmem_limit_bytes=8 << 20),
        name="all_gather",
    )(*owns)
    outs = pl.pallas_call(
        flush_kernel,
        out_shape=[jax.ShapeDtypeStruct(o.shape, BF16) for o in outs],
        in_specs=[WHOLE] * 3,
        out_specs=[ANY] * 3,
        scratch_shapes=[pltpu.SemaphoreType.DMA((6,))],
        compiler_params=pltpu.CompilerParams(vmem_limit_bytes=1 << 20),
        name="flush",
    )(*outs)
    return [o.reshape(2, DEVICES * o.shape[-2], o.shape[-1]) for o in outs]


def flush_kernel(*refs):
    copies = []
    for i in range(3):
        for layer in range(2):
            copies.append(pltpu.make_async_copy(refs[i].at[layer], refs[3 + i].at[layer], refs[6].at[2 * i + layer]))
    for c in copies:
        c.start()
    for c in copies:
        c.wait()


KINDS = (WIDE, WIDE, TALL)


def adamw_kernel(*refs):
    factor, shards, ms, vs, weights = refs[0], refs[1:7], refs[7:10], refs[10:13], refs[13:16]
    new_ws, new_ms, new_vs = refs[16:19], refs[19:22], refs[22:25]
    in_ms, in_vs, gs, (isem, osem) = refs[25:28], refs[28:31], refs[31:34], refs[34:]
    me = lax.axis_index("dp")
    loads, stores = [], []
    for i, kind in enumerate(KINDS):
        mine = pl.ds(pl.multiple_of(me * kind[0], 8), kind[0])
        for layer in range(2):
            pairs = (
                (shards[3 * layer + i], gs[i].at[layer]),
                (ms[i].at[layer], in_ms[i].at[layer]),
                (vs[i].at[layer], in_vs[i].at[layer]),
                (weights[i].at[layer, mine], new_ws[i].at[layer]),
            )
            loads.append([pltpu.make_async_copy(src, dst, isem.at[2 * i + layer, k]) for k, (src, dst) in enumerate(pairs)])
            pairs = (in_ms[i], new_ms[i]), (in_vs[i], new_vs[i])
            stores.append(
                [
                    pltpu.make_async_copy(src.at[layer], dst.at[layer], osem.at[2 * i + layer, k])
                    for k, (src, dst) in enumerate(pairs)
                ]
            )
    for copies in loads:
        for c in copies:
            c.start()
    f = factor[0:1, 0:1]
    for u in range(6):
        i, layer = divmod(u, 2)
        for c in loads[u]:
            c.wait()
        g = gs[i][layer].astype(F32) * f
        w = new_ws[i][layer].astype(F32)
        m = 0.9 * in_ms[i][layer] + 0.1 * g
        v = 0.95 * in_vs[i][layer] + 0.05 * g * g
        step = m * lax.rsqrt(v + 1e-8) + 0.1 * w
        new_ws[i][layer], in_ms[i][layer], in_vs[i][layer] = (w - 0.02 * step).astype(BF16), m, v
        for c in stores[u]:
            c.start()
    for copies in stores:
        for c in copies:
            c.wait()


def adamw(factor, shards, ms, vs, weights):
    own = [(2, *k[:2]) for k in KINDS]
    outs = pl.pallas_call(
        adamw_kernel,
        out_shape=[pltpu.VMEM(s, BF16) for s in own] + [jax.ShapeDtypeStruct(s, F32) for s in own * 2],
        in_specs=[WHOLE] + [ANY] * 15,
        out_specs=[WHOLE] * 3 + [ANY] * 6,
        scratch_shapes=[pltpu.VMEM(s, t) for t in (F32, F32, BF16) for s in own]
        + [pltpu.SemaphoreType.DMA((6, 4)), pltpu.SemaphoreType.DMA((6, 2))],
        compiler_params=pltpu.CompilerParams(vmem_limit_bytes=60 * 1024 * 1024),
        name="adamw",
    )(factor, *shards, *ms, *vs, *weights)
    return outs[:3], outs[3:]


def dot(a, b):
    return jnp.dot(a, b, preferred_element_type=F32)


def dot_t(a, b):
    return lax.dot_general(a, b, (((1,), (1,)), ((), ())), preferred_element_type=F32)


def norm(h):
    wide = h.astype(F32)
    scale = lax.rsqrt(jnp.mean(wide * wide, -1, keepdims=True) + 1e-6)
    return wide, scale, (wide * scale).astype(BF16)


def gated_back(gate, up, dact):
    sig = jax.nn.sigmoid(gate)
    d = dact.astype(F32)
    dup = d * (gate * sig)
    dgate = d * up * (sig * (1 + gate * (1 - sig)))
    return dgate.astype(BF16), dup.astype(BF16)


def forward_kernel(x, wg, wu, wd, h1, at, act, gate, up):
    h = x[...]
    _, _, a = norm(h)
    at[...] = a.T
    g = dot(a, wg[...])
    u = dot(a, wu[...])
    gate[...] = g
    up[...] = u
    s = (g * jax.nn.sigmoid(g) * u).astype(BF16)
    act[...] = s
    h1[...] = h + dot(s, wd[...]).astype(BF16)


def last_kernel(h1, dy, wg, wu, wd, at, dyt, act, dgate, dup):
    _, _, a = norm(h1[...])
    at[...] = a.T
    dyt[...] = dy[...].T
    g = dot(a, wg[...])
    u = dot(a, wu[...])
    act[...] = (g * jax.nn.sigmoid(g) * u).astype(BF16)
    dact = dot_t(dy[...], wd[...]).astype(BF16)
    dgate[...], dup[...] = gated_back(g, u, dact)


def between_kernel(dg1, du1, h1, dy, gate, up, wg, wu, wd, gg, gu, dht, dgate, dup, og, ou, *scratch):
    step = pl.program_id(0)
    units = [Reduce(WIDE, gg, og, scratch[:RS_SCRATCH]), Reduce(WIDE, gu, ou, scratch[RS_SCRATCH:])]

    @pl.when(step == 0)
    def _():
        for u in units:
            u.start()

    da = dot_t(dg1[...], wg[...]).astype(BF16) + dot_t(du1[...], wu[...]).astype(BF16)
    wide, scale, _ = norm(h1[...])
    d = da.astype(F32)
    through = d * scale - wide * (scale * scale * scale * (jnp.sum(d * wide, -1, keepdims=True) / D))
    dh = dy[...] + through.astype(BF16)
    dht[...] = dh.T
    dact = dot_t(dh, wd[...]).astype(BF16)
    dgate[...], dup[...] = gated_back(gate[...], up[...], dact)
    plan = {when: [(u, stage) for u in units] for when, stage in ((1, 0), (4, 1), (6, 2))}
    plan[7] = [(u, stage) for stage in (3, "finish") for u in units]
    at_end_of(step, plan)


def rows(cols):
    return pl.BlockSpec((TM, cols), lambda i: (i, 0))


SEQ = pl.BlockSpec((None, TM, D), lambda i: (0, i, 0))
COLUMNS = pl.BlockSpec((D, TM), lambda i: (0, i))


def weight(layer, shape):
    return pl.BlockSpec((None, *shape), lambda i: (layer, 0, 0), pipeline_mode=pl.Buffered(1))


def matrix(r, c, t=BF16):
    return jax.ShapeDtypeStruct((r, c), t)


def cost(matmuls):
    return pl.CostEstimate(flops=matmuls * 2 * TOKENS * D * FF, bytes_accessed=60 << 20, transcendentals=0)


def params(remote=False):
    return pltpu.CompilerParams(vmem_limit_bytes=60 * 1024 * 1024, has_side_effects=remote)


def forward(x, wg, wu, wd):
    return pl.pallas_call(
        forward_kernel,
        grid=(TOKENS // TM,),
        in_specs=[SEQ, weight(0, (D, FF)), weight(0, (D, FF)), weight(0, (FF, D))],
        out_specs=[rows(D), COLUMNS, rows(FF), rows(FF), rows(FF)],
        out_shape=[matrix(TOKENS, D), matrix(D, TOKENS), matrix(TOKENS, FF), matrix(TOKENS, FF, F32), matrix(TOKENS, FF, F32)],
        compiler_params=params(),
        cost_estimate=cost(3),
        name="forward",
    )(x, wg, wu, wd)


def last(h1, dy, wg, wu, wd):
    return pl.pallas_call(
        last_kernel,
        grid=(TOKENS // TM,),
        in_specs=[rows(D), SEQ, weight(1, (D, FF)), weight(1, (D, FF)), weight(1, (FF, D))],
        out_specs=[COLUMNS, COLUMNS, rows(FF), rows(FF), rows(FF)],
        out_shape=[matrix(D, TOKENS)] * 2 + [matrix(TOKENS, FF)] * 3,
        compiler_params=params(),
        cost_estimate=cost(3),
        name="last",
    )(h1, dy, wg, wu, wd)


def shard(kind):
    return pl.BlockSpec(kind[:2], lambda i: (0, 0))


def between(dg1, du1, h1, dy, gate, up, wg, wu, wd, gg, gu):
    return pl.pallas_call(
        between_kernel,
        grid=(TOKENS // TM,),
        in_specs=[rows(FF), rows(FF), rows(D), SEQ, rows(FF), rows(FF)]
        + [weight(1, (D, FF)), weight(1, (D, FF)), weight(0, (FF, D)), ANY, ANY],
        out_specs=[COLUMNS, rows(FF), rows(FF), shard(WIDE), shard(WIDE)],
        out_shape=[matrix(D, TOKENS)] + [matrix(TOKENS, FF)] * 2 + [matrix(*WIDE[:2])] * 2,
        scratch_shapes=rs_scratch(WIDE, False) * 2,
        compiler_params=params(True),
        cost_estimate=cost(3),
        name="between",
    )(dg1, du1, h1, dy, gate, up, wg, wu, wd, gg, gu)


def tall_into(g, i, dt, act):
    g.reshape(FF, D)[pl.ds(pl.multiple_of(i * NB, NB), NB)] = dot(dt[...], act[...]).astype(BF16).T


def wide_block(at, dg):
    return dot(at[...], dg[...]).reshape(8, 2, 56, NB).astype(BF16)


def upper_kernel(dt, at, act, dg, du, gg, gu, od, *scratch):
    step = pl.program_id(0)
    d = Reduce(TALL, None, od, scratch)

    @pl.when(step < STEPS)
    def _():
        tall_into(d.g, step, dt, act)

    @pl.when((step >= STEPS) & (step < 2 * STEPS))
    def _():
        gg[...] = wide_block(at, dg)

    @pl.when(step >= 2 * STEPS)
    def _():
        gu[...] = wide_block(at, du)

    at_end_of(step, {4: [(d, "start")], 6: [(d, 0)], 11: [(d, 1)], 13: [(d, 2)], 14: [(d, 3), (d, "finish")]})


def lower_kernel(dt, at, act, dg, du, d1, g1, u1, od, og, ou, factor, *scratch):
    step = pl.program_id(0)
    d, g, u = (
        Reduce(kind, None, o, scratch[RS_SCRATCH * i : RS_SCRATCH * (i + 1)])
        for i, (kind, o) in enumerate(((TALL, od), (WIDE, og), (WIDE, ou)))
    )

    @pl.when(step < STEPS)
    def _():
        tall_into(d.g, step, dt, act)

    def columns(first):
        return pl.ds(pl.multiple_of((step - first) * NB, NB), NB)

    @pl.when((step >= STEPS) & (step < 2 * STEPS))
    def _():
        g.g[:, :, :, columns(STEPS)] = wide_block(at, dg)

    @pl.when(step >= 2 * STEPS)
    def _():
        u.g[:, :, :, columns(2 * STEPS)] = wide_block(at, du)

    tail = [(u, "start"), (d, 3), (g, 1), (u, 0), (g, 2), (u, 1), (g, 3), (u, 2), (u, 3)]
    at_end_of(
        step,
        {4: [(d, "start")], 6: [(d, 0)], 9: [(g, "start")], 11: [(d, 1), (g, 0)], 13: [(d, 2)]}
        | {14: tail + [(unit, "finish") for unit in (d, g, u)]},
    )

    @pl.when(step == 3 * STEPS - 1)
    def _():
        clip_factor([d1, g1, u1, od, og, ou], factor, *scratch[3 * RS_SCRATCH :])


WHOLE_T = pl.BlockSpec((D, TOKENS), lambda i: (0, 0), pipeline_mode=pl.Buffered(1))


def in_turn(turn, block, index):
    return pl.BlockSpec(block, lambda i: index(jnp.clip(i - turn * STEPS, 0, STEPS - 1)))


COLUMNS_IN_TURN = [in_turn(turn, (TOKENS, NB), lambda i: (0, i)) for turn in range(3)]


def upper_gradients(dt, at, act, dg, du):
    return pl.pallas_call(
        upper_kernel,
        grid=(3 * STEPS,),
        in_specs=[WHOLE_T, WHOLE_T, *COLUMNS_IN_TURN],
        out_specs=[in_turn(turn, (8, 2, 56, NB), lambda i: (0, 0, 0, i)) for turn in (1, 2)] + [shard(TALL)],
        out_shape=[jax.ShapeDtypeStruct((8, 2, 56, FF), BF16)] * 2 + [matrix(*TALL[:2])],
        scratch_shapes=rs_scratch(TALL, True),
        compiler_params=params(True),
        cost_estimate=cost(3),
        name="upper_gradients",
    )(dt, at, act, dg, du)


def lower_gradients(dt, at, act, dg, du, before):
    kinds = (TALL, WIDE, WIDE)
    return pl.pallas_call(
        lower_kernel,
        grid=(3 * STEPS,),
        in_specs=[WHOLE_T, WHOLE_T, *COLUMNS_IN_TURN] + [shard(k) for k in kinds],
        out_specs=[shard(k) for k in kinds] + [pl.BlockSpec((8, 128), lambda i: (0, 0))],
        out_shape=[matrix(*k[:2]) for k in kinds] + [matrix(8, 128, F32)],
        scratch_shapes=sum((rs_scratch(k, True) for k in kinds), []) + CLIP_SCRATCH,
        compiler_params=params(True),
        cost_estimate=cost(3),
        name="lower_gradients",
    )(dt, at, act, dg, du, *before)


def solution(mesh):
    def step(x, dy, wg, wu, wd, *moments):
        h1, a0, act0, gate0, up0 = forward(x, wg, wu, wd)
        a1, dyt, act1, dg1, du1 = last(h1, dy, wg, wu, wd)
        gg1, gu1, d1 = upper_gradients(dyt, a1, act1, dg1, du1)
        dht, dg0, du0, g1, u1 = between(dg1, du1, h1, dy, gate0, up0, wg, wu, wd, gg1, gu1)
        d0, g0, u0, factor = lower_gradients(dht, a0, act0, dg0, du0, (d1, g1, u1))
        own, new_moments = adamw(factor, (g0, u0, d0, g1, u1, d1), moments[:3], moments[3:], (wg, wu, wd))
        return (*all_gather(own), *new_moments)

    seq = P(("rep", "dp"), None, None)
    whole = P(None, None, None)
    part = P(None, "dp", None)
    return jax.shard_map(
        step,
        mesh=mesh,
        in_specs=(seq, seq, whole, whole, whole) + (part,) * 6,
        out_specs=(P("rep", None, None),) * 3 + (P("rep", "dp", None),) * 6,
        check_vma=False,
    )
```

```python
import functools

import jax
import jax.numpy as jnp
from jax import lax
from jax.experimental import pallas as pl
from jax.experimental.pallas import tpu as pltpu
from jax.sharding import PartitionSpec as P

MESH = pl.DeviceIdType.MESH
F32, BF16 = jnp.float32, jnp.bfloat16
DEVICES, TOKENS, D, FF = 16, 2048, 896, 2560
COUNT = 2 * 3 * D * FF
TM = 256
NB = 512
STEPS = FF // NB
BN = 256
ANY = pl.BlockSpec(memory_space=pl.ANY)
WHOLE = pl.BlockSpec(memory_space=pltpu.VMEM)

STRIDE = (8, 4, 2)
ORDER = ((0, 1, 2), (1, 2, 0), (2, 0, 1))
WIDE = (56, 2560, tuple((slice(0, 56), s) for s in (slice(0, 896), slice(896, 1792), slice(1792, 2560))))
BLOCK = (56, 256, tuple((s, slice(0, 256)) for s in (slice(0, 24), slice(24, 40), slice(40, 56))))
PAIR = (56, 512, tuple((s, slice(0, 512)) for s in (slice(0, 24), slice(24, 40), slice(40, 56))))
TALL = (160, 896, tuple((s, slice(0, 896)) for s in (slice(0, 56), slice(56, 112), slice(112, 160))))


def size(s):
    return s.stop - s.start


def place():
    me = lax.axis_index("dp")
    return me, (me // 8 % 2, me // 4 % 2, me // 2 % 2), me % 2


def beside(me, xyz, axis):
    return me + STRIDE[axis] * (1 - 2 * xyz[axis])


def partner(me, core):
    return me + 1 - 2 * core


def rs_scratch(kind, sets=()):
    r, c, parts = kind
    flat = [pltpu.VMEM((*sets, 8, r, c), BF16)]
    for rows, cols in parts:
        flat += [pltpu.VMEM((*sets, 7, size(rows), size(cols)), BF16)] * 2
    return flat + [pltpu.SemaphoreType.DMA((*sets, 10))] * 2 + [pltpu.SemaphoreType.DMA((*sets, 1))]


RS_SCRATCH = 10


class Reduce:
    def __init__(self, kind, g, out, scratch, own=None, turn=0):
        self.kind, self.g, self.out, self.here = kind, g, out, own is None
        self.own = g if self.here else own
        self.other = scratch[0]
        self.send, self.got = scratch[1:7:2], scratch[2:7:2]
        self.ssem, self.rsem, self.lsem = scratch[7:]
        self.me, self.xyz, self.core = place()
        self.order = ORDER[turn:] + ORDER[:turn]

    def swap(self):
        return pltpu.make_async_remote_copy(
            self.g.at[:, 1 - self.core],
            self.other,
            self.ssem.at[9],
            self.rsem.at[9],
            device_id={"dp": partner(self.me, self.core)},
            device_id_type=MESH,
        )

    def load(self):
        return pltpu.make_async_copy(self.g.at[:, self.core], self.own, self.lsem.at[0])

    def hop(self, t, phase):
        at = pl.ds((0, 4, 6)[phase], (4, 2, 1)[phase])
        return pltpu.make_async_remote_copy(
            self.send[t].at[at],
            self.got[t].at[at],
            self.ssem.at[3 * t + phase],
            self.rsem.at[3 * t + phase],
            device_id={"dp": beside(self.me, self.xyz, self.order[t][phase])},
            device_id_type=MESH,
        )

    def total(self, t, at, got):
        rows, cols = self.kind[2][t]
        block = sum(p * (4, 2, 1)[axis] for p, axis in zip(at, self.order[t], strict=True))
        own = self.own[block, self.core, rows, cols] if self.here else self.own[block, rows, cols]
        sum_ = own.astype(F32) + self.other[block, rows, cols].astype(F32)
        for i in got:
            sum_ = sum_ + self.got[t][i].astype(F32)
        return sum_

    def start(self):
        self.swap().start()
        if not self.here:
            self.load().start()

    def stage(self, n):
        if n == 0:
            if not self.here:
                self.load().wait()
            self.swap().wait_recv()
        for t in range(3):
            p1, p2, p3 = (self.xyz[axis] for axis in self.order[t])
            if n:
                self.hop(t, n - 1).wait_recv()
            if n == 0:
                for j in range(2):
                    for k in range(2):
                        self.send[t][2 * j + k] = self.total(t, (1 - p1, j, k), ()).astype(BF16)
            elif n == 1:
                for k in range(2):
                    self.send[t][4 + k] = self.total(t, (p1, 1 - p2, k), (2 * (1 - p2) + k,)).astype(BF16)
            elif n == 2:
                self.send[t][6] = self.total(t, (p1, p2, 1 - p3), (2 * p2 + 1 - p3, 5 - p3)).astype(BF16)
            else:
                rows, cols = self.kind[2][t]
                self.out[rows, cols] = self.total(t, (p1, p2, p3), (2 * p2 + p3, 4 + p3, 6)).astype(BF16)
            if n < 3:
                self.hop(t, n).start()

    def finish(self):
        self.swap().wait_send()
        for t in range(3):
            for phase in range(3):
                self.hop(t, phase).wait_send()


def squares(g):
    wide = g.astype(F32)
    rows, cols = wide.shape
    s = jnp.sum((wide * wide).reshape(rows // 8, 8, cols), 0)
    return sum(s[:, i : i + 128] for i in range(0, cols, 128))


def clip_factor(shards, factor, squared, sums, ssem, rsem):
    me = lax.axis_index("dp")
    squared[...] = sum(squares(g[...]) for g in shards)

    def give(k, slot):
        to = (me + k) % DEVICES
        return pltpu.make_async_remote_copy(
            squared, sums.at[slot], ssem.at[k], rsem.at[slot], device_id={"dp": to}, device_id_type=MESH
        )

    for k in range(1, DEVICES):
        give(k, me).start()
    sums[me] = squared[...]
    for k in range(1, DEVICES):
        give(k, (me + k) % DEVICES).wait_recv()
    for k in range(1, DEVICES):
        give(k, me).wait_send()
    total = jnp.sum(jnp.sum(jnp.sum(sums[...], 0), 0, keepdims=True), 1, keepdims=True)
    f = jnp.minimum(1.0, 0.5 * lax.rsqrt(total / COUNT + 1e-30))
    factor[...] = jnp.broadcast_to(f, factor.shape)


CLIP_SCRATCH = [
    pltpu.VMEM((8, 128), F32),
    pltpu.VMEM((DEVICES, 8, 128), F32),
    pltpu.SemaphoreType.DMA((DEVICES,)),
    pltpu.SemaphoreType.DMA((DEVICES,)),
]


def at_end_of(step, plan):
    for when, entries in plan.items():

        @pl.when(step == when)
        def _(entries=entries):
            for unit, stage in entries:
                if stage == "start":
                    unit.start()
                elif stage == "finish":
                    unit.finish()
                else:
                    unit.stage(stage)


class Gather:
    def __init__(self, kind, own, out, layer, ssem, rsem, csem):
        self.kind, self.own, self.out, self.layer = kind, own, out, layer
        self.ssem, self.rsem, self.csem = ssem, rsem, csem
        self.me, self.xyz, self.core = place()

    def local(self):
        x, y, z = self.xyz
        return pltpu.make_async_copy(self.own, self.out.at[self.layer, x, y, z, self.core], self.csem)

    def blocks(self, t, core, known, other=None):
        rows, cols = self.kind[2][t]
        index = []
        for axis in range(3):
            p = self.xyz[axis]
            index.append(slice(None) if axis in known else (1 - p if axis == other else p))
        return self.out.at[(self.layer, *index, core, rows, cols)]

    def hop(self, t, phase, arriving=False):
        axis = ORDER[t][phase]
        known = ORDER[t][:phase]
        src = self.blocks(t, self.core, known)
        dst = self.blocks(t, self.core, known, axis) if arriving else src
        if phase == 0 and not arriving:
            src = self.own.at[self.kind[2][t]]
        return pltpu.make_async_remote_copy(
            src,
            dst,
            self.ssem.at[3 * t + phase],
            self.rsem.at[3 * t + phase],
            device_id={"dp": beside(self.me, self.xyz, axis)},
            device_id_type=MESH,
        )

    def share(self, t, phase, core):
        ref = self.blocks(t, core, ORDER[t][:phase], ORDER[t][phase])
        return pltpu.make_async_remote_copy(
            ref,
            ref,
            self.ssem.at[10 + 3 * t + phase],
            self.rsem.at[10 + 3 * t + phase],
            device_id={"dp": partner(self.me, self.core)},
            device_id_type=MESH,
        )

    def share_own(self, core):
        x, y, z = self.xyz
        return pltpu.make_async_remote_copy(
            self.own,
            self.out.at[self.layer, x, y, z, core],
            self.ssem.at[9],
            self.rsem.at[9],
            device_id={"dp": partner(self.me, self.core)},
            device_id_type=MESH,
        )

    def start(self):
        self.local().start()
        for t in range(3):
            self.hop(t, 0).start()
        self.share_own(self.core).start()

    def stage(self, phase):
        if phase == 0:
            self.local().wait()
        for t in range(3):
            self.hop(t, phase, True).wait_recv()
            if phase < 2:
                self.hop(t, phase + 1).start()
            self.share(t, phase, self.core).start()

    def finish(self):
        self.share_own(1 - self.core).wait_recv()
        self.share_own(self.core).wait_send()
        for t in range(3):
            for phase in range(3):
                self.share(t, phase, 1 - self.core).wait_recv()
                self.share(t, phase, self.core).wait_send()
                self.hop(t, phase).wait_send()


def gather_kernel(*refs):
    owns, outs, (ssem, rsem, csem) = refs[:3], refs[3:6], refs[6:]
    units = []
    for layer in range(2):
        for i, kind in enumerate((WIDE, WIDE, TALL)):
            u = 3 * layer + i
            units.append(Gather(kind, owns[i].at[layer], outs[i], layer, ssem.at[u], rsem.at[u], csem.at[u]))
    for u in units:
        u.start()
    for phase in range(3):
        for u in units:
            u.stage(phase)
    for u in units:
        u.finish()


def all_gather(owns):
    outs = pl.pallas_call(
        gather_kernel,
        out_shape=[pltpu.VMEM((2, 2, 2, 2, 2, *o.shape[1:]), BF16) for o in owns],
        in_specs=[WHOLE] * 3,
        out_specs=[WHOLE] * 3,
        scratch_shapes=[
            pltpu.SemaphoreType.DMA((6, 19)),
            pltpu.SemaphoreType.DMA((6, 19)),
            pltpu.SemaphoreType.DMA((6,)),
        ],
        compiler_params=pltpu.CompilerParams(has_side_effects=True, vmem_limit_bytes=8 << 20),
        name="all_gather",
    )(*owns)
    outs = pl.pallas_call(
        flush_kernel,
        out_shape=[jax.ShapeDtypeStruct(o.shape, BF16) for o in outs],
        in_specs=[WHOLE] * 3,
        out_specs=[ANY] * 3,
        scratch_shapes=[pltpu.SemaphoreType.DMA((6,))],
        compiler_params=pltpu.CompilerParams(vmem_limit_bytes=1 << 20),
        name="flush",
    )(*outs)
    return [o.reshape(2, DEVICES * o.shape[-2], o.shape[-1]) for o in outs]


def flush_kernel(*refs):
    copies = []
    for i in range(3):
        for layer in range(2):
            copies.append(pltpu.make_async_copy(refs[i].at[layer], refs[3 + i].at[layer], refs[6].at[2 * i + layer]))
    for c in copies:
        c.start()
    for c in copies:
        c.wait()


KINDS = (WIDE, WIDE, TALL)


def adamw_kernel(*refs):
    factor, shards, ms, vs, weights = refs[0], refs[1:7], refs[7:10], refs[10:13], refs[13:16]
    new_ws, new_ms, new_vs = refs[16:19], refs[19:22], refs[22:25]
    in_ms, in_vs, gs, (isem, osem) = refs[25:28], refs[28:31], refs[31:34], refs[34:]
    me = lax.axis_index("dp")
    loads, stores = [], []
    for i, kind in enumerate(KINDS):
        mine = pl.ds(pl.multiple_of(me * kind[0], 8), kind[0])
        for layer in range(2):
            pairs = (
                (shards[3 * layer + i], gs[i].at[layer]),
                (ms[i].at[layer], in_ms[i].at[layer]),
                (vs[i].at[layer], in_vs[i].at[layer]),
                (weights[i].at[layer, mine], new_ws[i].at[layer]),
            )
            loads.append([pltpu.make_async_copy(src, dst, isem.at[2 * i + layer, k]) for k, (src, dst) in enumerate(pairs)])
            pairs = (in_ms[i], new_ms[i]), (in_vs[i], new_vs[i])
            stores.append(
                [
                    pltpu.make_async_copy(src.at[layer], dst.at[layer], osem.at[2 * i + layer, k])
                    for k, (src, dst) in enumerate(pairs)
                ]
            )
    for copies in loads:
        for c in copies:
            c.start()
    f = factor[0:1, 0:1]
    for u in range(6):
        i, layer = divmod(u, 2)
        for c in loads[u]:
            c.wait()
        g = gs[i][layer].astype(F32) * f
        w = new_ws[i][layer].astype(F32)
        m = 0.9 * in_ms[i][layer] + 0.1 * g
        v = 0.95 * in_vs[i][layer] + 0.05 * g * g
        step = m * lax.rsqrt(v + 1e-8) + 0.1 * w
        new_ws[i][layer], in_ms[i][layer], in_vs[i][layer] = (w - 0.02 * step).astype(BF16), m, v
        for c in stores[u]:
            c.start()
    for copies in stores:
        for c in copies:
            c.wait()


def adamw(factor, shards, ms, vs, weights):
    own = [(2, *k[:2]) for k in KINDS]
    outs = pl.pallas_call(
        adamw_kernel,
        out_shape=[pltpu.VMEM(s, BF16) for s in own] + [jax.ShapeDtypeStruct(s, F32) for s in own * 2],
        in_specs=[WHOLE] + [ANY] * 15,
        out_specs=[WHOLE] * 3 + [ANY] * 6,
        scratch_shapes=[pltpu.VMEM(s, t) for t in (F32, F32, BF16) for s in own]
        + [pltpu.SemaphoreType.DMA((6, 4)), pltpu.SemaphoreType.DMA((6, 2))],
        compiler_params=pltpu.CompilerParams(vmem_limit_bytes=60 * 1024 * 1024),
        name="adamw",
    )(factor, *shards, *ms, *vs, *weights)
    return outs[:3], outs[3:]


def dot(a, b):
    return jnp.dot(a, b, preferred_element_type=F32)


def dot_t(a, b):
    return lax.dot_general(a, b, (((1,), (1,)), ((), ())), preferred_element_type=F32)


def norm(h):
    wide = h.astype(F32)
    scale = lax.rsqrt(jnp.mean(wide * wide, -1, keepdims=True) + 1e-6)
    return wide, scale, (wide * scale).astype(BF16)


def gated_back(gate, up, dact):
    sig = jax.nn.sigmoid(gate)
    d = dact.astype(F32)
    dup = d * (gate * sig)
    dgate = d * up * (sig * (1 + gate * (1 - sig)))
    return dgate.astype(BF16), dup.astype(BF16)


def forward_kernel(x, dy, wg, wu, wd, h1, a1, a1t, dyt, at, act, gate, up):
    h = x[...]
    _, _, a = norm(h)
    at[...] = a.T
    dyt[...] = dy[...].T
    g = dot(a, wg[...])
    u = dot(a, wu[...])
    gate[...] = g
    up[...] = u
    s = (g * jax.nn.sigmoid(g) * u).astype(BF16)
    act[...] = s
    h = h + dot(s, wd[...]).astype(BF16)
    h1[...] = h
    _, _, a = norm(h)
    a1[...] = a
    a1t[...] = a.T


def pieces(count):
    n = TOKENS // count
    return [slice(n * i, n * i + n) for i in range(count)]


def wide_block(at, dg):
    return dot(at[...], dg[...]).reshape(8, 2, 56, dg.shape[-1]).astype(BF16)


def last_kernel(hbm_a, hbm_at, hbm_dy, hbm_dyt, hbm_h, wg, wu, wd, gd, og, ou, out_dh, out_dht, *scratch):
    a, at, dy, dyt, h, act, dg, du, acc_g, acc_u, own_g, own_u, lsem, osem = scratch[:14]
    step = pl.program_id(0)
    sources = (hbm_a, hbm_dy, hbm_at, hbm_dyt, hbm_h)
    loads = [pltpu.make_async_copy(s, d, lsem.at[i]) for i, (s, d) in enumerate(zip(sources, (a, dy, at, dyt, h), strict=True))]

    def first(i):
        @pl.when(step == 0)
        def _():
            loads[i].wait()

    def units(k):
        columns = pl.ds(pl.multiple_of(k * NB, NB), NB)
        rest = [ref.at[k % 2] for ref in scratch[14:]]
        return [
            Reduce(PAIR, own, out.at[:, columns], rest[RS_SCRATCH * i : RS_SCRATCH * (i + 1)], turn=i)
            for i, (own, out) in enumerate(((own_g, og), (own_u, ou)))
        ]

    def reduce(k, *stages):
        for stage in stages:
            for u in units(k):
                if stage == "start":
                    u.start()
                elif stage == "finish":
                    u.finish()
                else:
                    u.stage(stage)

    @pl.when(step == 0)
    def _():
        for c in loads:
            c.start()
        acc_g[...] = jnp.zeros_like(acc_g)
        acc_u[...] = jnp.zeros_like(acc_u)
        loads[0].wait()
        loads[1].wait()

    def projections(r):
        g = dot(a[r], wg[...])
        u = dot(a[r], wu[...])
        dact = dot_t(dy[r], wd[...]).astype(BF16)
        act[r] = (g * jax.nn.sigmoid(g) * u).astype(BF16)
        dg[r], du[r] = gated_back(g, u, dact)

    quarters = pieces(4)
    for r in quarters[:2]:
        projections(r)

    @pl.when(step > 0)
    def _():
        reduce(step - 1, 2)

    for r in quarters[2:]:
        projections(r)

    @pl.when(step > 0)
    def _():
        reduce(step - 1, 3, "finish")

    first(2)
    own_g[...] = wide_block(at, dg)
    own_u[...] = wide_block(at, du)
    reduce(step, "start")
    first(3)
    gd[...] = dot(dyt[...], act[...]).astype(BF16).T
    reduce(step, 0)
    for r in quarters:
        acc_g[r] += dot_t(dg[r], wg[...])
        acc_u[r] += dot_t(du[r], wu[...])
    reduce(step, 1)

    @pl.when(step == STEPS - 1)
    def _():
        loads[4].wait()

        def through(i, carry):
            r = pl.ds(pl.multiple_of(i * 256, 256), 256)
            d = (acc_g[r].astype(BF16) + acc_u[r].astype(BF16)).astype(F32)
            wide, scale, _ = norm(h[r])
            d = d * scale - wide * (scale * scale * scale * (jnp.sum(d * wide, -1, keepdims=True) / D))
            d = dy[r] + d.astype(BF16)
            a[r] = d
            at[:, r] = d.T
            return carry

        lax.fori_loop(0, 4, through, 0)
        reduce(step, 2)
        lax.fori_loop(4, 8, through, 0)
        stores = [pltpu.make_async_copy(s, d, osem.at[i]) for i, (s, d) in enumerate(((a, out_dh), (at, out_dht)))]
        for c in stores:
            c.start()
        reduce(step, 3, "finish")
        for c in stores:
            c.wait()


SETS = 5


def lower_kernel(dh, dht, at, act, gate, up, wd, gd1, g1, u1, od1, od, og, ou, factor, *scratch):
    step = pl.program_id(0)
    dg, du, own_g, own_u, own_d, half_d1 = scratch[:6]
    rest = scratch[6:]
    sets = [rest[RS_SCRATCH * i : RS_SCRATCH * (i + 1)] for i in range(2 + 2 * SETS)]
    d1 = Reduce(TALL, gd1, od1, sets[0], half_d1)
    d = Reduce(TALL, own_d, od, sets[1], turn=1)

    @pl.when(step == 0)
    def _():
        d1.start()

    @pl.when(step < STEPS)
    def _():
        rows = pl.ds(pl.multiple_of(step * NB, NB), NB)
        own_d.reshape(FF, D)[rows] = dot(dht[...], act[...]).astype(BF16).T

    @pl.when(step >= STEPS)
    def _():
        for r in pieces(4):
            dact = dot_t(dh[r], wd[...]).astype(BF16)
            dg[r], du[r] = gated_back(gate[r], up[r], dact)
        i = (step - STEPS) % SETS
        own_g[i] = wide_block(at, dg)
        own_u[i] = wide_block(at, du)

    plan = {when: [] for when in range(3 * STEPS)}
    for when, unit, stage in ((2, d1, 0), (6, d1, 1), (8, d1, 2), (10, d1, 3), (4, d, "start"), (6, d, 0), (9, d, 1), (11, d, 2), (12, d, 3)):
        plan[when].append((unit, stage))
    tail = []
    for j in range(2 * STEPS):
        k = j % SETS
        pair = [
            Reduce(BLOCK, own.at[k], out.at[:, BN * j : BN * j + BN], sets[2 + 2 * k + i], turn=(i + j) % 3)
            for i, (own, out) in enumerate(((own_g, og), (own_u, ou)))
        ]
        for n, stage in enumerate(("start", 0, 1, 2, 3)):
            when = STEPS + j + n
            late = when - (3 * STEPS - 1)
            for unit in pair:
                if late <= 0:
                    plan[when].append((unit, stage))
                else:
                    tail.append((late, unit, stage))
        last = [(unit, "finish") for unit in pair]
        if STEPS + j + 4 < 3 * STEPS:
            plan[STEPS + j + 4] += last
        else:
            tail += [(9, *entry) for entry in last]
    tail = [entry[1:] for entry in sorted(tail, key=lambda entry: entry[0])]
    plan[3 * STEPS - 1] += tail + [(d1, "finish"), (d, "finish")]
    at_end_of(step, plan)

    @pl.when(step == 3 * STEPS - 1)
    def _():
        clip_factor([g1, u1, od1, od, og, ou], factor, *rest[RS_SCRATCH * (2 + 2 * SETS) :])


def rows(cols):
    return pl.BlockSpec((TM, cols), lambda i: (i, 0))


SEQ = pl.BlockSpec((None, TM, D), lambda i: (0, i, 0))
COLUMNS = pl.BlockSpec((D, TM), lambda i: (0, i))


def weight(layer, shape):
    return pl.BlockSpec((None, *shape), lambda i: (layer, 0, 0), pipeline_mode=pl.Buffered(1))


def matrix(r, c, t=BF16):
    return jax.ShapeDtypeStruct((r, c), t)


def cost(matmuls):
    return pl.CostEstimate(flops=matmuls * 2 * TOKENS * D * FF, bytes_accessed=60 << 20, transcendentals=0)


def params(remote=False):
    return pltpu.CompilerParams(vmem_limit_bytes=60 * 1024 * 1024, has_side_effects=remote)


def shard(kind):
    return pl.BlockSpec(kind[:2], lambda i: (0, 0))


def forward(x, dy, wg, wu, wd):
    return pl.pallas_call(
        forward_kernel,
        grid=(TOKENS // TM,),
        in_specs=[SEQ, SEQ, weight(0, (D, FF)), weight(0, (D, FF)), weight(0, (FF, D))],
        out_specs=[rows(D), rows(D), COLUMNS, COLUMNS, COLUMNS, rows(FF), rows(FF), rows(FF)],
        out_shape=[matrix(TOKENS, D)] * 2 + [matrix(D, TOKENS)] * 3 + [matrix(TOKENS, FF)] + [matrix(TOKENS, FF, F32)] * 2,
        compiler_params=params(),
        cost_estimate=cost(3),
        name="forward",
    )(x, dy, wg, wu, wd)


def last(a, at, dy, dyt, h, wg, wu, wd):
    wide = pl.BlockSpec((None, D, NB), lambda i: (1, 0, i))
    straight, turned = pltpu.VMEM((TOKENS, D), BF16), pltpu.VMEM((D, TOKENS), BF16)
    hidden, sums = pltpu.VMEM((TOKENS, NB), BF16), pltpu.VMEM((TOKENS, D), F32)
    own = pltpu.VMEM((8, 2, *PAIR[:2]), BF16)
    return pl.pallas_call(
        last_kernel,
        grid=(STEPS,),
        in_specs=[ANY] * 5 + [wide, wide, pl.BlockSpec((None, NB, D), lambda i: (1, i, 0))],
        out_specs=[pl.BlockSpec((NB, D), lambda i: (i, 0)), shard(WIDE), shard(WIDE), ANY, ANY],
        out_shape=[matrix(FF, D), matrix(*WIDE[:2]), matrix(*WIDE[:2]), matrix(TOKENS, D), matrix(D, TOKENS)],
        scratch_shapes=[straight, turned, straight, turned, straight, hidden, hidden, hidden, sums, sums, own, own]
        + [pltpu.SemaphoreType.DMA((5,)), pltpu.SemaphoreType.DMA((2,))]
        + rs_scratch(PAIR, (2,)) * 2,
        compiler_params=params(True),
        cost_estimate=cost(8),
        name="last",
    )(a, at, dy.reshape(TOKENS, D), dyt, h, wg, wu, wd)


WHOLE_S = pl.BlockSpec((TOKENS, D), lambda i: (0, 0), pipeline_mode=pl.Buffered(1))
WHOLE_T = pl.BlockSpec((D, TOKENS), lambda i: (0, 0), pipeline_mode=pl.Buffered(1))


def lower(dh, dht, at, act, gate, up, wd, gd1, g1, u1):
    def later(i):
        return jnp.maximum(i - STEPS, 0)

    block = pl.BlockSpec((TOKENS, BN), lambda i: (0, later(i)))
    outs = (TALL, TALL, WIDE, WIDE)
    return pl.pallas_call(
        lower_kernel,
        grid=(3 * STEPS,),
        in_specs=[
            WHOLE_S,
            WHOLE_T,
            WHOLE_T,
            pl.BlockSpec((TOKENS, NB), lambda i: (0, jnp.minimum(i, STEPS - 1))),
            block,
            block,
            pl.BlockSpec((None, BN, D), lambda i: (0, later(i), 0)),
            ANY,
            shard(WIDE),
            shard(WIDE),
        ],
        out_specs=[shard(k) for k in outs] + [pl.BlockSpec((8, 128), lambda i: (0, 0))],
        out_shape=[matrix(*k[:2]) for k in outs] + [matrix(8, 128, F32)],
        scratch_shapes=[pltpu.VMEM((TOKENS, BN), BF16)] * 2
        + [pltpu.VMEM((SETS, 8, 2, *BLOCK[:2]), BF16)] * 2
        + [pltpu.VMEM((8, 2, *TALL[:2]), BF16), pltpu.VMEM((8, *TALL[:2]), BF16)]
        + rs_scratch(TALL) * 2
        + rs_scratch(BLOCK) * (2 * SETS)
        + CLIP_SCRATCH,
        compiler_params=params(True),
        cost_estimate=cost(4),
        name="lower",
    )(dh, dht, at, act, gate, up, wd, gd1.reshape(8, 2, *TALL[:2]), g1, u1)


def solution(mesh):
    def step(x, dy, wg, wu, wd, *moments):
        h1, a1, a1t, dyt, a0t, act0, gate0, up0 = forward(x, dy, wg, wu, wd)
        gd1, g1, u1, dh, dht = last(a1, a1t, dy, dyt, h1, wg, wu, wd)
        d1, d0, g0, u0, factor = lower(dh, dht, a0t, act0, gate0, up0, wd, gd1, g1, u1)
        own, new_moments = adamw(factor, (g0, u0, d0, g1, u1, d1), moments[:3], moments[3:], (wg, wu, wd))
        return (*all_gather(own), *new_moments)

    seq = P(("rep", "dp"), None, None)
    whole = P(None, None, None)
    part = P(None, "dp", None)
    return jax.shard_map(
        step,
        mesh=mesh,
        in_specs=(seq, seq, whole, whole, whole) + (part,) * 6,
        out_specs=(P("rep", None, None),) * 3 + (P("rep", "dp", None),) * 6,
        check_vma=False,
    )
```

```python
import functools

import jax
import jax.numpy as jnp
from jax import lax
from jax.experimental import pallas as pl
from jax.experimental.pallas import tpu as pltpu
from jax.sharding import PartitionSpec as P

MESH = pl.DeviceIdType.MESH
F32, BF16 = jnp.float32, jnp.bfloat16
DEVICES, TOKENS, D, FF = 16, 2048, 896, 2560
COUNT = 2 * 3 * D * FF
TM = 256
NB = 512
STEPS = FF // NB
BN = 256
ANY = pl.BlockSpec(memory_space=pl.ANY)
WHOLE = pl.BlockSpec(memory_space=pltpu.VMEM)

STRIDE = (8, 4, 2)
ORDER = ((0, 1, 2), (1, 2, 0), (2, 0, 1))
WIDE = (56, 2560, tuple((slice(0, 56), s) for s in (slice(0, 896), slice(896, 1792), slice(1792, 2560))))
BLOCK = (56, 256, tuple((s, slice(0, 256)) for s in (slice(0, 24), slice(24, 40), slice(40, 56))))
PAIR = (56, 512, tuple((s, slice(0, 512)) for s in (slice(0, 24), slice(24, 40), slice(40, 56))))
TALL = (160, 896, tuple((s, slice(0, 896)) for s in (slice(0, 56), slice(56, 112), slice(112, 160))))
SPLIT = tuple(
    (slice(c, c + n), (160, n, tuple((s, slice(0, n)) for s in (slice(0, 56), slice(56, 112), slice(112, 160)))))
    for c, n in ((0, 512), (512, 384))
)


def size(s):
    return s.stop - s.start


def place():
    me = lax.axis_index("dp")
    return me, (me // 8 % 2, me // 4 % 2, me // 2 % 2), me % 2


def beside(me, xyz, axis):
    return me + STRIDE[axis] * (1 - 2 * xyz[axis])


def partner(me, core):
    return me + 1 - 2 * core


def rs_scratch(kind, sets=()):
    r, c, parts = kind
    flat = [pltpu.VMEM((*sets, 8, r, c), BF16)]
    for rows, cols in parts:
        flat += [pltpu.VMEM((*sets, 7, size(rows), size(cols)), BF16)] * 2
    return flat + [pltpu.SemaphoreType.DMA((*sets, 10))] * 2 + [pltpu.SemaphoreType.DMA((*sets, 1))]


RS_SCRATCH = 10


class Reduce:
    def __init__(self, kind, g, out, scratch, own=None, turn=0):
        self.kind, self.g, self.out, self.here = kind, g, out, own is None
        self.own = g if self.here else own
        self.other = scratch[0]
        self.send, self.got = scratch[1:7:2], scratch[2:7:2]
        self.ssem, self.rsem, self.lsem = scratch[7:]
        self.me, self.xyz, self.core = place()
        self.order = ORDER[turn:] + ORDER[:turn]

    def swap(self):
        return pltpu.make_async_remote_copy(
            self.g.at[:, 1 - self.core],
            self.other,
            self.ssem.at[9],
            self.rsem.at[9],
            device_id={"dp": partner(self.me, self.core)},
            device_id_type=MESH,
        )

    def load(self):
        return pltpu.make_async_copy(self.g.at[:, self.core], self.own, self.lsem.at[0])

    def hop(self, t, phase):
        at = pl.ds((0, 4, 6)[phase], (4, 2, 1)[phase])
        return pltpu.make_async_remote_copy(
            self.send[t].at[at],
            self.got[t].at[at],
            self.ssem.at[3 * t + phase],
            self.rsem.at[3 * t + phase],
            device_id={"dp": beside(self.me, self.xyz, self.order[t][phase])},
            device_id_type=MESH,
        )

    def total(self, t, at, got):
        rows, cols = self.kind[2][t]
        block = sum(p * (4, 2, 1)[axis] for p, axis in zip(at, self.order[t], strict=True))
        own = self.own[block, self.core, rows, cols] if self.here else self.own[block, rows, cols]
        sum_ = own.astype(F32) + self.other[block, rows, cols].astype(F32)
        for i in got:
            sum_ = sum_ + self.got[t][i].astype(F32)
        return sum_

    def start(self):
        self.swap().start()
        if not self.here:
            self.load().start()

    def stage(self, n):
        if n == 0:
            if not self.here:
                self.load().wait()
            self.swap().wait_recv()
        for t in range(3):
            p1, p2, p3 = (self.xyz[axis] for axis in self.order[t])
            if n:
                self.hop(t, n - 1).wait_recv()
            if n == 0:
                for j in range(2):
                    for k in range(2):
                        self.send[t][2 * j + k] = self.total(t, (1 - p1, j, k), ()).astype(BF16)
            elif n == 1:
                for k in range(2):
                    self.send[t][4 + k] = self.total(t, (p1, 1 - p2, k), (2 * (1 - p2) + k,)).astype(BF16)
            elif n == 2:
                self.send[t][6] = self.total(t, (p1, p2, 1 - p3), (2 * p2 + 1 - p3, 5 - p3)).astype(BF16)
            else:
                rows, cols = self.kind[2][t]
                self.out[rows, cols] = self.total(t, (p1, p2, p3), (2 * p2 + p3, 4 + p3, 6)).astype(BF16)
            if n < 3:
                self.hop(t, n).start()

    def run(self, stage):
        if stage == "start":
            self.start()
        elif stage == "finish":
            self.finish()
        else:
            self.stage(stage)

    def finish(self):
        self.swap().wait_send()
        for t in range(3):
            for phase in range(3):
                self.hop(t, phase).wait_send()


def squares(g):
    wide = g.astype(F32)
    rows, cols = wide.shape
    s = jnp.sum((wide * wide).reshape(rows // 8, 8, cols), 0)
    return sum(s[:, i : i + 128] for i in range(0, cols, 128))


def clip_factor(shards, factor, squared, sums, ssem, rsem):
    me = lax.axis_index("dp")
    squared[...] = sum(squares(g[...]) for g in shards)

    def give(k, slot):
        to = (me + k) % DEVICES
        return pltpu.make_async_remote_copy(
            squared, sums.at[slot], ssem.at[k], rsem.at[slot], device_id={"dp": to}, device_id_type=MESH
        )

    for k in range(1, DEVICES):
        give(k, me).start()
    sums[me] = squared[...]
    for k in range(1, DEVICES):
        give(k, (me + k) % DEVICES).wait_recv()
    for k in range(1, DEVICES):
        give(k, me).wait_send()
    total = jnp.sum(jnp.sum(jnp.sum(sums[...], 0), 0, keepdims=True), 1, keepdims=True)
    f = jnp.minimum(1.0, 0.5 * lax.rsqrt(total / COUNT + 1e-30))
    factor[...] = jnp.broadcast_to(f, factor.shape)


CLIP_SCRATCH = [
    pltpu.VMEM((8, 128), F32),
    pltpu.VMEM((DEVICES, 8, 128), F32),
    pltpu.SemaphoreType.DMA((DEVICES,)),
    pltpu.SemaphoreType.DMA((DEVICES,)),
]


def at_end_of(step, plan):
    for when, entries in plan.items():

        @pl.when(step == when)
        def _(entries=entries):
            for unit, stage in entries:
                unit.run(stage)


class Gather:
    def __init__(self, kind, own, out, layer, ssem, rsem, csem):
        self.kind, self.own, self.out, self.layer = kind, own, out, layer
        self.ssem, self.rsem, self.csem = ssem, rsem, csem
        self.me, self.xyz, self.core = place()

    def local(self):
        x, y, z = self.xyz
        return pltpu.make_async_copy(self.own, self.out.at[self.layer, x, y, z, self.core], self.csem)

    def blocks(self, t, core, known, other=None):
        rows, cols = self.kind[2][t]
        index = []
        for axis in range(3):
            p = self.xyz[axis]
            index.append(slice(None) if axis in known else (1 - p if axis == other else p))
        return self.out.at[(self.layer, *index, core, rows, cols)]

    def hop(self, t, phase, arriving=False):
        axis = ORDER[t][phase]
        known = ORDER[t][:phase]
        src = self.blocks(t, self.core, known)
        dst = self.blocks(t, self.core, known, axis) if arriving else src
        if phase == 0 and not arriving:
            src = self.own.at[self.kind[2][t]]
        return pltpu.make_async_remote_copy(
            src,
            dst,
            self.ssem.at[3 * t + phase],
            self.rsem.at[3 * t + phase],
            device_id={"dp": beside(self.me, self.xyz, axis)},
            device_id_type=MESH,
        )

    def share(self, t, phase, core):
        ref = self.blocks(t, core, ORDER[t][:phase], ORDER[t][phase])
        return pltpu.make_async_remote_copy(
            ref,
            ref,
            self.ssem.at[10 + 3 * t + phase],
            self.rsem.at[10 + 3 * t + phase],
            device_id={"dp": partner(self.me, self.core)},
            device_id_type=MESH,
        )

    def share_own(self, core):
        x, y, z = self.xyz
        return pltpu.make_async_remote_copy(
            self.own,
            self.out.at[self.layer, x, y, z, core],
            self.ssem.at[9],
            self.rsem.at[9],
            device_id={"dp": partner(self.me, self.core)},
            device_id_type=MESH,
        )

    def start(self):
        self.local().start()
        for t in range(3):
            self.hop(t, 0).start()
        self.share_own(self.core).start()

    def stage(self, phase):
        if phase == 0:
            self.local().wait()
        for t in range(3):
            self.hop(t, phase, True).wait_recv()
            if phase < 2:
                self.hop(t, phase + 1).start()
            self.share(t, phase, self.core).start()

    def finish(self):
        self.share_own(1 - self.core).wait_recv()
        self.share_own(self.core).wait_send()
        for t in range(3):
            for phase in range(3):
                self.share(t, phase, 1 - self.core).wait_recv()
                self.share(t, phase, self.core).wait_send()
                self.hop(t, phase).wait_send()


def gather_kernel(*refs):
    owns, outs, (ssem, rsem, csem) = refs[:3], refs[3:6], refs[6:]
    units = []
    for layer in range(2):
        for i, kind in enumerate((WIDE, WIDE, TALL)):
            u = 3 * layer + i
            units.append(Gather(kind, owns[i].at[layer], outs[i], layer, ssem.at[u], rsem.at[u], csem.at[u]))
    for u in units:
        u.start()
    for phase in range(3):
        for u in units:
            u.stage(phase)
    for u in units:
        u.finish()


def all_gather(owns):
    outs = pl.pallas_call(
        gather_kernel,
        out_shape=[pltpu.VMEM((2, 2, 2, 2, 2, *o.shape[1:]), BF16) for o in owns],
        in_specs=[WHOLE] * 3,
        out_specs=[WHOLE] * 3,
        scratch_shapes=[
            pltpu.SemaphoreType.DMA((6, 19)),
            pltpu.SemaphoreType.DMA((6, 19)),
            pltpu.SemaphoreType.DMA((6,)),
        ],
        compiler_params=pltpu.CompilerParams(has_side_effects=True, vmem_limit_bytes=8 << 20),
        name="all_gather",
    )(*owns)
    outs = pl.pallas_call(
        flush_kernel,
        out_shape=[jax.ShapeDtypeStruct(o.shape, BF16) for o in outs],
        in_specs=[WHOLE] * 3,
        out_specs=[ANY] * 3,
        scratch_shapes=[pltpu.SemaphoreType.DMA((6,))],
        compiler_params=pltpu.CompilerParams(vmem_limit_bytes=1 << 20),
        name="flush",
    )(*outs)
    return [o.reshape(2, DEVICES * o.shape[-2], o.shape[-1]) for o in outs]


def flush_kernel(*refs):
    copies = []
    for i in range(3):
        for layer in range(2):
            copies.append(pltpu.make_async_copy(refs[i].at[layer], refs[3 + i].at[layer], refs[6].at[2 * i + layer]))
    for c in copies:
        c.start()
    for c in copies:
        c.wait()


KINDS = (WIDE, WIDE, TALL)


def adamw_kernel(*refs):
    factor, shards, ms, vs, weights = refs[0], refs[1:7], refs[7:10], refs[10:13], refs[13:16]
    new_ws, new_ms, new_vs = refs[16:19], refs[19:22], refs[22:25]
    in_ms, in_vs, gs, (isem, osem) = refs[25:28], refs[28:31], refs[31:34], refs[34:]
    me = lax.axis_index("dp")
    loads, stores = [], []
    for i, kind in enumerate(KINDS):
        mine = pl.ds(pl.multiple_of(me * kind[0], 8), kind[0])
        for layer in range(2):
            pairs = (
                (shards[3 * layer + i], gs[i].at[layer]),
                (ms[i].at[layer], in_ms[i].at[layer]),
                (vs[i].at[layer], in_vs[i].at[layer]),
                (weights[i].at[layer, mine], new_ws[i].at[layer]),
            )
            loads.append([pltpu.make_async_copy(src, dst, isem.at[2 * i + layer, k]) for k, (src, dst) in enumerate(pairs)])
            pairs = (in_ms[i], new_ms[i]), (in_vs[i], new_vs[i])
            stores.append(
                [
                    pltpu.make_async_copy(src.at[layer], dst.at[layer], osem.at[2 * i + layer, k])
                    for k, (src, dst) in enumerate(pairs)
                ]
            )
    for copies in loads:
        for c in copies:
            c.start()
    f = factor[0:1, 0:1]
    for u in range(6):
        i, layer = divmod(u, 2)
        for c in loads[u]:
            c.wait()
        g = gs[i][layer].astype(F32) * f
        w = new_ws[i][layer].astype(F32)
        m = 0.9 * in_ms[i][layer] + 0.1 * g
        v = 0.95 * in_vs[i][layer] + 0.05 * g * g
        step = m * lax.rsqrt(v + 1e-8) + 0.1 * w
        new_ws[i][layer], in_ms[i][layer], in_vs[i][layer] = (w - 0.02 * step).astype(BF16), m, v
        for c in stores[u]:
            c.start()
    for copies in stores:
        for c in copies:
            c.wait()


def adamw(factor, shards, ms, vs, weights):
    own = [(2, *k[:2]) for k in KINDS]
    outs = pl.pallas_call(
        adamw_kernel,
        out_shape=[pltpu.VMEM(s, BF16) for s in own] + [jax.ShapeDtypeStruct(s, F32) for s in own * 2],
        in_specs=[WHOLE] + [ANY] * 15,
        out_specs=[WHOLE] * 3 + [ANY] * 6,
        scratch_shapes=[pltpu.VMEM(s, t) for t in (F32, F32, BF16) for s in own]
        + [pltpu.SemaphoreType.DMA((6, 4)), pltpu.SemaphoreType.DMA((6, 2))],
        compiler_params=pltpu.CompilerParams(vmem_limit_bytes=60 * 1024 * 1024),
        name="adamw",
    )(factor, *shards, *ms, *vs, *weights)
    return outs[:3], outs[3:]


def dot(a, b):
    return jnp.dot(a, b, preferred_element_type=F32)


def dot_t(a, b):
    return lax.dot_general(a, b, (((1,), (1,)), ((), ())), preferred_element_type=F32)


def norm(h):
    wide = h.astype(F32)
    scale = lax.rsqrt(jnp.mean(wide * wide, -1, keepdims=True) + 1e-6)
    return wide, scale, (wide * scale).astype(BF16)


def gated_back(gate, up, dact):
    sig = jax.nn.sigmoid(gate)
    d = dact.astype(F32)
    dup = d * (gate * sig)
    dgate = d * up * (sig * (1 + gate * (1 - sig)))
    return dgate.astype(BF16), dup.astype(BF16)


def forward_kernel(x, dy, wg, wu, wd, h1, a1, a1t, dyt, at, act, gate, up):
    h = x[...]
    _, _, a = norm(h)
    at[...] = a.T
    dyt[...] = dy[...].T
    g = dot(a, wg[...])
    u = dot(a, wu[...])
    gate[...] = g
    up[...] = u
    s = (g * jax.nn.sigmoid(g) * u).astype(BF16)
    act[...] = s
    h = h + dot(s, wd[...]).astype(BF16)
    h1[...] = h
    _, _, a = norm(h)
    a1[...] = a
    a1t[...] = a.T


def pieces(count):
    n = TOKENS // count
    return [slice(n * i, n * i + n) for i in range(count)]


def wide_block(at, dg):
    return dot(at[...], dg[...]).reshape(8, 2, 56, dg.shape[-1]).astype(BF16)


def upper_kernel(a, dy, dyt, wg, wu, wd, gd, dg, du, act):
    for c in (slice(0, 256), slice(256, 512)):
        g = dot(a[...], wg[:, c])
        u = dot(a[...], wu[:, c])
        dact = dot_t(dy[...], wd[c]).astype(BF16)
        act[:, c] = (g * jax.nn.sigmoid(g) * u).astype(BF16)
        dg[:, c], du[:, c] = gated_back(g, u, dact)
        gd[c] = dot(dyt[...], act[:, c]).astype(BF16).T


LAST_SETS = 3


def last_kernel(at_in, h_in, dy, dg, du, wg, wu, gd1, og, ou, od1, out_dh, out_dht, *scratch):
    at, acc_g, acc_u, dh, own_g, own_u, half_d1, lsem, osem = scratch[:9]
    step = pl.program_id(0)
    d1 = Reduce(TALL, gd1, od1, scratch[9 : 9 + RS_SCRATCH], half_d1)

    def reduce(k, *stages):
        i = k % LAST_SETS
        rest = [ref.at[i] for ref in scratch[9 + RS_SCRATCH :]]
        columns = pl.ds(pl.multiple_of(k * NB, NB), NB)
        units = [
            Reduce(PAIR, own.at[i], out.at[:, columns], rest[RS_SCRATCH * n : RS_SCRATCH * (n + 1)], turn=n)
            for n, (own, out) in enumerate(((own_g, og), (own_u, ou)))
        ]
        for stage in stages:
            for u in units:
                u.run(stage)

    load = pltpu.make_async_copy(at_in, at, lsem.at[0])
    load_h = pltpu.make_async_copy(h_in, dh, lsem.at[1])

    @pl.when(step == 0)
    def _():
        load.start()
        load_h.start()
        d1.start()
        acc_g[...] = jnp.zeros_like(acc_g)
        acc_u[...] = jnp.zeros_like(acc_u)
        load.wait()

    i = step % LAST_SETS
    own_g[i] = wide_block(at, dg)
    own_u[i] = wide_block(at, du)

    @pl.when(step > 1)
    def _():
        reduce(step - 2, 3, "finish")

    @pl.when(step > 0)
    def _():
        reduce(step - 1, 1)

    reduce(step, "start")
    at_end_of(step, {1: [(d1, 1)], 2: [(d1, 2)], 3: [(d1, 3), (d1, "finish")]})
    blocks = [slice(c, min(c + 256, D)) for c in range(0, D, 256)]
    for c in blocks:
        acc_g[:, c] += dot_t(dg[...], wg[c])
    reduce(step, 0)
    at_end_of(step, {0: [(d1, 0)]})
    for c in blocks:
        acc_u[:, c] += dot_t(du[...], wu[c])

    @pl.when(step > 0)
    def _():
        reduce(step - 1, 2)

    @pl.when(step == STEPS - 1)
    def _():
        def through(i, carry):
            r = pl.ds(pl.multiple_of(i * 256, 256), 256)
            d = (acc_g[r].astype(BF16) + acc_u[r].astype(BF16)).astype(F32)
            wide, scale, _ = norm(dh[r])
            d = d * scale - wide * (scale * scale * scale * (jnp.sum(d * wide, -1, keepdims=True) / D))
            d = dy[r] + d.astype(BF16)
            dh[r] = d
            at[:, r] = d.T
            return carry

        load_h.wait()
        reduce(step - 1, 3, "finish")
        lax.fori_loop(0, 3, through, 0)
        reduce(step, 1)
        lax.fori_loop(3, 8, through, 0)
        stores = [pltpu.make_async_copy(s, d, osem.at[i]) for i, (s, d) in enumerate(((dh, out_dh), (at, out_dht)))]
        for c in stores:
            c.start()
        reduce(step, 2, 3, "finish")
        for c in stores:
            c.wait()


SETS = 7
LOWER_STEPS = 2 * STEPS + 2 * STEPS


def lower_kernel(dh, dht, at, act, gate, up, wd, d1, g1, u1, od, og, ou, factor, *scratch):
    step = pl.program_id(0)
    dg, du, own_g, own_u = scratch[:4]
    own_d = scratch[4:6]
    rest = scratch[6:]
    sets = [rest[RS_SCRATCH * i : RS_SCRATCH * (i + 1)] for i in range(4)]

    @pl.when(step < 2 * STEPS)
    def _():
        dact = dot_t(dh[...], wd[...]).astype(BF16)
        for r in pieces(4):
            dg[r], du[r] = gated_back(gate[r], up[r], dact[r])
        i = step % SETS
        own_g[i] = wide_block(at, dg)
        own_u[i] = wide_block(at, du)

    for part, (columns, kind) in enumerate(SPLIT):
        first = (2 + part) * STEPS

        @pl.when((step >= first) & (step < first + STEPS))
        def _(part=part, columns=columns, first=first, n=kind[1]):
            rows = pl.ds(pl.multiple_of((step - first) * NB, NB), NB)
            own_d[part].reshape(FF, n)[rows] = dot(dht[columns], act[...]).astype(BF16).T

    for late, stages in ((6, (3, "finish")), (5, (2,)), (3, (1,)), (1, (0,)), (0, ("start",))):

        @pl.when((step >= late) & (step < 2 * STEPS + late))
        def _(late=late, stages=stages):
            j = step - late
            k = j % SETS
            columns = pl.ds(pl.multiple_of(j * BN, BN), BN)
            for n, (own, out) in enumerate(((own_g, og), (own_u, ou))):
                unit = Reduce(BLOCK, own.at[k], out.at[:, columns], [ref.at[k] for ref in sets[2 + n]], turn=n)
                for stage in stages:
                    unit.run(stage)

    plan = {when: [] for when in (3 * STEPS - 1, 3 * STEPS + 2, LOWER_STEPS - 1)}
    da, db = (
        Reduce(kind, own_d[part], od.at[:, columns], sets[part], turn=1 + part) for part, (columns, kind) in enumerate(SPLIT)
    )
    plan[3 * STEPS - 1] += [(da, "start")]
    plan[3 * STEPS + 2] += [(da, 0)]
    plan[LOWER_STEPS - 1] += [(db, "start"), (da, 1), (db, 0), (da, 2), (db, 1), (da, 3), (db, 2), (db, 3)]
    plan[LOWER_STEPS - 1] += [(da, "finish"), (db, "finish")]
    at_end_of(step, plan)

    @pl.when(step == LOWER_STEPS - 1)
    def _():
        clip_factor([d1, g1, u1, od, og, ou], factor, *rest[RS_SCRATCH * 4 :])


def rows(cols):
    return pl.BlockSpec((TM, cols), lambda i: (i, 0))


SEQ = pl.BlockSpec((None, TM, D), lambda i: (0, i, 0))
COLUMNS = pl.BlockSpec((D, TM), lambda i: (0, i))


def weight(layer, shape):
    return pl.BlockSpec((None, *shape), lambda i: (layer, 0, 0), pipeline_mode=pl.Buffered(1))


def matrix(r, c, t=BF16):
    return jax.ShapeDtypeStruct((r, c), t)


def cost(matmuls):
    return pl.CostEstimate(flops=matmuls * 2 * TOKENS * D * FF, bytes_accessed=60 << 20, transcendentals=0)


def params(remote=False):
    return pltpu.CompilerParams(vmem_limit_bytes=67043328 if remote else 60 * 1024 * 1024, has_side_effects=remote)


def shard(kind):
    return pl.BlockSpec(kind[:2], lambda i: (0, 0))


def forward(x, dy, wg, wu, wd):
    return pl.pallas_call(
        forward_kernel,
        grid=(TOKENS // TM,),
        in_specs=[SEQ, SEQ, weight(0, (D, FF)), weight(0, (D, FF)), weight(0, (FF, D))],
        out_specs=[rows(D), rows(D), COLUMNS, COLUMNS, COLUMNS, rows(FF), rows(FF), rows(FF)],
        out_shape=[matrix(TOKENS, D)] * 2 + [matrix(D, TOKENS)] * 3 + [matrix(TOKENS, FF)] + [matrix(TOKENS, FF, F32)] * 2,
        compiler_params=params(),
        cost_estimate=cost(3),
        name="forward",
    )(x, dy, wg, wu, wd)


WHOLE_S = pl.BlockSpec((TOKENS, D), lambda i: (0, 0), pipeline_mode=pl.Buffered(1))
WHOLE_T = pl.BlockSpec((D, TOKENS), lambda i: (0, 0), pipeline_mode=pl.Buffered(1))
HIDDEN = pl.BlockSpec((TOKENS, NB), lambda i: (0, i))
WIDE_W = pl.BlockSpec((None, D, NB), lambda i: (1, 0, i))


def upper(a, dy, dyt, wg, wu, wd):
    return pl.pallas_call(
        upper_kernel,
        grid=(STEPS,),
        in_specs=[WHOLE_S, WHOLE_S, WHOLE_T, WIDE_W, WIDE_W, pl.BlockSpec((None, NB, D), lambda i: (1, i, 0))],
        out_specs=[pl.BlockSpec((NB, D), lambda i: (i, 0)), HIDDEN, HIDDEN],
        out_shape=[matrix(FF, D), matrix(TOKENS, FF), matrix(TOKENS, FF)],
        scratch_shapes=[pltpu.VMEM((TOKENS, NB), BF16)],
        compiler_params=params(),
        cost_estimate=cost(4),
        name="upper",
    )(a, dy, dyt, wg, wu, wd)


def last(at, h, dy, dg, du, wg, wu, gd1):
    straight, turned, sums = pltpu.VMEM((TOKENS, D), BF16), pltpu.VMEM((D, TOKENS), BF16), pltpu.VMEM((TOKENS, D), F32)
    own = pltpu.VMEM((LAST_SETS, 8, 2, *PAIR[:2]), BF16)
    return pl.pallas_call(
        last_kernel,
        grid=(STEPS,),
        in_specs=[ANY, ANY, WHOLE_S, HIDDEN, HIDDEN, WIDE_W, WIDE_W, ANY],
        out_specs=[shard(WIDE), shard(WIDE), shard(TALL), ANY, ANY],
        out_shape=[matrix(*k[:2]) for k in (WIDE, WIDE, TALL)] + [matrix(TOKENS, D), matrix(D, TOKENS)],
        scratch_shapes=[turned, sums, sums, straight, own, own, pltpu.VMEM((8, *TALL[:2]), BF16)]
        + [pltpu.SemaphoreType.DMA((2,)), pltpu.SemaphoreType.DMA((2,))]
        + rs_scratch(TALL)
        + rs_scratch(PAIR, (LAST_SETS,)) * 2,
        compiler_params=params(True),
        cost_estimate=cost(4),
        name="last",
    )(at, h, dy, dg, du, wg, wu, gd1.reshape(8, 2, *TALL[:2]))


def lower(dh, dht, at, act, gate, up, wd, shards):
    def column(i):
        return jnp.minimum(i, 2 * STEPS - 1)

    block = pl.BlockSpec((TOKENS, BN), lambda i: (0, column(i)))
    outs = (TALL, WIDE, WIDE)
    return pl.pallas_call(
        lower_kernel,
        grid=(LOWER_STEPS,),
        in_specs=[
            WHOLE_S,
            WHOLE_T,
            WHOLE_T,
            pl.BlockSpec((TOKENS, NB), lambda i: (0, jnp.maximum(i - 2 * STEPS, 0) % STEPS)),
            block,
            block,
            pl.BlockSpec((None, BN, D), lambda i: (0, column(i), 0)),
            shard(TALL),
            shard(WIDE),
            shard(WIDE),
        ],
        out_specs=[shard(k) for k in outs] + [pl.BlockSpec((8, 128), lambda i: (0, 0))],
        out_shape=[matrix(*k[:2]) for k in outs] + [matrix(8, 128, F32)],
        scratch_shapes=[pltpu.VMEM((TOKENS, BN), BF16)] * 2
        + [pltpu.VMEM((SETS, 8, 2, *BLOCK[:2]), BF16)] * 2
        + [pltpu.VMEM((8, 2, *kind[:2]), BF16) for _, kind in SPLIT]
        + sum((rs_scratch(kind) for _, kind in SPLIT), [])
        + rs_scratch(BLOCK, (SETS,)) * 2
        + CLIP_SCRATCH,
        compiler_params=params(True),
        cost_estimate=cost(4),
        name="lower",
    )(dh, dht, at, act, gate, up, wd, *shards)


def solution(mesh):
    def step(x, dy, wg, wu, wd, *moments):
        h1, a1, a1t, dyt, a0t, act0, gate0, up0 = forward(x, dy, wg, wu, wd)
        flat_dy = dy.reshape(TOKENS, D)
        gd1, dg1, du1 = upper(a1, flat_dy, dyt, wg, wu, wd)
        g1, u1, d1, dh, dht = last(a1t, h1, flat_dy, dg1, du1, wg, wu, gd1)
        d0, g0, u0, factor = lower(dh, dht, a0t, act0, gate0, up0, wd, (d1, g1, u1))
        own, new_moments = adamw(factor, (g0, u0, d0, g1, u1, d1), moments[:3], moments[3:], (wg, wu, wd))
        return (*all_gather(own), *new_moments)

    seq = P(("rep", "dp"), None, None)
    whole = P(None, None, None)
    part = P(None, "dp", None)
    return jax.shard_map(
        step,
        mesh=mesh,
        in_specs=(seq, seq, whole, whole, whole) + (part,) * 6,
        out_specs=(P("rep", None, None),) * 3 + (P("rep", "dp", None),) * 6,
        check_vma=False,
    )
```

```python
import functools

import jax
import jax.numpy as jnp
from jax import lax
from jax.experimental import pallas as pl
from jax.experimental.pallas import tpu as pltpu
from jax.sharding import PartitionSpec as P

MESH = pl.DeviceIdType.MESH
F32, BF16 = jnp.float32, jnp.bfloat16
DEVICES, TOKENS, D, FF = 16, 2048, 896, 2560
COUNT = 2 * 3 * D * FF
TM = 256
Z = 0
NB = 512
STEPS = FF // NB
BN = 256
ANY = pl.BlockSpec(memory_space=pl.ANY)
WHOLE = pl.BlockSpec(memory_space=pltpu.VMEM)

STRIDE = (8, 4, 2)
ORDER = ((0, 1, 2), (1, 2, 0), (2, 0, 1))
def cuts(*at):
    return [slice(*pair) for pair in zip(at, at[1:])]


WIDE = (56, FF, tuple((slice(Z, 56), s) for s in cuts(Z, 896, 1792, FF)))
BOTH = (56, 1024, tuple((slice(Z, 56), s) for s in cuts(Z, 384, 768, 1024)))
TALL = (160, D, tuple((s, slice(Z, D)) for s in cuts(Z, 56, 112, 160)))
SPLIT = tuple(
    (slice(c, c + n), (160, n, tuple((s, slice(Z, n)) for s in cuts(Z, 56, 112, 160))))
    for c, n in ((0, 512), (512, 384))
)


def size(s):
    return s.stop - s.start


def place():
    me = lax.axis_index("dp")
    return me, (me // 8 % 2, me // 4 % 2, me // 2 % 2), me % 2


def beside(me, xyz, axis):
    return me + STRIDE[axis] * (1 - 2 * xyz[axis])


def partner(me, core):
    return me + 1 - 2 * core


def rs_scratch(kind, sets=()):
    r, c, parts = kind
    flat = [pltpu.VMEM((*sets, 8, r, c), BF16)]
    for rows, cols in parts:
        flat += [pltpu.VMEM((*sets, 7, size(rows), size(cols)), BF16)] * 2
    return flat + [pltpu.SemaphoreType.DMA((*sets, 10))] * 2 + [pltpu.SemaphoreType.DMA((*sets, 1))]


RS_SCRATCH = 10


class Reduce:
    def __init__(self, kind, g, out, scratch, own=None, turn=0):
        self.kind, self.g, self.out, self.here = kind, g, out, own is None
        self.own = g if self.here else own
        self.other = scratch[0]
        self.send, self.got = scratch[1:7:2], scratch[2:7:2]
        self.ssem, self.rsem, self.lsem = scratch[7:]
        self.me, self.xyz, self.core = place()
        self.order = ORDER[turn:] + ORDER[:turn]

    def swap(self):
        return pltpu.make_async_remote_copy(
            self.g.at[:, 1 - self.core],
            self.other,
            self.ssem.at[9],
            self.rsem.at[9],
            device_id={"dp": partner(self.me, self.core)},
            device_id_type=MESH,
        )

    def load(self):
        return pltpu.make_async_copy(self.g.at[:, self.core], self.own, self.lsem.at[0])

    def hop(self, t, phase):
        at = pl.ds((0, 4, 6)[phase], (4, 2, 1)[phase])
        return pltpu.make_async_remote_copy(
            self.send[t].at[at],
            self.got[t].at[at],
            self.ssem.at[3 * t + phase],
            self.rsem.at[3 * t + phase],
            device_id={"dp": beside(self.me, self.xyz, self.order[t][phase])},
            device_id_type=MESH,
        )

    def total(self, t, at, got):
        rows, cols = self.kind[2][t]
        block = sum(p * (4, 2, 1)[axis] for p, axis in zip(at, self.order[t], strict=True))
        own = self.own[block, self.core, rows, cols] if self.here else self.own[block, rows, cols]
        sum_ = own.astype(F32) + self.other[block, rows, cols].astype(F32)
        for i in got:
            sum_ = sum_ + self.got[t][i].astype(F32)
        return sum_

    def start(self):
        self.swap().start()
        if not self.here:
            self.load().start()

    def stage(self, n):
        if n == 0:
            if not self.here:
                self.load().wait()
            self.swap().wait_recv()
        for t in range(3):
            p1, p2, p3 = (self.xyz[axis] for axis in self.order[t])
            if n:
                self.hop(t, n - 1).wait_recv()
            if n == 0:
                for j in range(2):
                    for k in range(2):
                        self.send[t][2 * j + k] = self.total(t, (1 - p1, j, k), ()).astype(BF16)
            elif n == 1:
                for k in range(2):
                    self.send[t][4 + k] = self.total(t, (p1, 1 - p2, k), (2 * (1 - p2) + k,)).astype(BF16)
            elif n == 2:
                self.send[t][6] = self.total(t, (p1, p2, 1 - p3), (2 * p2 + 1 - p3, 5 - p3)).astype(BF16)
            else:
                rows, cols = self.kind[2][t]
                self.out[rows, cols] = self.total(t, (p1, p2, p3), (2 * p2 + p3, 4 + p3, 6)).astype(BF16)
            if n < 3:
                self.hop(t, n).start()

    def run(self, stage):
        if stage == "start":
            self.start()
        elif stage == "finish":
            self.finish()
        else:
            self.stage(stage)

    def finish(self):
        self.swap().wait_send()
        for t in range(3):
            for phase in range(3):
                self.hop(t, phase).wait_send()


def squares(g):
    wide = g.astype(F32).reshape(-1, g.shape[-1])
    rows, cols = wide.shape
    s = jnp.sum((wide * wide).reshape(rows // 8, 8, cols), 0)
    return sum(s[:, i : i + 128] for i in range(0, cols, 128))


def clip_factor(shards, factor, squared, sums, ssem, rsem):
    me = lax.axis_index("dp")
    squared[...] = sum(squares(g[...]) for g in shards)

    def give(k, slot):
        to = (me + k) % DEVICES
        return pltpu.make_async_remote_copy(
            squared, sums.at[slot], ssem.at[k], rsem.at[slot], device_id={"dp": to}, device_id_type=MESH
        )

    for k in range(1, DEVICES):
        give(k, me).start()
    sums[me] = squared[...]
    for k in range(1, DEVICES):
        give(k, (me + k) % DEVICES).wait_recv()
    for k in range(1, DEVICES):
        give(k, me).wait_send()
    total = jnp.sum(jnp.sum(jnp.sum(sums[...], 0), 0, keepdims=True), 1, keepdims=True)
    f = jnp.minimum(1.0, 0.5 * lax.rsqrt(total / COUNT + 1e-30))
    factor[...] = jnp.broadcast_to(f, factor.shape)


CLIP_SCRATCH = [
    pltpu.VMEM((8, 128), F32),
    pltpu.VMEM((DEVICES, 8, 128), F32),
    pltpu.SemaphoreType.DMA((DEVICES,)),
    pltpu.SemaphoreType.DMA((DEVICES,)),
]


def at_end_of(step, plan):
    for when, entries in plan.items():

        @pl.when(step == when)
        def _(entries=entries):
            for unit, stage in entries:
                unit.run(stage)


class Gather:
    def __init__(self, kind, own, out, ssem, rsem, csem):
        self.kind, self.own, self.out = kind, own, out
        self.ssem, self.rsem, self.csem = ssem, rsem, csem
        self.me, self.xyz, self.core = place()

    def local(self):
        x, y, z = self.xyz
        return pltpu.make_async_copy(self.own, self.out.at[:, x, y, z, self.core], self.csem)

    def blocks(self, t, core, known, other=None):
        rows, cols = self.kind[2][t]
        index = []
        for axis in range(3):
            p = self.xyz[axis]
            index.append(slice(None) if axis in known else (1 - p if axis == other else p))
        return self.out.at[(slice(None), *index, core, rows, cols)]

    def hop(self, t, phase, arriving=False):
        axis = ORDER[t][phase]
        known = ORDER[t][:phase]
        src = self.blocks(t, self.core, known)
        dst = self.blocks(t, self.core, known, axis) if arriving else src
        if phase == 0 and not arriving:
            src = self.own.at[(slice(None), *self.kind[2][t])]
        return pltpu.make_async_remote_copy(
            src,
            dst,
            self.ssem.at[3 * t + phase],
            self.rsem.at[3 * t + phase],
            device_id={"dp": beside(self.me, self.xyz, axis)},
            device_id_type=MESH,
        )

    def share(self, t, phase, core):
        ref = self.blocks(t, core, ORDER[t][:phase], ORDER[t][phase])
        return pltpu.make_async_remote_copy(
            ref,
            ref,
            self.ssem.at[10 + 3 * t + phase],
            self.rsem.at[10 + 3 * t + phase],
            device_id={"dp": partner(self.me, self.core)},
            device_id_type=MESH,
        )

    def share_own(self, core):
        x, y, z = self.xyz
        return pltpu.make_async_remote_copy(
            self.own,
            self.out.at[:, x, y, z, core],
            self.ssem.at[9],
            self.rsem.at[9],
            device_id={"dp": partner(self.me, self.core)},
            device_id_type=MESH,
        )

    def start(self):
        self.local().start()
        for t in range(3):
            self.hop(t, 0).start()
        self.share_own(self.core).start()

    def stage(self, phase):
        if phase == 0:
            self.local().wait()
        for t in range(3):
            self.hop(t, phase, True).wait_recv()
            if phase < 2:
                self.hop(t, phase + 1).start()
            self.share(t, phase, self.core).start()

    def finish(self):
        self.share_own(1 - self.core).wait_recv()
        self.share_own(self.core).wait_send()
        for t in range(3):
            for phase in range(3):
                self.share(t, phase, 1 - self.core).wait_recv()
                self.share(t, phase, self.core).wait_send()
                self.hop(t, phase).wait_send()


def gather_kernel(*refs):
    owns, outs, (ssem, rsem, csem) = refs[:3], refs[3:6], refs[6:]
    units = [Gather(kind, owns[i], outs[i], ssem.at[i], rsem.at[i], csem.at[i]) for i, kind in enumerate((WIDE, WIDE, TALL))]
    for u in units:
        u.start()
    for phase in range(3):
        for u in units:
            u.stage(phase)
    for u in units:
        u.finish()


def all_gather(owns):
    outs = pl.pallas_call(
        gather_kernel,
        out_shape=[pltpu.VMEM((2, 2, 2, 2, 2, *o.shape[1:]), BF16) for o in owns],
        in_specs=[WHOLE] * 3,
        out_specs=[WHOLE] * 3,
        scratch_shapes=[
            pltpu.SemaphoreType.DMA((3, 19)),
            pltpu.SemaphoreType.DMA((3, 19)),
            pltpu.SemaphoreType.DMA((3,)),
        ],
        compiler_params=pltpu.CompilerParams(has_side_effects=True, vmem_limit_bytes=8 << 20),
        name="all_gather",
    )(*owns)
    outs = pl.pallas_call(
        flush_kernel,
        out_shape=[jax.ShapeDtypeStruct(o.shape, BF16) for o in outs],
        in_specs=[WHOLE] * 3,
        out_specs=[ANY] * 3,
        scratch_shapes=[pltpu.SemaphoreType.DMA((6,))],
        compiler_params=pltpu.CompilerParams(vmem_limit_bytes=1 << 20),
        name="flush",
    )(*outs)
    return [o.reshape(2, DEVICES * o.shape[-2], o.shape[-1]) for o in outs]


def flush_kernel(*refs):
    copies = []
    for i in range(3):
        for layer in range(2):
            copies.append(pltpu.make_async_copy(refs[i].at[layer], refs[3 + i].at[layer], refs[6].at[2 * i + layer]))
    for c in copies:
        c.start()
    for c in copies:
        c.wait()


KINDS = (WIDE, WIDE, TALL)


def adamw_kernel(*refs):
    factor, shards, ms, vs, weights = refs[0], refs[1:5], refs[5:8], refs[8:11], refs[11:14]
    new_ws, new_ms, new_vs = refs[14:17], refs[17:20], refs[20:23]
    in_ms, in_vs, gs, (isem, osem) = refs[23:26], refs[26:29], refs[29:32], refs[32:]
    me = lax.axis_index("dp")
    loads, stores = [], []
    for i, kind in enumerate(KINDS):
        mine = pl.ds(pl.multiple_of(me * kind[0], 8), kind[0])
        for layer in range(2):
            pairs = [
                (ms[i].at[layer], in_ms[i].at[layer]),
                (vs[i].at[layer], in_vs[i].at[layer]),
                (weights[i].at[layer, mine], new_ws[i].at[layer]),
            ]
            if kind is TALL:
                pairs.append((shards[2 * layer + 1], gs[i].at[layer]))
            else:
                at = slice(i * NB, i * NB + NB)
                pairs += [
                    (shards[2 * layer].at[k, :, at], gs[i].at[layer, :, k * NB : k * NB + NB]) for k in range(STEPS)
                ]
            loads.append([pltpu.make_async_copy(src, dst, isem.at[2 * i + layer, k]) for k, (src, dst) in enumerate(pairs)])
            pairs = (in_ms[i], new_ms[i]), (in_vs[i], new_vs[i])
            stores.append(
                [
                    pltpu.make_async_copy(src.at[layer], dst.at[layer], osem.at[2 * i + layer, k])
                    for k, (src, dst) in enumerate(pairs)
                ]
            )
    for copies in loads:
        for c in copies:
            c.start()
    f = factor[0:1, 0:1]
    for u in range(6):
        i, layer = divmod(u, 2)
        for c in loads[u]:
            c.wait()
        g = gs[i][layer].astype(F32) * f
        w = new_ws[i][layer].astype(F32)
        m = 0.9 * in_ms[i][layer] + 0.1 * g
        v = 0.95 * in_vs[i][layer] + 0.05 * g * g
        step = m * lax.rsqrt(v + 1e-8) + 0.1 * w
        new_ws[i][layer], in_ms[i][layer], in_vs[i][layer] = (w - 0.02 * step).astype(BF16), m, v
        for c in stores[u]:
            c.start()
    for copies in stores:
        for c in copies:
            c.wait()


def adamw(factor, shards, ms, vs, weights):
    own = [(2, *k[:2]) for k in KINDS]
    outs = pl.pallas_call(
        adamw_kernel,
        out_shape=[pltpu.VMEM(s, BF16) for s in own] + [jax.ShapeDtypeStruct(s, F32) for s in own * 2],
        in_specs=[WHOLE] + [ANY] * 13,
        out_specs=[WHOLE] * 3 + [ANY] * 6,
        scratch_shapes=[pltpu.VMEM(s, t) for t in (F32, F32, BF16) for s in own]
        + [pltpu.SemaphoreType.DMA((6, 8)), pltpu.SemaphoreType.DMA((6, 2))],
        compiler_params=pltpu.CompilerParams(vmem_limit_bytes=60 * 1024 * 1024),
        name="adamw",
    )(factor, *shards, *ms, *vs, *weights)
    return outs[:3], outs[3:]


def dot(a, b):
    return jnp.dot(a, b, preferred_element_type=F32)


def dot_t(a, b):
    return lax.dot_general(a, b, (((1,), (1,)), ((), ())), preferred_element_type=F32)


def norm(h):
    wide = h.astype(F32)
    scale = lax.rsqrt(jnp.mean(wide * wide, -1, keepdims=True) + 1e-6)
    return wide, scale, (wide * scale).astype(BF16)


def gated_back(gate, up, dact):
    sig = jax.nn.sigmoid(gate)
    d = dact.astype(F32)
    dup = d * (gate * sig)
    dgate = d * up * (sig * (1 + gate * (1 - sig)))
    return dgate.astype(BF16), dup.astype(BF16)


def forward_kernel(x, dy, wg, wu, wd, h1, a1, a1t, dyt, at, act, gate, up):
    h = x[...]
    _, _, a = norm(h)
    at[...] = a.T
    dyt[...] = dy[...].T
    g = dot(a, wg[...])
    u = dot(a, wu[...])
    gate[...] = g
    up[...] = u
    s = (g * jax.nn.sigmoid(g) * u).astype(BF16)
    act[...] = s
    h = h + dot(s, wd[...]).astype(BF16)
    h1[...] = h
    _, _, a = norm(h)
    a1[...] = a
    a1t[...] = a.T


def pieces(count):
    n = TOKENS // count
    return [slice(n * i, n * i + n) for i in range(count)]


def wide_block(at, dg):
    return dot(at[...], dg[...]).reshape(8, 2, 56, dg.shape[-1]).astype(BF16)


def upper_kernel(a, dy, dyt, wg, wu, wd, gd, dg, du, act):
    for c in (slice(0, 256), slice(256, 512)):
        g = dot(a[...], wg[:, c])
        u = dot(a[...], wu[:, c])
        dact = dot_t(dy[...], wd[c]).astype(BF16)
        act[:, c] = (g * jax.nn.sigmoid(g) * u).astype(BF16)
        dg[:, c], du[:, c] = gated_back(g, u, dact)
        gd[c] = dot(dyt[...], act[:, c]).astype(BF16).T


LAST_SETS = 3


def last_kernel(at_in, h_in, dy, dg, du, wg, wu, gd1, ogu, od1, out_dh, out_dht, *scratch):
    at, acc_g, acc_u, dh, own, half_d1, lsem, osem = scratch[:8]
    step = pl.program_id(0)
    d1 = Reduce(TALL, gd1, od1, scratch[8 : 8 + RS_SCRATCH], half_d1)

    def reduce(k, *stages):
        i = k % LAST_SETS
        unit = Reduce(BOTH, own.at[i], ogu.at[k], [ref.at[i] for ref in scratch[8 + RS_SCRATCH :]])
        for stage in stages:
            unit.run(stage)

    load = pltpu.make_async_copy(at_in, at, lsem.at[0])
    load_h = pltpu.make_async_copy(h_in, dh, lsem.at[1])

    @pl.when(step == 0)
    def _():
        load.start()
        load_h.start()
        d1.start()
        acc_g[...] = jnp.zeros_like(acc_g)
        acc_u[...] = jnp.zeros_like(acc_u)
        load.wait()

    i = step % LAST_SETS
    own[i, :, :, :, :NB] = wide_block(at, dg)
    own[i, :, :, :, NB:] = wide_block(at, du)

    @pl.when(step > 1)
    def _():
        reduce(step - 2, 3, "finish")

    @pl.when(step > 0)
    def _():
        reduce(step - 1, 1)

    reduce(step, "start")
    at_end_of(step, {1: [(d1, 1)], 2: [(d1, 2)], 3: [(d1, 3), (d1, "finish")]})
    blocks = [slice(c, min(c + 256, D)) for c in range(0, D, 256)]
    for c in blocks:
        acc_g[:, c] += dot_t(dg[...], wg[c])
    reduce(step, 0)
    at_end_of(step, {0: [(d1, 0)]})
    for c in blocks:
        acc_u[:, c] += dot_t(du[...], wu[c])

    @pl.when(step > 0)
    def _():
        reduce(step - 1, 2)

    @pl.when(step == STEPS - 1)
    def _():
        def through(i, carry):
            r = pl.ds(pl.multiple_of(i * 256, 256), 256)
            d = (acc_g[r].astype(BF16) + acc_u[r].astype(BF16)).astype(F32)
            wide, scale, _ = norm(dh[r])
            d = d * scale - wide * (scale * scale * scale * (jnp.sum(d * wide, -1, keepdims=True) / D))
            d = dy[r] + d.astype(BF16)
            dh[r] = d
            at[:, r] = d.T
            return carry

        load_h.wait()
        reduce(step - 1, 3, "finish")
        lax.fori_loop(0, 3, through, 0)
        reduce(step, 1)
        lax.fori_loop(3, 8, through, 0)
        stores = [pltpu.make_async_copy(s, d, osem.at[i]) for i, (s, d) in enumerate(((dh, out_dh), (at, out_dht)))]
        for c in stores:
            c.start()
        reduce(step, 2, 3, "finish")
        for c in stores:
            c.wait()


SETS = 4
LOWER_STEPS = 4 * STEPS


def lower_kernel(dh, dht, at, act, gate, up, wd, d1, gu1, od, ogu, factor, *scratch):
    step = pl.program_id(0)
    dg, du, own = scratch[:3]
    own_d = scratch[3:5]
    rest = scratch[5:]
    sets = [rest[RS_SCRATCH * i : RS_SCRATCH * (i + 1)] for i in range(3)]

    @pl.when(step < 2 * STEPS)
    def _():
        dact = dot_t(dh[...], wd[...]).astype(BF16)
        for r in pieces(4):
            dg[r], du[r] = gated_back(gate[r], up[r], dact[r])
        i = step // 2 % SETS
        for first, grad in ((0, dg), (NB, du)):
            own[i, :, :, :, pl.ds(pl.multiple_of(first + step % 2 * BN, BN), BN)] = wide_block(at, grad)

    for part, (columns, kind) in enumerate(SPLIT):
        first = (2 + part) * STEPS

        @pl.when((step >= first) & (step < first + STEPS))
        def _(part=part, columns=columns, first=first, n=kind[1]):
            rows = pl.ds(pl.multiple_of((step - first) * NB, NB), NB)
            own_d[part].reshape(FF, n)[rows] = dot(dht[columns], act[...]).astype(BF16).T

    for late, stages in ((7, (3, "finish")), (6, (2,)), (4, (1,)), (2, (0,)), (1, ("start",))):

        @pl.when((step >= late) & (step < 2 * STEPS + late) & ((step - late) % 2 == 0))
        def _(late=late, stages=stages):
            j = (step - late) // 2
            k = j % SETS
            unit = Reduce(BOTH, own.at[k], ogu.at[j], [ref.at[k] for ref in sets[2]])
            for stage in stages:
                unit.run(stage)

    plan = {when: [] for when in (3 * STEPS - 1, 3 * STEPS + 2, LOWER_STEPS - 1)}
    da, db = (
        Reduce(kind, own_d[part], od.at[:, columns], sets[part], turn=1 + part) for part, (columns, kind) in enumerate(SPLIT)
    )
    plan[3 * STEPS - 1] += [(da, "start")]
    plan[3 * STEPS + 2] += [(da, 0)]
    plan[LOWER_STEPS - 1] += [(db, "start"), (da, 1), (db, 0), (da, 2), (db, 1), (da, 3), (db, 2), (db, 3)]
    plan[LOWER_STEPS - 1] += [(da, "finish"), (db, "finish")]
    at_end_of(step, plan)

    @pl.when(step == LOWER_STEPS - 1)
    def _():
        clip_factor([d1, gu1, od, ogu], factor, *rest[RS_SCRATCH * 3 :])


def rows(cols):
    return pl.BlockSpec((TM, cols), lambda i: (i, Z))


SEQ = pl.BlockSpec((None, TM, D), lambda i: (Z, i, Z))
COLUMNS = pl.BlockSpec((D, TM), lambda i: (Z, i))


def weight(layer, shape):
    return pl.BlockSpec((None, *shape), lambda i: (layer, Z, Z), pipeline_mode=pl.Buffered(1))


def matrix(r, c, t=BF16):
    return jax.ShapeDtypeStruct((r, c), t)


def cost(matmuls):
    return pl.CostEstimate(flops=matmuls * 2 * TOKENS * D * FF, bytes_accessed=60 << 20, transcendentals=0)


def params(remote=False):
    return pltpu.CompilerParams(vmem_limit_bytes=67043328 if remote else 60 * 1024 * 1024, has_side_effects=remote)


def shard(kind):
    return pl.BlockSpec(kind[:2], lambda i: (Z, Z))


SHARDS = (STEPS, *BOTH[:2])
BOTH_SHARD = pl.BlockSpec(SHARDS, lambda i: (Z, Z, Z))


def forward(x, dy, wg, wu, wd):
    return pl.pallas_call(
        forward_kernel,
        grid=(TOKENS // TM,),
        in_specs=[SEQ, SEQ, weight(0, (D, FF)), weight(0, (D, FF)), weight(0, (FF, D))],
        out_specs=[rows(D), rows(D), COLUMNS, COLUMNS, COLUMNS, rows(FF), rows(FF), rows(FF)],
        out_shape=[matrix(TOKENS, D)] * 2 + [matrix(D, TOKENS)] * 3 + [matrix(TOKENS, FF)] + [matrix(TOKENS, FF, F32)] * 2,
        compiler_params=params(),
        cost_estimate=cost(3),
        name="forward",
    )(x, dy, wg, wu, wd)


WHOLE_S = pl.BlockSpec((TOKENS, D), lambda i: (Z, Z), pipeline_mode=pl.Buffered(1))
WHOLE_T = pl.BlockSpec((D, TOKENS), lambda i: (Z, Z), pipeline_mode=pl.Buffered(1))
HIDDEN = pl.BlockSpec((TOKENS, NB), lambda i: (Z, i))
WIDE_W = pl.BlockSpec((None, D, NB), lambda i: (1, Z, i))


def upper(a, dy, dyt, wg, wu, wd):
    return pl.pallas_call(
        upper_kernel,
        grid=(STEPS,),
        in_specs=[WHOLE_S, WHOLE_S, WHOLE_T, WIDE_W, WIDE_W, pl.BlockSpec((None, NB, D), lambda i: (1, i, Z))],
        out_specs=[pl.BlockSpec((NB, D), lambda i: (i, Z)), HIDDEN, HIDDEN],
        out_shape=[matrix(FF, D), matrix(TOKENS, FF), matrix(TOKENS, FF)],
        scratch_shapes=[pltpu.VMEM((TOKENS, NB), BF16)],
        compiler_params=params(),
        cost_estimate=cost(4),
        name="upper",
    )(a, dy, dyt, wg, wu, wd)


def last(at, h, dy, dg, du, wg, wu, gd1):
    straight, turned, sums = pltpu.VMEM((TOKENS, D), BF16), pltpu.VMEM((D, TOKENS), BF16), pltpu.VMEM((TOKENS, D), F32)
    own = pltpu.VMEM((LAST_SETS, 8, 2, *BOTH[:2]), BF16)
    return pl.pallas_call(
        last_kernel,
        grid=(STEPS,),
        in_specs=[ANY, ANY, WHOLE_S, HIDDEN, HIDDEN, WIDE_W, WIDE_W, ANY],
        out_specs=[BOTH_SHARD, shard(TALL), ANY, ANY],
        out_shape=[jax.ShapeDtypeStruct(SHARDS, BF16), matrix(*TALL[:2]), matrix(TOKENS, D), matrix(D, TOKENS)],
        scratch_shapes=[turned, sums, sums, straight, own, pltpu.VMEM((8, *TALL[:2]), BF16)]
        + [pltpu.SemaphoreType.DMA((2,)), pltpu.SemaphoreType.DMA((2,))]
        + rs_scratch(TALL)
        + rs_scratch(BOTH, (LAST_SETS,)),
        compiler_params=params(True),
        cost_estimate=cost(4),
        name="last",
    )(at, h, dy, dg, du, wg, wu, gd1.reshape(8, 2, *TALL[:2]))


def lower(dh, dht, at, act, gate, up, wd, shards):
    def column(i):
        return jnp.minimum(i, 2 * STEPS - 1)

    block = pl.BlockSpec((TOKENS, BN), lambda i: (Z, column(i)))
    return pl.pallas_call(
        lower_kernel,
        grid=(LOWER_STEPS,),
        in_specs=[
            WHOLE_S,
            WHOLE_T,
            WHOLE_T,
            pl.BlockSpec((TOKENS, NB), lambda i: (Z, jnp.maximum(i - 2 * STEPS, Z) % STEPS)),
            block,
            block,
            pl.BlockSpec((None, BN, D), lambda i: (Z, column(i), Z)),
            shard(TALL),
            BOTH_SHARD,
        ],
        out_specs=[shard(TALL), BOTH_SHARD, pl.BlockSpec((8, 128), lambda i: (Z, Z))],
        out_shape=[matrix(*TALL[:2]), jax.ShapeDtypeStruct(SHARDS, BF16), matrix(8, 128, F32)],
        scratch_shapes=[pltpu.VMEM((TOKENS, BN), BF16)] * 2
        + [pltpu.VMEM((SETS, 8, 2, *BOTH[:2]), BF16)]
        + [pltpu.VMEM((8, 2, *kind[:2]), BF16) for _, kind in SPLIT]
        + sum((rs_scratch(kind) for _, kind in SPLIT), [])
        + rs_scratch(BOTH, (SETS,))
        + CLIP_SCRATCH,
        compiler_params=params(True),
        cost_estimate=cost(4),
        name="lower",
    )(dh, dht, at, act, gate, up, wd, *shards)


def solution(mesh):
    def step(x, dy, wg, wu, wd, *moments):
        h1, a1, a1t, dyt, a0t, act0, gate0, up0 = forward(x, dy, wg, wu, wd)
        flat_dy = dy.reshape(TOKENS, D)
        gd1, dg1, du1 = upper(a1, flat_dy, dyt, wg, wu, wd)
        gu1, d1, dh, dht = last(a1t, h1, flat_dy, dg1, du1, wg, wu, gd1)
        d0, gu0, factor = lower(dh, dht, a0t, act0, gate0, up0, wd, (d1, gu1))
        own, new_moments = adamw(factor, (gu0, d0, gu1, d1), moments[:3], moments[3:], (wg, wu, wd))
        return (*all_gather(own), *new_moments)

    seq = P(("rep", "dp"), None, None)
    whole = P(None, None, None)
    part = P(None, "dp", None)
    return jax.shard_map(
        step,
        mesh=mesh,
        in_specs=(seq, seq, whole, whole, whole) + (part,) * 6,
        out_specs=(P("rep", None, None),) * 3 + (P("rep", "dp", None),) * 6,
        check_vma=False,
    )
```

```python
import functools

import jax
import jax.numpy as jnp
from jax import lax
from jax.experimental import pallas as pl
from jax.experimental.pallas import tpu as pltpu
from jax.sharding import PartitionSpec as P

MESH = pl.DeviceIdType.MESH
F32, BF16 = jnp.float32, jnp.bfloat16
DEVICES, TOKENS, D, FF = 16, 2048, 896, 2560
COUNT = 2 * 3 * D * FF
TM = 256
Z = 0
NB = 512
STEPS = FF // NB
BN = 256
ANY = pl.BlockSpec(memory_space=pl.ANY)
WHOLE = pl.BlockSpec(memory_space=pltpu.VMEM)

STRIDE = (8, 4, 2)
ORDER = ((0, 1, 2), (1, 2, 0), (2, 0, 1))
WIDE = (56, 2560, tuple((slice(0, 56), s) for s in (slice(0, 896), slice(896, 1792), slice(1792, 2560))))
BLOCK = (56, 256, tuple((s, slice(0, 256)) for s in (slice(0, 24), slice(24, 40), slice(40, 56))))
PAIR = (56, 512, tuple((s, slice(0, 512)) for s in (slice(0, 24), slice(24, 40), slice(40, 56))))
TALL = (160, 896, tuple((s, slice(0, 896)) for s in (slice(0, 56), slice(56, 112), slice(112, 160))))


def size(s):
    return s.stop - s.start


def place():
    me = lax.axis_index("dp")
    return me, (me // 8 % 2, me // 4 % 2, me // 2 % 2), me % 2


def beside(me, xyz, axis):
    return me + STRIDE[axis] * (1 - 2 * xyz[axis])


def partner(me, core):
    return me + 1 - 2 * core


def rs_scratch(kind, sets=()):
    r, c, parts = kind
    flat = [pltpu.VMEM((*sets, 8, r, c), BF16)]
    for rows, cols in parts:
        flat += [pltpu.VMEM((*sets, 7, size(rows), size(cols)), BF16)] * 2
    return flat + [pltpu.SemaphoreType.DMA((*sets, 10))] * 2 + [pltpu.SemaphoreType.DMA((*sets, 1))]


RS_SCRATCH = 10


class Reduce:
    def __init__(self, kind, g, out, scratch, own=None, turn=0):
        self.kind, self.g, self.out, self.here = kind, g, out, own is None
        self.own = g if self.here else own
        self.other = scratch[0]
        self.send, self.got = scratch[1:7:2], scratch[2:7:2]
        self.ssem, self.rsem, self.lsem = scratch[7:]
        self.me, self.xyz, self.core = place()
        self.order = ORDER[turn:] + ORDER[:turn]

    def swap(self):
        return pltpu.make_async_remote_copy(
            self.g.at[:, 1 - self.core],
            self.other,
            self.ssem.at[9],
            self.rsem.at[9],
            device_id={"dp": partner(self.me, self.core)},
            device_id_type=MESH,
        )

    def load(self):
        return pltpu.make_async_copy(self.g.at[:, self.core], self.own, self.lsem.at[0])

    def hop(self, t, phase):
        at = pl.ds((0, 4, 6)[phase], (4, 2, 1)[phase])
        return pltpu.make_async_remote_copy(
            self.send[t].at[at],
            self.got[t].at[at],
            self.ssem.at[3 * t + phase],
            self.rsem.at[3 * t + phase],
            device_id={"dp": beside(self.me, self.xyz, self.order[t][phase])},
            device_id_type=MESH,
        )

    def total(self, t, at, got):
        rows, cols = self.kind[2][t]
        block = sum(p * (4, 2, 1)[axis] for p, axis in zip(at, self.order[t], strict=True))
        own = self.own[block, self.core, rows, cols] if self.here else self.own[block, rows, cols]
        sum_ = own.astype(F32) + self.other[block, rows, cols].astype(F32)
        for i in got:
            sum_ = sum_ + self.got[t][i].astype(F32)
        return sum_

    def start(self):
        self.swap().start()
        if not self.here:
            self.load().start()

    def stage(self, n):
        if n == 0:
            if not self.here:
                self.load().wait()
            self.swap().wait_recv()
        for t in range(3):
            p1, p2, p3 = (self.xyz[axis] for axis in self.order[t])
            if n:
                self.hop(t, n - 1).wait_recv()
            if n == 0:
                for j in range(2):
                    for k in range(2):
                        self.send[t][2 * j + k] = self.total(t, (1 - p1, j, k), ()).astype(BF16)
            elif n == 1:
                for k in range(2):
                    self.send[t][4 + k] = self.total(t, (p1, 1 - p2, k), (2 * (1 - p2) + k,)).astype(BF16)
            elif n == 2:
                self.send[t][6] = self.total(t, (p1, p2, 1 - p3), (2 * p2 + 1 - p3, 5 - p3)).astype(BF16)
            else:
                rows, cols = self.kind[2][t]
                self.out[rows, cols] = self.total(t, (p1, p2, p3), (2 * p2 + p3, 4 + p3, 6)).astype(BF16)
            if n < 3:
                self.hop(t, n).start()

    def finish(self):
        self.swap().wait_send()
        for t in range(3):
            for phase in range(3):
                self.hop(t, phase).wait_send()


def squares(g):
    wide = g.astype(F32)
    rows, cols = wide.shape
    s = jnp.sum((wide * wide).reshape(rows // 8, 8, cols), 0)
    return sum(s[:, i : i + 128] for i in range(0, cols, 128))


def clip_factor(shards, factor, squared, sums, ssem, rsem):
    me = lax.axis_index("dp")
    squared[...] = sum(squares(g[...]) for g in shards)

    def give(k, slot):
        to = (me + k) % DEVICES
        return pltpu.make_async_remote_copy(
            squared, sums.at[slot], ssem.at[k], rsem.at[slot], device_id={"dp": to}, device_id_type=MESH
        )

    for k in range(1, DEVICES):
        give(k, me).start()
    sums[me] = squared[...]
    for k in range(1, DEVICES):
        give(k, (me + k) % DEVICES).wait_recv()
    for k in range(1, DEVICES):
        give(k, me).wait_send()
    total = jnp.sum(jnp.sum(jnp.sum(sums[...], 0), 0, keepdims=True), 1, keepdims=True)
    f = jnp.minimum(1.0, 0.5 * lax.rsqrt(total / COUNT + 1e-30))
    factor[...] = jnp.broadcast_to(f, factor.shape)


CLIP_SCRATCH = [
    pltpu.VMEM((8, 128), F32),
    pltpu.VMEM((DEVICES, 8, 128), F32),
    pltpu.SemaphoreType.DMA((DEVICES,)),
    pltpu.SemaphoreType.DMA((DEVICES,)),
]


def at_end_of(step, plan):
    for when, entries in plan.items():

        @pl.when(step == when)
        def _(entries=entries):
            for unit, stage in entries:
                if stage == "start":
                    unit.start()
                elif stage == "finish":
                    unit.finish()
                else:
                    unit.stage(stage)


class Gather:
    def __init__(self, kind, own, out, layer, ssem, rsem, csem):
        self.kind, self.own, self.out, self.layer = kind, own, out, layer
        self.ssem, self.rsem, self.csem = ssem, rsem, csem
        self.me, self.xyz, self.core = place()

    def local(self):
        x, y, z = self.xyz
        return pltpu.make_async_copy(self.own, self.out.at[self.layer, x, y, z, self.core], self.csem)

    def blocks(self, t, core, known, other=None):
        rows, cols = self.kind[2][t]
        index = []
        for axis in range(3):
            p = self.xyz[axis]
            index.append(slice(None) if axis in known else (1 - p if axis == other else p))
        return self.out.at[(self.layer, *index, core, rows, cols)]

    def hop(self, t, phase, arriving=False):
        axis = ORDER[t][phase]
        known = ORDER[t][:phase]
        src = self.blocks(t, self.core, known)
        dst = self.blocks(t, self.core, known, axis) if arriving else src
        if phase == 0 and not arriving:
            src = self.own.at[self.kind[2][t]]
        return pltpu.make_async_remote_copy(
            src,
            dst,
            self.ssem.at[3 * t + phase],
            self.rsem.at[3 * t + phase],
            device_id={"dp": beside(self.me, self.xyz, axis)},
            device_id_type=MESH,
        )

    def share(self, t, phase, core):
        ref = self.blocks(t, core, ORDER[t][:phase], ORDER[t][phase])
        return pltpu.make_async_remote_copy(
            ref,
            ref,
            self.ssem.at[10 + 3 * t + phase],
            self.rsem.at[10 + 3 * t + phase],
            device_id={"dp": partner(self.me, self.core)},
            device_id_type=MESH,
        )

    def share_own(self, core):
        x, y, z = self.xyz
        return pltpu.make_async_remote_copy(
            self.own,
            self.out.at[self.layer, x, y, z, core],
            self.ssem.at[9],
            self.rsem.at[9],
            device_id={"dp": partner(self.me, self.core)},
            device_id_type=MESH,
        )

    def start(self):
        self.local().start()
        for t in range(3):
            self.hop(t, 0).start()
        self.share_own(self.core).start()

    def stage(self, phase):
        if phase == 0:
            self.local().wait()
        for t in range(3):
            self.hop(t, phase, True).wait_recv()
            if phase < 2:
                self.hop(t, phase + 1).start()
            self.share(t, phase, self.core).start()

    def finish(self):
        self.share_own(1 - self.core).wait_recv()
        self.share_own(self.core).wait_send()
        for t in range(3):
            for phase in range(3):
                self.share(t, phase, 1 - self.core).wait_recv()
                self.share(t, phase, self.core).wait_send()
                self.hop(t, phase).wait_send()


def gather_kernel(*refs):
    owns, outs, (ssem, rsem, csem) = refs[:3], refs[3:6], refs[6:]
    units = []
    for layer in range(2):
        for i, kind in enumerate((WIDE, WIDE, TALL)):
            u = 3 * layer + i
            units.append(Gather(kind, owns[i].at[layer], outs[i], layer, ssem.at[u], rsem.at[u], csem.at[u]))
    for u in units:
        u.start()
    for phase in range(3):
        for u in units:
            u.stage(phase)
    for u in units:
        u.finish()


def all_gather(owns):
    outs = pl.pallas_call(
        gather_kernel,
        out_shape=[pltpu.VMEM((2, 2, 2, 2, 2, *o.shape[1:]), BF16) for o in owns],
        in_specs=[WHOLE] * 3,
        out_specs=[WHOLE] * 3,
        scratch_shapes=[
            pltpu.SemaphoreType.DMA((6, 19)),
            pltpu.SemaphoreType.DMA((6, 19)),
            pltpu.SemaphoreType.DMA((6,)),
        ],
        compiler_params=pltpu.CompilerParams(has_side_effects=True, vmem_limit_bytes=8 << 20),
        name="all_gather",
    )(*owns)
    outs = pl.pallas_call(
        flush_kernel,
        out_shape=[jax.ShapeDtypeStruct(o.shape, BF16) for o in outs],
        in_specs=[WHOLE] * 3,
        out_specs=[ANY] * 3,
        scratch_shapes=[pltpu.SemaphoreType.DMA((6,))],
        compiler_params=pltpu.CompilerParams(vmem_limit_bytes=1 << 20),
        name="flush",
    )(*outs)
    return [o.reshape(2, DEVICES * o.shape[-2], o.shape[-1]) for o in outs]


def flush_kernel(*refs):
    copies = []
    for i in range(3):
        for layer in range(2):
            copies.append(pltpu.make_async_copy(refs[i].at[layer], refs[3 + i].at[layer], refs[6].at[2 * i + layer]))
    for c in copies:
        c.start()
    for c in copies:
        c.wait()


KINDS = (WIDE, WIDE, TALL)


def adamw_kernel(*refs):
    factor, shards, ms, vs, weights = refs[0], refs[1:7], refs[7:10], refs[10:13], refs[13:16]
    new_ws, new_ms, new_vs = refs[16:19], refs[19:22], refs[22:25]
    in_ms, in_vs, gs, (isem, osem) = refs[25:28], refs[28:31], refs[31:34], refs[34:]
    me = lax.axis_index("dp")
    loads, stores = [], []
    for i, kind in enumerate(KINDS):
        mine = pl.ds(pl.multiple_of(me * kind[0], 8), kind[0])
        for layer in range(2):
            pairs = (
                (shards[3 * layer + i], gs[i].at[layer]),
                (ms[i].at[layer], in_ms[i].at[layer]),
                (vs[i].at[layer], in_vs[i].at[layer]),
                (weights[i].at[layer, mine], new_ws[i].at[layer]),
            )
            loads.append([pltpu.make_async_copy(src, dst, isem.at[2 * i + layer, k]) for k, (src, dst) in enumerate(pairs)])
            pairs = (in_ms[i], new_ms[i]), (in_vs[i], new_vs[i])
            stores.append(
                [
                    pltpu.make_async_copy(src.at[layer], dst.at[layer], osem.at[2 * i + layer, k])
                    for k, (src, dst) in enumerate(pairs)
                ]
            )
    for copies in loads:
        for c in copies:
            c.start()
    f = factor[0:1, 0:1]
    for u in range(6):
        i, layer = divmod(u, 2)
        for c in loads[u]:
            c.wait()
        g = gs[i][layer].astype(F32) * f
        w = new_ws[i][layer].astype(F32)
        m = 0.9 * in_ms[i][layer] + 0.1 * g
        v = 0.95 * in_vs[i][layer] + 0.05 * g * g
        step = m * lax.rsqrt(v + 1e-8) + 0.1 * w
        new_ws[i][layer], in_ms[i][layer], in_vs[i][layer] = (w - 0.02 * step).astype(BF16), m, v
        for c in stores[u]:
            c.start()
    for copies in stores:
        for c in copies:
            c.wait()


def adamw(factor, shards, ms, vs, weights):
    own = [(2, *k[:2]) for k in KINDS]
    outs = pl.pallas_call(
        adamw_kernel,
        out_shape=[pltpu.VMEM(s, BF16) for s in own] + [jax.ShapeDtypeStruct(s, F32) for s in own * 2],
        in_specs=[WHOLE] + [ANY] * 15,
        out_specs=[WHOLE] * 3 + [ANY] * 6,
        scratch_shapes=[pltpu.VMEM(s, t) for t in (F32, F32, BF16) for s in own]
        + [pltpu.SemaphoreType.DMA((6, 4)), pltpu.SemaphoreType.DMA((6, 2))],
        compiler_params=pltpu.CompilerParams(vmem_limit_bytes=60 * 1024 * 1024),
        name="adamw",
    )(factor, *shards, *ms, *vs, *weights)
    return outs[:3], outs[3:]


def dot(a, b):
    return jnp.dot(a, b, preferred_element_type=F32)


def dot_t(a, b):
    return lax.dot_general(a, b, (((1,), (1,)), ((), ())), preferred_element_type=F32)


def norm(h):
    wide = h.astype(F32)
    scale = lax.rsqrt(jnp.mean(wide * wide, -1, keepdims=True) + 1e-6)
    return wide, scale, (wide * scale).astype(BF16)


def gated_back(gate, up, dact):
    sig = jax.nn.sigmoid(gate)
    d = dact.astype(F32)
    dup = d * (gate * sig)
    dgate = d * up * (sig * (1 + gate * (1 - sig)))
    return dgate.astype(BF16), dup.astype(BF16)


def forward_kernel(x, dy, wg, wu, wd, h1, a1, a1t, dyt, at, act, gate, up):
    h = x[...]
    _, _, a = norm(h)
    at[...] = a.T
    dyt[...] = dy[...].T
    g = dot(a, wg[...])
    u = dot(a, wu[...])
    gate[...] = g
    up[...] = u
    s = (g * jax.nn.sigmoid(g) * u).astype(BF16)
    act[...] = s
    h = h + dot(s, wd[...]).astype(BF16)
    h1[...] = h
    _, _, a = norm(h)
    a1[...] = a
    a1t[...] = a.T


def pieces(count):
    n = TOKENS // count
    return [slice(n * i, n * i + n) for i in range(count)]


def wide_block(at, dg):
    return dot(at[...], dg[...]).reshape(8, 2, 56, dg.shape[-1]).astype(BF16)


def last_kernel(hbm_a, hbm_at, hbm_dy, hbm_dyt, hbm_h, wg, wu, wd, gd, og, ou, out_dh, out_dht, *scratch):
    a, at, dy, dyt, h, act, dg, du, acc_g, acc_u, own_g, own_u, lsem, osem = scratch[:14]
    step = pl.program_id(0)
    sources = (hbm_a, hbm_dy, hbm_at, hbm_dyt, hbm_h)
    loads = [pltpu.make_async_copy(s, d, lsem.at[i]) for i, (s, d) in enumerate(zip(sources, (a, dy, at, dyt, h), strict=True))]

    def first(i):
        @pl.when(step == 0)
        def _():
            loads[i].wait()

    def units(k):
        columns = pl.ds(pl.multiple_of(k * NB, NB), NB)
        rest = [ref.at[k % 3] for ref in scratch[14:]]
        return [
            Reduce(PAIR, own.at[k % 2], out.at[:, columns], rest[RS_SCRATCH * i : RS_SCRATCH * (i + 1)], turn=i)
            for i, (own, out) in enumerate(((own_g, og), (own_u, ou)))
        ]

    def reduce(k, *stages):
        for stage in stages:
            for u in units(k):
                if stage == "start":
                    u.start()
                elif stage == "finish":
                    u.finish()
                else:
                    u.stage(stage)

    @pl.when(step == 0)
    def _():
        for c in loads:
            c.start()
        acc_g[...] = jnp.zeros_like(acc_g)
        acc_u[...] = jnp.zeros_like(acc_u)
        loads[0].wait()
        loads[1].wait()

    def projections(r):
        g = dot(a[r], wg[...])
        u = dot(a[r], wu[...])
        dact = dot_t(dy[r], wd[...]).astype(BF16)
        act[r] = (g * jax.nn.sigmoid(g) * u).astype(BF16)
        dg[r], du[r] = gated_back(g, u, dact)

    quarters = pieces(4)
    for r in quarters:
        projections(r)

    @pl.when(step > 0)
    def _():
        reduce(step - 1, 1)

    first(2)
    own_g[step % 2] = wide_block(at, dg)
    own_u[step % 2] = wide_block(at, du)
    reduce(step, "start")
    first(3)
    gd[...] = dot(dyt[...], act[...]).astype(BF16).T

    @pl.when(step > 0)
    def _():
        reduce(step - 1, 2)

    for r in quarters:
        acc_g[r] += dot_t(dg[r], wg[...])
        acc_u[r] += dot_t(du[r], wu[...])

    @pl.when(step > 0)
    def _():
        reduce(step - 1, 3, "finish")

    reduce(step, 0)

    @pl.when(step == STEPS - 1)
    def _():
        loads[4].wait()

        def through(i, carry):
            r = pl.ds(pl.multiple_of(i * 256, 256), 256)
            d = (acc_g[r].astype(BF16) + acc_u[r].astype(BF16)).astype(F32)
            wide, scale, _ = norm(h[r])
            d = d * scale - wide * (scale * scale * scale * (jnp.sum(d * wide, -1, keepdims=True) / D))
            d = dy[r] + d.astype(BF16)
            a[r] = d
            at[:, r] = d.T
            return carry

        lax.fori_loop(0, 8, through, 0)
        reduce(step, 1)
        stores = [pltpu.make_async_copy(s, d, osem.at[i]) for i, (s, d) in enumerate(((a, out_dh), (at, out_dht)))]
        for c in stores:
            c.start()
        reduce(step, 2, 3, "finish")
        for c in stores:
            c.wait()


SETS = 7


def lower_kernel(dh, dht, at, act, gate, up, wd, gd1, g1, u1, od1, od, og, ou, factor, *scratch):
    step = pl.program_id(0)
    dg, du, own_g, own_u, own_d, half_d1 = scratch[:6]
    rest = scratch[6:]
    sets = [rest[RS_SCRATCH * i : RS_SCRATCH * (i + 1)] for i in range(2 + 2 * SETS)]
    d1 = Reduce(TALL, gd1, od1, sets[0], half_d1)
    d = Reduce(TALL, own_d, od, sets[1], turn=1)

    @pl.when(step == 0)
    def _():
        d1.start()

    @pl.when(step < STEPS)
    def _():
        rows = pl.ds(pl.multiple_of(step * NB, NB), NB)
        own_d.reshape(FF, D)[rows] = dot(dht[...], act[...]).astype(BF16).T

    @pl.when(step >= STEPS)
    def _():
        for r in pieces(4):
            dact = dot_t(dh[r], wd[...]).astype(BF16)
            dg[r], du[r] = gated_back(gate[r], up[r], dact)
        i = (step - STEPS) % SETS
        own_g[i] = wide_block(at, dg)
        own_u[i] = wide_block(at, du)

    plan = {when: [] for when in range(3 * STEPS)}
    for when, unit, stage in ((2, d1, 0), (6, d1, 1), (8, d1, 2), (10, d1, 3), (4, d, "start"), (6, d, 0), (9, d, 1), (11, d, 2), (12, d, 3)):
        plan[when].append((unit, stage))
    tail = []
    for j in range(2 * STEPS):
        k = j % SETS
        pair = [
            Reduce(BLOCK, own.at[k], out.at[:, BN * j : BN * j + BN], sets[2 + 2 * k + i], turn=(i + j) % 3)
            for i, (own, out) in enumerate(((own_g, og), (own_u, ou)))
        ]
        for n, stage in zip((0, 1, 3, 5, 6), ("start", 0, 1, 2, 3), strict=True):
            when = STEPS + j + n
            late = when - (3 * STEPS - 1)
            for unit in pair:
                if late <= 0:
                    plan[when].append((unit, stage))
                else:
                    tail.append((late, unit, stage))
        last = [(unit, "finish") for unit in pair]
        if STEPS + j + 6 < 3 * STEPS:
            plan[STEPS + j + 6] += last
        else:
            tail += [(9, *entry) for entry in last]
    tail = [entry[1:] for entry in sorted(tail, key=lambda entry: entry[0])]
    plan[3 * STEPS - 1] += tail + [(d1, "finish"), (d, "finish")]
    at_end_of(step, plan)

    @pl.when(step == 3 * STEPS - 1)
    def _():
        clip_factor([g1, u1, od1, od, og, ou], factor, *rest[RS_SCRATCH * (2 + 2 * SETS) :])


def rows(cols):
    return pl.BlockSpec((TM, cols), lambda i: (i, Z))


SEQ = pl.BlockSpec((None, TM, D), lambda i: (Z, i, Z))
COLUMNS = pl.BlockSpec((D, TM), lambda i: (Z, i))


def weight(layer, shape):
    return pl.BlockSpec((None, *shape), lambda i: (layer, Z, Z), pipeline_mode=pl.Buffered(1))


def matrix(r, c, t=BF16):
    return jax.ShapeDtypeStruct((r, c), t)


def cost(matmuls):
    return pl.CostEstimate(flops=matmuls * 2 * TOKENS * D * FF, bytes_accessed=60 << 20, transcendentals=0)


def params(remote=False):
    return pltpu.CompilerParams(vmem_limit_bytes=67043328 if remote else 60 * 1024 * 1024, has_side_effects=remote)


def shard(kind):
    return pl.BlockSpec(kind[:2], lambda i: (Z, Z))


def forward(x, dy, wg, wu, wd):
    return pl.pallas_call(
        forward_kernel,
        grid=(TOKENS // TM,),
        in_specs=[SEQ, SEQ, weight(0, (D, FF)), weight(0, (D, FF)), weight(0, (FF, D))],
        out_specs=[rows(D), rows(D), COLUMNS, COLUMNS, COLUMNS, rows(FF), rows(FF), rows(FF)],
        out_shape=[matrix(TOKENS, D)] * 2 + [matrix(D, TOKENS)] * 3 + [matrix(TOKENS, FF)] + [matrix(TOKENS, FF, F32)] * 2,
        compiler_params=params(),
        cost_estimate=cost(3),
        name="forward",
    )(x, dy, wg, wu, wd)


def last(a, at, dy, dyt, h, wg, wu, wd):
    wide = pl.BlockSpec((None, D, NB), lambda i: (1, Z, i))
    straight, turned = pltpu.VMEM((TOKENS, D), BF16), pltpu.VMEM((D, TOKENS), BF16)
    hidden, sums = pltpu.VMEM((TOKENS, NB), BF16), pltpu.VMEM((TOKENS, D), F32)
    own = pltpu.VMEM((2, 8, 2, *PAIR[:2]), BF16)
    return pl.pallas_call(
        last_kernel,
        grid=(STEPS,),
        in_specs=[ANY] * 5 + [wide, wide, pl.BlockSpec((None, NB, D), lambda i: (1, i, Z))],
        out_specs=[pl.BlockSpec((NB, D), lambda i: (i, Z)), shard(WIDE), shard(WIDE), ANY, ANY],
        out_shape=[matrix(FF, D), matrix(*WIDE[:2]), matrix(*WIDE[:2]), matrix(TOKENS, D), matrix(D, TOKENS)],
        scratch_shapes=[straight, turned, straight, turned, straight, hidden, hidden, hidden, sums, sums, own, own]
        + [pltpu.SemaphoreType.DMA((5,)), pltpu.SemaphoreType.DMA((2,))]
        + rs_scratch(PAIR, (3,)) * 2,
        compiler_params=params(True),
        cost_estimate=cost(8),
        name="last",
    )(a, at, dy.reshape(TOKENS, D), dyt, h, wg, wu, wd)


WHOLE_S = pl.BlockSpec((TOKENS, D), lambda i: (Z, Z), pipeline_mode=pl.Buffered(1))
WHOLE_T = pl.BlockSpec((D, TOKENS), lambda i: (Z, Z), pipeline_mode=pl.Buffered(1))


def lower(dh, dht, at, act, gate, up, wd, gd1, g1, u1):
    def later(i):
        return jnp.maximum(i - STEPS, 0)

    block = pl.BlockSpec((TOKENS, BN), lambda i: (Z, later(i)))
    outs = (TALL, TALL, WIDE, WIDE)
    return pl.pallas_call(
        lower_kernel,
        grid=(3 * STEPS,),
        in_specs=[
            WHOLE_S,
            WHOLE_T,
            WHOLE_T,
            pl.BlockSpec((TOKENS, NB), lambda i: (Z, jnp.minimum(i, STEPS - 1))),
            block,
            block,
            pl.BlockSpec((None, BN, D), lambda i: (Z, later(i), Z)),
            ANY,
            shard(WIDE),
            shard(WIDE),
        ],
        out_specs=[shard(k) for k in outs] + [pl.BlockSpec((8, 128), lambda i: (Z, Z))],
        out_shape=[matrix(*k[:2]) for k in outs] + [matrix(8, 128, F32)],
        scratch_shapes=[pltpu.VMEM((TOKENS, BN), BF16)] * 2
        + [pltpu.VMEM((SETS, 8, 2, *BLOCK[:2]), BF16)] * 2
        + [pltpu.VMEM((8, 2, *TALL[:2]), BF16), pltpu.VMEM((8, *TALL[:2]), BF16)]
        + rs_scratch(TALL) * 2
        + rs_scratch(BLOCK) * (2 * SETS)
        + CLIP_SCRATCH,
        compiler_params=params(True),
        cost_estimate=cost(4),
        name="lower",
    )(dh, dht, at, act, gate, up, wd, gd1.reshape(8, 2, *TALL[:2]), g1, u1)


def solution(mesh):
    def step(x, dy, wg, wu, wd, *moments):
        h1, a1, a1t, dyt, a0t, act0, gate0, up0 = forward(x, dy, wg, wu, wd)
        gd1, g1, u1, dh, dht = last(a1, a1t, dy, dyt, h1, wg, wu, wd)
        d1, d0, g0, u0, factor = lower(dh, dht, a0t, act0, gate0, up0, wd, gd1, g1, u1)
        own, new_moments = adamw(factor, (g0, u0, d0, g1, u1, d1), moments[:3], moments[3:], (wg, wu, wd))
        return (*all_gather(own), *new_moments)

    seq = P(("rep", "dp"), None, None)
    whole = P(None, None, None)
    part = P(None, "dp", None)
    return jax.shard_map(
        step,
        mesh=mesh,
        in_specs=(seq, seq, whole, whole, whole) + (part,) * 6,
        out_specs=(P("rep", None, None),) * 3 + (P("rep", "dp", None),) * 6,
        check_vma=False,
    )
```
